32 devices in a mesh: dp: 2 (over x), m1: 4 (over z), m2: 4 (over y, core).
Axes of the slice: x: 2, y: 2, z: 4, core: 2. Of those that a mesh axis runs over, the one named last changes fastest.
Arguments:
- x: bfloat16 [16, 256, 6144], P('dp', None, 'm1'), parts along dimension 0
- ln_scale: float32 [6144], replicated
- qn_scale: float32 [128], replicated
- kn_scale: float32 [128], replicated
- w_qkv: bfloat16 [6144, 3, 6144], P('m1', None, 'm2')
- w_up: bfloat16 [6144, 24576], P('m1', 'm2')
- b_up: float32 [24576], P('m2')
- w_o: bfloat16 [6144, 6144], P('m2', 'm1')
- w_down: bfloat16 [24576, 6144], P('m2', 'm1')
- b_out: float32 [6144], P('m1')
Outputs:
- output: bfloat16 [16, 256, 6144], P('dp', None, 'm1'), parts along dimension 0
There are 2 independent parts. The reference program is written for one: setup_inputs(seed, part) draws one part's arguments, and reference() takes and returns one part's arrays. A program takes and returns all parts, laid end to end along the dimension named above; an argument that names none is the same for every part.
All inputs are finite; a program needn't handle non-finite values.
Results may differ from the reference program's by a relative error of at most 0.0107519.
Values are sent between devices in bfloat16 or wider.
A program may use at most 1 GiB of HBM per device.

```python
import jax
import jax.numpy as jnp
from jax import lax

BATCH = 8
PATCHES = 256
MODEL_DIM = 6144
HEADS = 48
HEAD_DIM = 128
MLP_DIM = 24576
LN_EPS = 1e-6


def setup_inputs(seed: int = 0, part: int = 0) -> dict:
    part_key = jax.random.fold_in(jax.random.key(seed), part)
    key_mean, key_scale, key_noise = jax.random.split(part_key, 3)
    shared = jax.random.split(jax.random.key(seed + 1), 9)
    qkv_width = HEADS * HEAD_DIM
    tok_mean = 1.5 * jax.random.normal(key_mean, (BATCH, PATCHES, 1), jnp.float32)
    tok_scale = jax.random.uniform(key_scale, (BATCH, PATCHES, 1), jnp.float32, 0.5, 2.0)
    col_scale = 0.5 + 1.5 * jnp.arange(MODEL_DIM, dtype=jnp.float32) / MODEL_DIM
    noise = jax.random.normal(key_noise, (BATCH, PATCHES, MODEL_DIM), jnp.float32)
    x = (tok_mean + tok_scale * col_scale * noise).astype(jnp.bfloat16)
    ln_scale = jax.random.uniform(shared[0], (MODEL_DIM,), jnp.float32, 0.5, 1.5)
    qn_scale = jax.random.uniform(shared[1], (HEAD_DIM,), jnp.float32, 1.0, 2.5)
    kn_scale = jax.random.uniform(shared[2], (HEAD_DIM,), jnp.float32, 1.0, 2.5)
    w_qkv = (jax.random.normal(shared[3], (MODEL_DIM, 3, qkv_width), jnp.float32) * MODEL_DIM ** -0.5).astype(jnp.bfloat16)
    w_up = (jax.random.normal(shared[4], (MODEL_DIM, MLP_DIM), jnp.float32) * MODEL_DIM ** -0.5).astype(jnp.bfloat16)
    b_up = 0.5 * jax.random.normal(shared[5], (MLP_DIM,), jnp.float32)
    w_o = (jax.random.normal(shared[6], (qkv_width, MODEL_DIM), jnp.float32) * qkv_width ** -0.5).astype(jnp.bfloat16)
    w_down = (jax.random.normal(shared[7], (MLP_DIM, MODEL_DIM), jnp.float32) * MLP_DIM ** -0.5).astype(jnp.bfloat16)
    b_out = 0.5 * jax.random.normal(shared[8], (MODEL_DIM,), jnp.float32)
    return {'x': x, 'ln_scale': ln_scale, 'qn_scale': qn_scale, 'kn_scale': kn_scale, 'w_qkv': w_qkv, 'w_up': w_up, 'b_up': b_up, 'w_o': w_o, 'w_down': w_down, 'b_out': b_out}


def layer_norm(values, scale):
    mean = jnp.mean(values, axis=-1, keepdims=True)
    centered = values - mean
    variance = jnp.mean(centered * centered, axis=-1, keepdims=True)
    return centered * lax.rsqrt(variance + LN_EPS) * scale


def attend_one(operands):
    queries, keys, values = operands
    scores = jnp.einsum('nhd,mhd->hnm', queries.astype(jnp.float32), keys.astype(jnp.float32)) * HEAD_DIM ** -0.5
    attn_probs = jax.nn.softmax(scores, axis=-1).astype(jnp.bfloat16)
    attended = jnp.einsum('hnm,mhd->nhd', attn_probs.astype(jnp.float32), values.astype(jnp.float32))
    return attended.astype(jnp.bfloat16)


def reference(x, ln_scale, qn_scale, kn_scale, w_qkv, w_up, b_up, w_o, w_down, b_out):
    tokens = BATCH * PATCHES
    qkv_width = HEADS * HEAD_DIM
    x_flat = x.reshape(tokens, MODEL_DIM).astype(jnp.float32)
    normed = layer_norm(x_flat, ln_scale).astype(jnp.bfloat16)
    proj_qkv = jnp.dot(normed, w_qkv.reshape(MODEL_DIM, 3 * qkv_width), preferred_element_type=jnp.float32).astype(jnp.bfloat16)
    proj_qkv = proj_qkv.reshape(BATCH, PATCHES, 3, HEADS, HEAD_DIM)
    queries = layer_norm(proj_qkv[:, :, 0].astype(jnp.float32), qn_scale).astype(jnp.bfloat16)
    keys = layer_norm(proj_qkv[:, :, 1].astype(jnp.float32), kn_scale).astype(jnp.bfloat16)
    attended = lax.map(attend_one, (queries, keys, proj_qkv[:, :, 2]))
    up_in = jnp.dot(normed, w_up, preferred_element_type=jnp.float32).astype(jnp.bfloat16)
    hidden = jax.nn.gelu(up_in.astype(jnp.float32) + b_up, approximate=False).astype(jnp.bfloat16)
    mixed_sum = jnp.dot(attended.reshape(tokens, qkv_width), w_o, preferred_element_type=jnp.float32) + jnp.dot(hidden, w_down, preferred_element_type=jnp.float32)
    result = x_flat + mixed_sum + b_out
    return result.astype(jnp.bfloat16).reshape(BATCH, PATCHES, MODEL_DIM)
```

```python
import functools

import jax
import jax.numpy as jnp
from jax import lax
from jax.experimental import pallas as pl
from jax.experimental.pallas import tpu as pltpu
from jax.sharding import PartitionSpec as P

LN_EPS = 1e-6
MESH = pl.DeviceIdType.MESH
LANES = 128
LAG = 3


def xors(value):
    return (value, value + 1 - 2 * lax.rem(value, 2), value + 2 - 4 * lax.div(value, 2), 3 - value)


def ds(start, size):
    return pl.ds(pl.multiple_of(start, size if size < LANES else LANES), size)


def rows_at(start, size):
    return pl.ds(pl.multiple_of(start, 8), size)


def rcopy(src, dst, send_sem, recv_sem, device):
    return pltpu.make_async_remote_copy(src_ref=src, dst_ref=dst, send_sem=send_sem, recv_sem=recv_sem, device_id=device, device_id_type=MESH)


def dot(lhs, rhs):
    return jnp.dot(lhs, rhs, preferred_element_type=jnp.float32)


def head_norm(values, scale):
    mean = jnp.mean(values, axis=-1, keepdims=True)
    centered = values - mean
    variance = jnp.mean(centered * centered, axis=-1, keepdims=True)
    return (centered * lax.rsqrt(variance + LN_EPS) * scale).astype(jnp.bfloat16)


def kernel(sizes, x, lns, qns, kns, wq, wu, bu, wo, wd, bo,
           out, u, w1, w2, ra,
           xg, ubl, zq, h, rhs, lhs, w2b, pa, po, rav, ss, rb, rc, ud, rd, fin,
           xs, xr, w1s, w1r, f1s, f1r, us, ur, w2s, w2r, f2s, f2r,
           as_, ar, bs, br, cs, cr, dsm, drm, es, er, own_sem, rhs_sem, lhs_sem, ub_sem, w2b_sem, rav_sem, fin_sem):
    batch, patches, dim, qw, uw = sizes
    tokens = batch * patches
    rows = tokens // 4
    block = rows // 2
    half = dim // 2
    total = 4 * dim
    nub = uw // qw
    nc = dim // LANES
    wide = 4 * LANES
    heads = qw // LANES
    ln_rows = min(64, rows)

    g, i, j = lax.axis_index('dp'), lax.axis_index('m1'), lax.axis_index('m2')
    ip, jp = xors(i), xors(j)
    jy, jc = lax.div(j, 2), lax.rem(j, 2)

    barrier = pltpu.get_barrier_semaphore()
    peers = [{'m1': ip[e]} for e in (1, 2, 3)] + [{'m2': jp[e]} for e in (1, 2, 3)] + [{'dp': 1 - g}]
    for peer in peers:
        pl.semaphore_signal(barrier, inc=1, device_id=peer, device_id_type=MESH)
    pl.semaphore_wait(barrier, len(peers))

    mine = rows_at(j * rows, rows)
    x_far = rcopy(x.at[mine, :], xg.at[i], xs.at[0], xr.at[0], {'m1': ip[2]})
    x_near = rcopy(x.at[mine, :], xg.at[i], xs.at[1], xr.at[1], {'m1': ip[1]})
    x_own = pltpu.make_async_copy(x.at[mine, :], xg.at[i], own_sem.at[0])
    x_far.start()
    x_near.start()
    x_own.start()
    x_far_in = rcopy(xg.at[ip[2]], xg.at[ip[2]], xs.at[0], xr.at[0], {'m1': ip[2]})
    x_far_in.wait_recv()
    x_fwd = rcopy(xg.at[ip[2]], xg.at[ip[2]], xs.at[2], xr.at[2], {'m1': ip[1]})
    x_fwd.start()

    def z1(b, e):
        t = ip[e]
        if b < 3:
            src = wq.at[b, rows_at(g * half, half), ds(t * qw, qw)]
        else:
            src = wu.at[rows_at(g * half, half), ds(t * uw + (b - 3) * qw, qw)]
        return rcopy(src, w1.at[b, rows_at(i * dim + g * half, half), :], w1s.at[b, e - 1], w1r.at[b, e - 1], {'m1': t})

    def f1(b, e):
        part = w1.at[b, rows_at(ip[e] * dim + g * half, half), :]
        return rcopy(part, part, f1s.at[b, e - 1], f1r.at[b, e - 1], {'dp': 1 - g})

    def z1_in(b, e):
        part = w1.at[b, rows_at(ip[e] * dim + g * half, half), :]
        return rcopy(part, part, w1s.at[b, e - 1], w1r.at[b, e - 1], {'m1': ip[e]})

    def f1_in(b, e):
        part = w1.at[b, rows_at(ip[e] * dim + (1 - g) * half, half), :]
        return rcopy(part, part, f1s.at[b, e - 1], f1r.at[b, e - 1], {'dp': 1 - g})

    def forward1(b):
        for e in (2, 3, 1):
            z1_in(b, e).wait_recv()
            f1(b, e).start()

    for b in range(3 + nub):
        for e in (2, 3, 1):
            z1(b, e).start()

    def parts2(c, e, group, kind):
        size, first = (qw // 2, 0) if kind == 0 else (uw // 2, qw)
        return size, first + group * size

    def z2(c, e, kind):
        size, at = parts2(c, e, g, kind)
        t = ip[e]
        src = wo if kind == 0 else wd
        start = t * (2 * size) + g * size
        return rcopy(src.at[rows_at(start, size), ds(c * LANES, LANES)], w2.at[c, rows_at(at, size), ds(i * LANES, LANES)],
                     w2s.at[c, e - 1, kind], w2r.at[c, e - 1, kind], {'m1': t})

    def region2(c, e, group, kind):
        size, at = parts2(c, e, group, kind)
        return w2.at[c, rows_at(at, size), ds(ip[e] * LANES, LANES)]

    def z2_in(c, e, kind):
        part = region2(c, e, g, kind)
        return rcopy(part, part, w2s.at[c, e - 1, kind], w2r.at[c, e - 1, kind], {'m1': ip[e]})

    def f2(c, e, kind):
        part = region2(c, e, g, kind)
        return rcopy(part, part, f2s.at[c, e - 1, kind], f2r.at[c, e - 1, kind], {'dp': 1 - g})

    def f2_in(c, e, kind):
        part = region2(c, e, 1 - g, kind)
        return rcopy(part, part, f2s.at[c, e - 1, kind], f2r.at[c, e - 1, kind], {'dp': 1 - g})

    pieces2 = [(e, kind) for e in (2, 3, 1) for kind in (1, 0)]

    def issue2(first, last):
        @pl.loop(first, last)
        def _(c):
            for e, kind in pieces2:
                z2(c, e, kind).start()

    def forward2(c):
        for e, kind in pieces2:
            z2_in(c, e, kind).wait_recv()
            f2(c, e, kind).start()

    cuts = [nc * k // 4 for k in range(5)]

    x_own.wait()
    rcopy(xg.at[ip[1]], xg.at[ip[1]], xs.at[1], xr.at[1], {'m1': ip[1]}).wait_recv()
    rcopy(xg.at[ip[3]], xg.at[ip[3]], xs.at[2], xr.at[2], {'m1': ip[1]}).wait_recv()

    def u_out(r, slot):
        return pltpu.make_async_copy(ubl.at[slot], u.at[rows_at(j * rows + r * ln_rows, ln_rows), :], ub_sem.at[slot])

    @pl.loop(0, rows // ln_rows)
    def _(r):
        slot = lax.rem(r, 2)

        @pl.when(r >= 2)
        def _():
            u_out(r - 2, slot).wait()
        at = rows_at(r * ln_rows, ln_rows)
        parts = [xg[s, at, :].astype(jnp.float32) for s in range(4)]
        mean = sum(jnp.sum(part, axis=-1, keepdims=True) for part in parts) / total
        parts = [part - mean for part in parts]
        variance = sum(jnp.sum(part * part, axis=-1, keepdims=True) for part in parts) / total
        inverse = lax.rsqrt(variance + LN_EPS)
        for s in range(4):
            cols = slice(s * dim, (s + 1) * dim)
            ubl[slot, :, cols] = (parts[s] * inverse * lns[:, cols]).astype(jnp.bfloat16)
        u_out(r, slot).start()

    for r in range(max(0, rows // ln_rows - 2), rows // ln_rows):
        u_out(r, r % 2).wait()

    def u_rows(q):
        return u.at[rows_at(q * rows, rows), :]

    u_far = rcopy(u_rows(j), u_rows(j), us.at[0], ur.at[0], {'m2': jp[2]})
    u_near = rcopy(u_rows(j), u_rows(j), us.at[1], ur.at[1], {'m2': jp[1]})
    u_far.start()
    u_near.start()
    for b in range(4):
        forward1(b)
    issue2(cuts[0], cuts[1])
    rcopy(u_rows(jp[2]), u_rows(jp[2]), us.at[0], ur.at[0], {'m2': jp[2]}).wait_recv()
    u_fwd = rcopy(u_rows(jp[2]), u_rows(jp[2]), us.at[2], ur.at[2], {'m2': jp[1]})
    u_fwd.start()
    rcopy(u_rows(jp[1]), u_rows(jp[1]), us.at[1], ur.at[1], {'m2': jp[1]}).wait_recv()
    rcopy(u_rows(jp[3]), u_rows(jp[3]), us.at[2], ur.at[2], {'m2': jp[1]}).wait_recv()

    def lhs_in(m, slot):
        return pltpu.make_async_copy(u.at[rows_at(m * block, block), :], lhs.at[slot], lhs_sem.at[slot])

    def product1(b, own, store):
        for e in (1, 2, 3):
            f1_in(b, e).wait_recv()
        loads = [pltpu.make_async_copy(own, rhs.at[rows_at(i * dim, dim), :], rhs_sem.at[0])]
        for e in (1, 2, 3):
            at = rows_at(ip[e] * dim, dim)
            loads.append(pltpu.make_async_copy(w1.at[b, at, :], rhs.at[at, :], rhs_sem.at[e]))
        for load in loads:
            load.start()
        lhs_in(0, 0).start()
        for load in loads:
            load.wait()

        @pl.loop(0, tokens // block)
        def _(m):
            slot = lax.rem(m, 2)
            lhs_in(m, slot).wait()

            @pl.when(m + 1 < tokens // block)
            def _():
                lhs_in(m + 1, 1 - slot).start()
            store(rows_at(m * block, block), dot(lhs[slot], rhs[...]))

    @pl.loop(0, 3)
    def _(b):
        def store(at, value):
            zq[b, at, :] = value.astype(jnp.bfloat16)
        product1(b, wq.at[b, :, ds(i * qw, qw)], store)

    forward1(4)
    issue2(cuts[1], cuts[2])

    @pl.loop(0, batch)
    def _(n):
        at = rows_at(n * patches, patches)
        for head in range(heads):
            cols = slice(head * LANES, (head + 1) * LANES)
            query = head_norm(zq[0, at, cols].astype(jnp.float32), qns[...])
            key = head_norm(zq[1, at, cols].astype(jnp.float32), kns[...])
            scores = lax.dot_general(query, key, (((1,), (1,)), ((), ())), preferred_element_type=jnp.float32) * LANES ** -0.5
            scores = jnp.exp(scores - jnp.max(scores, axis=-1, keepdims=True))
            probs = (scores / jnp.sum(scores, axis=-1, keepdims=True)).astype(jnp.bfloat16)
            h[at, cols] = dot(probs, zq[2, at, cols]).astype(jnp.bfloat16)

    forward1(5)
    issue2(cuts[2], cuts[3])

    @pl.loop(0, nub)
    def _(b):
        def store(at, value):
            value = value.astype(jnp.bfloat16).astype(jnp.float32) + bu[:, ds(i * uw + b * qw, qw)]
            value = 0.5 * value * (1.0 + lax.erf(value * 2.0 ** -0.5))
            h[at, ds(qw + b * qw, qw)] = value.astype(jnp.bfloat16)
        product1(b + 3, wu.at[:, ds(i * uw + b * qw, qw)], store)

        @pl.when(b == 1)
        def _():
            forward1(6)
            issue2(cuts[3], cuts[4])

    def quarter(yy, core):
        return (2 * yy + core) * rows

    def send_a(c, yy):
        return rcopy(pa.at[lax.rem(c, 2), yy], ra.at[c, yy], as_.at[c, yy], ar.at[c, yy], {'m2': jp[1]})

    def send_b(c):
        return rcopy(ss.at[lax.rem(c, 2)], rb.at[c], bs.at[c], br.at[c], {'m2': jp[2]})

    def send_c(c, k):
        src = rb.at[c, :, ds(ip[1 + 2 * k] * LANES, LANES)]
        return rcopy(src, rc.at[c, k], cs.at[c, k], cr.at[c, k], {'m1': ip[1]})

    def send_d(c):
        return rcopy(ud.at[c], rd.at[c], dsm.at[c], drm.at[c], {'m1': ip[2]})

    def out_part(c, q):
        return out.at[rows_at(q * rows, rows), ds(c * LANES, LANES)]

    def send_e(c, e):
        return rcopy(fin.at[c], out_part(c, j), es.at[c, e - 1], er.at[c, e - 1], {'m2': jp[e]})

    def out_own(c):
        return pltpu.make_async_copy(fin.at[c], out_part(c, j), fin_sem.at[c])

    forward2(0)

    @pl.loop(0, nc + 2)
    def _(c):
        @pl.when(c + 1 < nc)
        def _():
            forward2(c + 1)

        @pl.when(c < nc)
        def _():
            slot = lax.rem(c, 2)
            for e, kind in pieces2:
                f2_in(c, e, kind).wait_recv()
            cols = ds(i * LANES, LANES)
            loads = [pltpu.make_async_copy(wo.at[rows_at(i * qw, qw), ds(c * LANES, LANES)], w2b.at[slot, 0:qw, cols], w2b_sem.at[0]),
                     pltpu.make_async_copy(wd.at[rows_at(i * uw, uw), ds(c * LANES, LANES)], w2b.at[slot, qw:qw + uw, cols], w2b_sem.at[4])]
            for e in (1, 2, 3):
                cols = ds(ip[e] * LANES, LANES)
                loads.append(pltpu.make_async_copy(w2.at[c, :, cols], w2b.at[slot, :, cols], w2b_sem.at[e]))
            for load in loads:
                load.start()

            @pl.when(c >= 2)
            def _():
                for yy in range(2):
                    send_a(c - 2, yy).wait_send()
            for load in loads:
                load.wait()
            for yy in range(2):
                for sub in range(2):
                    at = rows_at(quarter(yy, 1 - jc) + sub * block, block)
                    pa[slot, yy, sub * block:(sub + 1) * block, :] = dot(h[at, :], w2b[slot]).astype(jnp.bfloat16)
                send_a(c, yy).start()
            keep = lax.rem(c, 3)
            for yy in range(2):
                for sub in range(2):
                    at = rows_at(quarter(yy, jc) + sub * block, block)
                    po[keep, yy, sub * block:(sub + 1) * block, :] = dot(h[at, :], w2b[slot]).astype(jnp.bfloat16)

        @pl.when((c >= 1) & (c <= nc))
        def _():
            d = c - 1
            keep = lax.rem(d, 3)
            for yy in range(2):
                part = ra.at[d, yy]
                rcopy(part, part, as_.at[d, yy], ar.at[d, yy], {'m2': jp[1]}).wait_recv()
            load = pltpu.make_async_copy(ra.at[d], rav, rav_sem.at[0])
            load.start()

            @pl.when(d >= 2)
            def _():
                send_b(d - 2).wait_send()
            load.wait()
            ss[lax.rem(d, 2)] = (po[keep, 1 - jy].astype(jnp.float32) + rav[1 - jy].astype(jnp.float32)).astype(jnp.bfloat16)
            send_b(d).start()
            po[keep, jy] = (po[keep, jy].astype(jnp.float32) + rav[jy].astype(jnp.float32)).astype(jnp.bfloat16)

        @pl.when(c >= 2)
        def _():
            d = c - 2
            rcopy(rb.at[d], rb.at[d], bs.at[d], br.at[d], {'m2': jp[2]}).wait_recv()
            rb[d] = (po[lax.rem(d, 3), jy].astype(jnp.float32) + rb[d].astype(jnp.float32)).astype(jnp.bfloat16)
            for k in range(2):
                send_c(d, k).start()

    @pl.loop(0, nc + LAG)
    def _(c):
        @pl.when(c < nc)
        def _():
            for k in range(2):
                rcopy(rc.at[c, k], rc.at[c, k], cs.at[c, k], cr.at[c, k], {'m1': ip[1]}).wait_recv()
            far = rb[c, :, ds(ip[2] * LANES, LANES)].astype(jnp.float32) + rc[c, 1].astype(jnp.float32)
            ud[c] = far.astype(jnp.bfloat16)
            send_d(c).start()

        @pl.when(c >= LAG)
        def _():
            d = c - LAG
            rcopy(rd.at[d], rd.at[d], dsm.at[d], drm.at[d], {'m1': ip[2]}).wait_recv()
            cols = ds(d * LANES, LANES)
            value = rb[d, :, ds(i * LANES, LANES)].astype(jnp.float32) + rc[d, 0].astype(jnp.float32) + rd[d].astype(jnp.float32)
            value = xg[i, :, cols].astype(jnp.float32) + value + bo[:, cols]
            fin[d] = value.astype(jnp.bfloat16)
            for e in (2, 3, 1):
                send_e(d, e).start()
            out_own(d).start()

    for copy in (x_far, x_near, x_fwd, u_far, u_near, u_fwd):
        copy.wait_send()
    for b in range(3 + nub):
        for e in (2, 3, 1):
            z1(b, e).wait_send()
            f1(b, e).wait_send()

    @pl.loop(0, nc)
    def _(c):
        for e, kind in pieces2:
            z2(c, e, kind).wait_send()
            f2(c, e, kind).wait_send()
        for k in range(2):
            send_c(c, k).wait_send()
        send_d(c).wait_send()
        out_own(c).wait()
        for e in (1, 2, 3):
            send_e(c, e).wait_send()
            part = out_part(c, jp[e])
            rcopy(part, part, es.at[c, e - 1], er.at[c, e - 1], {'m2': jp[e]}).wait_recv()

        @pl.when(c >= nc - 2)
        def _():
            for yy in range(2):
                send_a(c, yy).wait_send()
            send_b(c).wait_send()


def solution(mesh):
    assert mesh.shape['m1'] == 4 and mesh.shape['m2'] == 4 and mesh.shape['dp'] == 2

    def local_layer(x_blk, ln_scale, qn_scale, kn_scale, w_qkv, w_up, b_up, w_o, w_down, b_out):
        batch, patches, dim = x_blk.shape
        tokens = batch * patches
        qw, uw = w_qkv.shape[2] // 4, w_up.shape[1] // 4
        rows, block, nc, nb = tokens // 4, tokens // 8, dim // LANES, 3 + uw // qw
        assert qn_scale.shape[0] == LANES and uw % qw == 0 and nb == 7
        wide = 4 * LANES
        bf16 = jnp.bfloat16
        dma = pltpu.SemaphoreType.DMA
        hbm = pl.BlockSpec(memory_space=pltpu.HBM)
        vmem = pl.BlockSpec(memory_space=pltpu.VMEM)
        ln_rows = min(64, rows)
        out = pl.pallas_call(
            functools.partial(kernel, (batch, patches, dim, qw, uw)),
            out_shape=[
                jax.ShapeDtypeStruct((tokens, dim), bf16),
                jax.ShapeDtypeStruct((tokens, 4 * dim), bf16),
                jax.ShapeDtypeStruct((nb, 4 * dim, qw), bf16),
                jax.ShapeDtypeStruct((nc, qw + uw, wide), bf16),
                jax.ShapeDtypeStruct((nc, 2, rows, wide), bf16)],
            in_specs=[hbm, vmem, vmem, vmem, hbm, hbm, vmem, hbm, hbm, vmem],
            out_specs=[hbm] * 5,
            scratch_shapes=[
                pltpu.VMEM((4, rows, dim), bf16),
                pltpu.VMEM((2, ln_rows, 4 * dim), bf16),
                pltpu.VMEM((3, tokens, qw), bf16),
                pltpu.VMEM((tokens, qw + uw), bf16),
                pltpu.VMEM((4 * dim, qw), bf16),
                pltpu.VMEM((2, block, 4 * dim), bf16),
                pltpu.VMEM((2, qw + uw, wide), bf16),
                pltpu.VMEM((2, 2, rows, wide), bf16),
                pltpu.VMEM((3, 2, rows, wide), bf16),
                pltpu.VMEM((2, rows, wide), bf16),
                pltpu.VMEM((2, rows, wide), bf16),
                pltpu.VMEM((nc, rows, wide), bf16),
                pltpu.VMEM((nc, 2, rows, LANES), bf16),
                pltpu.VMEM((nc, rows, LANES), bf16),
                pltpu.VMEM((nc, rows, LANES), bf16),
                pltpu.VMEM((nc, rows, LANES), bf16),
                dma((3,)), dma((3,)),
                dma((nb, 3)), dma((nb, 3)), dma((nb, 3)), dma((nb, 3)),
                dma((3,)), dma((3,)),
                dma((nc, 3, 2)), dma((nc, 3, 2)), dma((nc, 3, 2)), dma((nc, 3, 2)),
                dma((nc, 2)), dma((nc, 2)), dma((nc,)), dma((nc,)), dma((nc, 2)), dma((nc, 2)), dma((nc,)), dma((nc,)),
                dma((nc, 3)), dma((nc, 3)),
                dma((1,)), dma((4,)), dma((2,)), dma((2,)), dma((5,)), dma((1,)), dma((nc,))],
            compiler_params=pltpu.CompilerParams(collective_id=0, has_side_effects=True, vmem_limit_bytes=67_043_328),
            name='layer',
        )(x_blk.reshape(tokens, dim), ln_scale[None], qn_scale[None], kn_scale[None], w_qkv.transpose(1, 0, 2), w_up,
          b_up_all(b_up), w_o, w_down, b_out[None])[0]
        return out.reshape(batch, patches, dim)

    def b_up_all(b_up):
        return b_up[None]

    return jax.shard_map(local_layer, mesh=mesh, in_specs=(P('dp', None, 'm1'), P(), P(), P(), P('m1', None, 'm2'), P('m1', 'm2'), P('m2'), P('m2', 'm1'), P('m2', 'm1'), P('m1')), out_specs=P('dp', None, 'm1'), check_vma=False)
```

```python
import functools

import jax
import jax.numpy as jnp
from jax import lax
from jax.experimental import pallas as pl
from jax.experimental.pallas import tpu as pltpu
from jax.sharding import PartitionSpec as P

LN_EPS = 1e-6
MESH = pl.DeviceIdType.MESH
LANES = 128
LAG = 5
AHEAD = 4


def xors(value):
    return (value, value + 1 - 2 * lax.rem(value, 2), value + 2 - 4 * lax.div(value, 2), 3 - value)


def ds(start, size):
    return pl.ds(pl.multiple_of(start, size if size < LANES else LANES), size)


def rows_at(start, size):
    return pl.ds(pl.multiple_of(start, 8), size)


def rcopy(src, dst, send_sem, recv_sem, device):
    return pltpu.make_async_remote_copy(src_ref=src, dst_ref=dst, send_sem=send_sem, recv_sem=recv_sem, device_id=device, device_id_type=MESH)


def dot(lhs, rhs):
    return jnp.dot(lhs, rhs, preferred_element_type=jnp.float32)


def head_norm(values, scale):
    mean = jnp.mean(values, axis=-1, keepdims=True)
    centered = values - mean
    variance = jnp.mean(centered * centered, axis=-1, keepdims=True)
    return (centered * lax.rsqrt(variance + LN_EPS) * scale).astype(jnp.bfloat16)


def kernel(sizes, x, lns, qns, kns, wq, wu, bu, wo, wd, bo,
           out, u, w1, w2, ra,
           xg, ubl, zq, h, rhs, lhs, w2b, pa, po, rav, ss, rb, rc, ud, rd, fin,
           xs, xr, w1s, w1r, f1s, f1r, us, ur, w2s, w2r, f2s, f2r,
           as_, ar, bs, br, cs, cr, dsm, drm, es, er, own_sem, rhs_sem, lhs_sem, ub_sem, w2b_sem, rav_sem, fin_sem):
    batch, patches, dim, qw, uw = sizes
    tokens = batch * patches
    rows = tokens // 4
    block = rows // 2
    half = dim // 2
    total = 4 * dim
    nub = uw // qw
    nc = dim // LANES
    wide = 4 * LANES
    heads = qw // LANES
    ln_rows = min(64, rows)

    g, i, j = lax.axis_index('dp'), lax.axis_index('m1'), lax.axis_index('m2')
    ip, jp = xors(i), xors(j)
    jy, jc = lax.div(j, 2), lax.rem(j, 2)

    barrier = pltpu.get_barrier_semaphore()
    peers = [{'m1': ip[e]} for e in (1, 2, 3)] + [{'m2': jp[e]} for e in (1, 2, 3)] + [{'dp': 1 - g}]
    for peer in peers:
        pl.semaphore_signal(barrier, inc=1, device_id=peer, device_id_type=MESH)
    with jax.named_scope('barrier'):
        pl.semaphore_wait(barrier, len(peers))

    mine = rows_at(j * rows, rows)
    x_far = rcopy(x.at[mine, :], xg.at[i], xs.at[0], xr.at[0], {'m1': ip[2]})
    x_near = rcopy(x.at[mine, :], xg.at[i], xs.at[1], xr.at[1], {'m1': ip[1]})
    x_own = pltpu.make_async_copy(x.at[mine, :], xg.at[i], own_sem.at[0])
    x_far.start()
    x_near.start()
    x_own.start()
    x_far_in = rcopy(xg.at[ip[2]], xg.at[ip[2]], xs.at[0], xr.at[0], {'m1': ip[2]})
    with jax.named_scope('w_xfar'):
        x_far_in.wait_recv()
    x_fwd = rcopy(xg.at[ip[2]], xg.at[ip[2]], xs.at[2], xr.at[2], {'m1': ip[1]})
    x_fwd.start()

    def z1(b, e):
        t = ip[e]
        if b < 3:
            src = wq.at[b, rows_at(g * half, half), ds(t * qw, qw)]
        else:
            src = wu.at[rows_at(g * half, half), ds(t * uw + (b - 3) * qw, qw)]
        return rcopy(src, w1.at[b, rows_at(i * dim + g * half, half), :], w1s.at[b, e - 1], w1r.at[b, e - 1], {'m1': t})

    def f1(b, e):
        part = w1.at[b, rows_at(ip[e] * dim + g * half, half), :]
        return rcopy(part, part, f1s.at[b, e - 1], f1r.at[b, e - 1], {'dp': 1 - g})

    def z1_in(b, e):
        part = w1.at[b, rows_at(ip[e] * dim + g * half, half), :]
        return rcopy(part, part, w1s.at[b, e - 1], w1r.at[b, e - 1], {'m1': ip[e]})

    def f1_in(b, e):
        part = w1.at[b, rows_at(ip[e] * dim + (1 - g) * half, half), :]
        return rcopy(part, part, f1s.at[b, e - 1], f1r.at[b, e - 1], {'dp': 1 - g})

    def forward1(b):
        for e in (2, 3, 1):
            with jax.named_scope(f'w_z1e{e}'):
                z1_in(b, e).wait_recv()
            f1(b, e).start()

    def issue1(b):
        for e in (2, 3, 1):
            z1(b, e).start()

    issue1(0)
    issue1(1)

    def parts2(c, e, group, kind):
        size, first = (qw // 2, 0) if kind == 0 else (uw // 2, qw)
        return size, first + group * size

    def z2(c, e, kind):
        size, at = parts2(c, e, g, kind)
        t = ip[e]
        src = wo if kind == 0 else wd
        start = t * (2 * size) + g * size
        return rcopy(src.at[rows_at(start, size), ds(c * LANES, LANES)], w2.at[c, rows_at(at, size), ds(i * LANES, LANES)],
                     w2s.at[c, e - 1, kind], w2r.at[c, e - 1, kind], {'m1': t})

    def region2(c, e, group, kind):
        size, at = parts2(c, e, group, kind)
        return w2.at[c, rows_at(at, size), ds(ip[e] * LANES, LANES)]

    def z2_in(c, e, kind):
        part = region2(c, e, g, kind)
        return rcopy(part, part, w2s.at[c, e - 1, kind], w2r.at[c, e - 1, kind], {'m1': ip[e]})

    def f2(c, e, kind):
        part = region2(c, e, g, kind)
        return rcopy(part, part, f2s.at[c, e - 1, kind], f2r.at[c, e - 1, kind], {'dp': 1 - g})

    def f2_in(c, e, kind):
        part = region2(c, e, 1 - g, kind)
        return rcopy(part, part, f2s.at[c, e - 1, kind], f2r.at[c, e - 1, kind], {'dp': 1 - g})

    def next2(c):
        forward2(c)

        @pl.when(c + AHEAD < nc)
        def _():
            issue2(c + AHEAD)

    pieces2 = [(e, kind) for e in (2, 3, 1) for kind in (1, 0)]

    def issue2(c):
        for e, kind in pieces2:
            z2(c, e, kind).start()

    def forward2(c):
        for e, kind in pieces2:
            with jax.named_scope(f'w_z2e{e}k{kind}'):
                z2_in(c, e, kind).wait_recv()
            f2(c, e, kind).start()

    with jax.named_scope('w_xown'):
        x_own.wait()
    with jax.named_scope('w_xnear'):
        rcopy(xg.at[ip[1]], xg.at[ip[1]], xs.at[1], xr.at[1], {'m1': ip[1]}).wait_recv()
    with jax.named_scope('w_xfwd'):
        rcopy(xg.at[ip[3]], xg.at[ip[3]], xs.at[2], xr.at[2], {'m1': ip[1]}).wait_recv()

    def u_out(r, slot):
        return pltpu.make_async_copy(ubl.at[slot], u.at[rows_at(j * rows + r * ln_rows, ln_rows), :], ub_sem.at[slot])

    @pl.loop(0, rows // ln_rows)
    def _(r):
        slot = lax.rem(r, 2)

        @pl.when(r >= 2)
        def _():
            u_out(r - 2, slot).wait()
        at = rows_at(r * ln_rows, ln_rows)
        parts = [xg[s, at, :].astype(jnp.float32) for s in range(4)]
        mean = sum(jnp.sum(part, axis=-1, keepdims=True) for part in parts) / total
        parts = [part - mean for part in parts]
        variance = sum(jnp.sum(part * part, axis=-1, keepdims=True) for part in parts) / total
        inverse = lax.rsqrt(variance + LN_EPS)
        for s in range(4):
            cols = slice(s * dim, (s + 1) * dim)
            ubl[slot, :, cols] = (parts[s] * inverse * lns[:, cols]).astype(jnp.bfloat16)
        u_out(r, slot).start()

    for r in range(max(0, rows // ln_rows - 2), rows // ln_rows):
        u_out(r, r % 2).wait()

    def u_rows(q):
        return u.at[rows_at(q * rows, rows), :]

    u_far = rcopy(u_rows(j), u_rows(j), us.at[0], ur.at[0], {'m2': jp[2]})
    u_near = rcopy(u_rows(j), u_rows(j), us.at[1], ur.at[1], {'m2': jp[1]})
    u_far.start()
    u_near.start()
    for b in range(4):
        forward1(b)
        issue1(b + 2)
    with jax.named_scope('w_ufar'):
        rcopy(u_rows(jp[2]), u_rows(jp[2]), us.at[0], ur.at[0], {'m2': jp[2]}).wait_recv()
    u_fwd = rcopy(u_rows(jp[2]), u_rows(jp[2]), us.at[2], ur.at[2], {'m2': jp[1]})
    u_fwd.start()
    rcopy(u_rows(jp[1]), u_rows(jp[1]), us.at[1], ur.at[1], {'m2': jp[1]}).wait_recv()
    with jax.named_scope('w_ufwd'):
        rcopy(u_rows(jp[3]), u_rows(jp[3]), us.at[2], ur.at[2], {'m2': jp[1]}).wait_recv()

    def lhs_in(m, slot):
        return pltpu.make_async_copy(u.at[rows_at(m * block, block), :], lhs.at[slot], lhs_sem.at[slot])

    def product1(b, own, store):
        with jax.named_scope('w_f1'):
            for e in (1, 2, 3):
                f1_in(b, e).wait_recv()
        loads = [pltpu.make_async_copy(own, rhs.at[rows_at(i * dim, dim), :], rhs_sem.at[0])]
        for e in (1, 2, 3):
            at = rows_at(ip[e] * dim, dim)
            loads.append(pltpu.make_async_copy(w1.at[b, at, :], rhs.at[at, :], rhs_sem.at[e]))
        for load in loads:
            load.start()
        lhs_in(0, 0).start()
        for load in loads:
            load.wait()

        @pl.loop(0, tokens // block)
        def _(m):
            slot = lax.rem(m, 2)
            lhs_in(m, slot).wait()

            @pl.when(m + 1 < tokens // block)
            def _():
                lhs_in(m + 1, 1 - slot).start()
            with jax.named_scope('mm1'):
                store(rows_at(m * block, block), dot(lhs[slot], rhs[...]))

    @pl.loop(0, 3)
    def _(b):
        def store(at, value):
            zq[b, at, :] = value.astype(jnp.bfloat16)
        product1(b, wq.at[b, :, ds(i * qw, qw)], store)

        @pl.when(b == 1)
        def _():
            forward1(4)
            issue1(6)

    @pl.loop(0, batch)
    def _(n):
        at = rows_at(n * patches, patches)
        for head in range(heads):
            cols = slice(head * LANES, (head + 1) * LANES)
            query = head_norm(zq[0, at, cols].astype(jnp.float32), qns[...])
            key = head_norm(zq[1, at, cols].astype(jnp.float32), kns[...])
            scores = lax.dot_general(query, key, (((1,), (1,)), ((), ())), preferred_element_type=jnp.float32) * LANES ** -0.5
            scores = jnp.exp(scores - jnp.max(scores, axis=-1, keepdims=True))
            probs = (scores / jnp.sum(scores, axis=-1, keepdims=True)).astype(jnp.bfloat16)
            with jax.named_scope('attn'):
                h[at, cols] = dot(probs, zq[2, at, cols]).astype(jnp.bfloat16)

    forward1(5)
    for c in range(AHEAD // 2):
        issue2(c)

    @pl.loop(0, nub)
    def _(b):
        def store(at, value):
            value = value.astype(jnp.bfloat16).astype(jnp.float32) + bu[:, ds(i * uw + b * qw, qw)]
            value = 0.5 * value * (1.0 + lax.erf(value * 2.0 ** -0.5))
            h[at, ds(qw + b * qw, qw)] = value.astype(jnp.bfloat16)
        product1(b + 3, wu.at[:, ds(i * uw + b * qw, qw)], store)

        @pl.when(b == 1)
        def _():
            forward1(6)
            for c in range(AHEAD // 2, AHEAD):
                issue2(c)

        @pl.when(b == 2)
        def _():
            next2(0)

        @pl.when(b == 3)
        def _():
            next2(1)

    def quarter(yy, core):
        return (2 * yy + core) * rows

    def send_a(c, yy):
        return rcopy(pa.at[lax.rem(c, 2), yy], ra.at[c, yy], as_.at[c, yy], ar.at[c, yy], {'m2': jp[1]})

    def send_b(c):
        return rcopy(ss.at[lax.rem(c, 2)], rb.at[c], bs.at[c], br.at[c], {'m2': jp[2]})

    def send_c(c, k):
        src = rb.at[c, :, ds(ip[1 + 2 * k] * LANES, LANES)]
        return rcopy(src, rc.at[c, k], cs.at[c, k], cr.at[c, k], {'m1': ip[1]})

    def send_d(c):
        return rcopy(ud.at[c], rd.at[c], dsm.at[c], drm.at[c], {'m1': ip[2]})

    def out_part(c, q):
        return out.at[rows_at(q * rows, rows), ds(c * LANES, LANES)]

    def send_e(c, e):
        return rcopy(fin.at[c], out_part(c, j), es.at[c, e - 1], er.at[c, e - 1], {'m2': jp[e]})

    def out_own(c):
        return pltpu.make_async_copy(fin.at[c], out_part(c, j), fin_sem.at[c])

    @pl.loop(0, nc + 2 + 2 * LAG)
    def _(c):
        @pl.when((c >= 1) & (c + 1 < nc))
        def _():
            next2(c + 1)

        @pl.when(c < nc)
        def _():
            slot = lax.rem(c, 2)
            with jax.named_scope('w_f2'):
                for e, kind in pieces2:
                    f2_in(c, e, kind).wait_recv()
            cols = ds(i * LANES, LANES)
            loads = [pltpu.make_async_copy(wo.at[rows_at(i * qw, qw), ds(c * LANES, LANES)], w2b.at[slot, 0:qw, cols], w2b_sem.at[0]),
                     pltpu.make_async_copy(wd.at[rows_at(i * uw, uw), ds(c * LANES, LANES)], w2b.at[slot, qw:qw + uw, cols], w2b_sem.at[4])]
            for e in (1, 2, 3):
                cols = ds(ip[e] * LANES, LANES)
                loads.append(pltpu.make_async_copy(w2.at[c, :, cols], w2b.at[slot, :, cols], w2b_sem.at[e]))
            for load in loads:
                load.start()

            @pl.when(c >= 2)
            def _():
                for yy in range(2):
                    send_a(c - 2, yy).wait_send()
            with jax.named_scope('w_w2b'):
                for load in loads:
                    load.wait()
            for yy in range(2):
                for sub in range(2):
                    at = rows_at(quarter(yy, 1 - jc) + sub * block, block)
                    pa[slot, yy, sub * block:(sub + 1) * block, :] = dot(h[at, :], w2b[slot]).astype(jnp.bfloat16)
                send_a(c, yy).start()
            keep = lax.rem(c, 3)
            for yy in range(2):
                for sub in range(2):
                    at = rows_at(quarter(yy, jc) + sub * block, block)
                    po[keep, yy, sub * block:(sub + 1) * block, :] = dot(h[at, :], w2b[slot]).astype(jnp.bfloat16)

        @pl.when((c >= 1) & (c <= nc))
        def _():
            d = c - 1
            keep = lax.rem(d, 3)
            for yy in range(2):
                part = ra.at[d, yy]
                with jax.named_scope('w_a'):
                  rcopy(part, part, as_.at[d, yy], ar.at[d, yy], {'m2': jp[1]}).wait_recv()
            load = pltpu.make_async_copy(ra.at[d], rav, rav_sem.at[0])
            load.start()

            @pl.when(d >= 2)
            def _():
                send_b(d - 2).wait_send()
            load.wait()
            ss[lax.rem(d, 2)] = (po[keep, 1 - jy].astype(jnp.float32) + rav[1 - jy].astype(jnp.float32)).astype(jnp.bfloat16)
            send_b(d).start()
            po[keep, jy] = (po[keep, jy].astype(jnp.float32) + rav[jy].astype(jnp.float32)).astype(jnp.bfloat16)

        @pl.when((c >= 2) & (c < nc + 2))
        def _():
            d = c - 2
            with jax.named_scope('w_b'):
              rcopy(rb.at[d], rb.at[d], bs.at[d], br.at[d], {'m2': jp[2]}).wait_recv()
            rb[d] = (po[lax.rem(d, 3), jy].astype(jnp.float32) + rb[d].astype(jnp.float32)).astype(jnp.bfloat16)
            for k in range(2):
                send_c(d, k).start()

        @pl.when((c >= 2 + LAG) & (c < nc + 2 + LAG))
        def _():
            d = c - 2 - LAG
            for k in range(2):
                with jax.named_scope('w_c'):
                  rcopy(rc.at[d, k], rc.at[d, k], cs.at[d, k], cr.at[d, k], {'m1': ip[1]}).wait_recv()
            far = rb[d, :, ds(ip[2] * LANES, LANES)].astype(jnp.float32) + rc[d, 1].astype(jnp.float32)
            ud[d] = far.astype(jnp.bfloat16)
            send_d(d).start()

        @pl.when(c >= 2 + 2 * LAG)
        def _():
            d = c - 2 - 2 * LAG
            with jax.named_scope('w_d'):
              rcopy(rd.at[d], rd.at[d], dsm.at[d], drm.at[d], {'m1': ip[2]}).wait_recv()
            cols = ds(d * LANES, LANES)
            value = rb[d, :, ds(i * LANES, LANES)].astype(jnp.float32) + rc[d, 0].astype(jnp.float32) + rd[d].astype(jnp.float32)
            value = xg[i, :, cols].astype(jnp.float32) + value + bo[:, cols]
            fin[d] = value.astype(jnp.bfloat16)
            for e in (2, 3, 1):
                send_e(d, e).start()
            out_own(d).start()

    with jax.named_scope('drain0'):
      for copy in (x_far, x_near, x_fwd, u_far, u_near, u_fwd):
        copy.wait_send()
    for b in range(3 + nub):
        for e in (2, 3, 1):
            z1(b, e).wait_send()
            f1(b, e).wait_send()

    @pl.loop(0, nc)
    def _(c):
        with jax.named_scope('drain_z2'):
          for e, kind in pieces2:
            z2(c, e, kind).wait_send()
            f2(c, e, kind).wait_send()
        for k in range(2):
            send_c(c, k).wait_send()
        send_d(c).wait_send()
        out_own(c).wait()
        for e in (1, 2, 3):
            send_e(c, e).wait_send()
            part = out_part(c, jp[e])
            with jax.named_scope('w_e'):
              rcopy(part, part, es.at[c, e - 1], er.at[c, e - 1], {'m2': jp[e]}).wait_recv()

        @pl.when(c >= nc - 2)
        def _():
            for yy in range(2):
                send_a(c, yy).wait_send()
            send_b(c).wait_send()


def solution(mesh):
    assert mesh.shape['m1'] == 4 and mesh.shape['m2'] == 4 and mesh.shape['dp'] == 2

    def local_layer(x_blk, ln_scale, qn_scale, kn_scale, w_qkv, w_up, b_up, w_o, w_down, b_out):
        batch, patches, dim = x_blk.shape
        tokens = batch * patches
        qw, uw = w_qkv.shape[2] // 4, w_up.shape[1] // 4
        rows, block, nc, nb = tokens // 4, tokens // 8, dim // LANES, 3 + uw // qw
        assert qn_scale.shape[0] == LANES and uw % qw == 0 and nb == 7
        wide = 4 * LANES
        bf16 = jnp.bfloat16
        dma = pltpu.SemaphoreType.DMA
        hbm = pl.BlockSpec(memory_space=pltpu.HBM)
        vmem = pl.BlockSpec(memory_space=pltpu.VMEM)
        ln_rows = min(64, rows)
        out = pl.pallas_call(
            functools.partial(kernel, (batch, patches, dim, qw, uw)),
            out_shape=[
                jax.ShapeDtypeStruct((tokens, dim), bf16),
                jax.ShapeDtypeStruct((tokens, 4 * dim), bf16),
                jax.ShapeDtypeStruct((nb, 4 * dim, qw), bf16),
                jax.ShapeDtypeStruct((nc, qw + uw, wide), bf16),
                jax.ShapeDtypeStruct((nc, 2, rows, wide), bf16)],
            in_specs=[hbm, vmem, vmem, vmem, hbm, hbm, vmem, hbm, hbm, vmem],
            out_specs=[hbm] * 5,
            scratch_shapes=[
                pltpu.VMEM((4, rows, dim), bf16),
                pltpu.VMEM((2, ln_rows, 4 * dim), bf16),
                pltpu.VMEM((3, tokens, qw), bf16),
                pltpu.VMEM((tokens, qw + uw), bf16),
                pltpu.VMEM((4 * dim, qw), bf16),
                pltpu.VMEM((2, block, 4 * dim), bf16),
                pltpu.VMEM((2, qw + uw, wide), bf16),
                pltpu.VMEM((2, 2, rows, wide), bf16),
                pltpu.VMEM((3, 2, rows, wide), bf16),
                pltpu.VMEM((2, rows, wide), bf16),
                pltpu.VMEM((2, rows, wide), bf16),
                pltpu.VMEM((nc, rows, wide), bf16),
                pltpu.VMEM((nc, 2, rows, LANES), bf16),
                pltpu.VMEM((nc, rows, LANES), bf16),
                pltpu.VMEM((nc, rows, LANES), bf16),
                pltpu.VMEM((nc, rows, LANES), bf16),
                dma((3,)), dma((3,)),
                dma((nb, 3)), dma((nb, 3)), dma((nb, 3)), dma((nb, 3)),
                dma((3,)), dma((3,)),
                dma((nc, 3, 2)), dma((nc, 3, 2)), dma((nc, 3, 2)), dma((nc, 3, 2)),
                dma((nc, 2)), dma((nc, 2)), dma((nc,)), dma((nc,)), dma((nc, 2)), dma((nc, 2)), dma((nc,)), dma((nc,)),
                dma((nc, 3)), dma((nc, 3)),
                dma((1,)), dma((4,)), dma((2,)), dma((2,)), dma((5,)), dma((1,)), dma((nc,))],
            compiler_params=pltpu.CompilerParams(collective_id=0, has_side_effects=True, vmem_limit_bytes=67_043_328),
            name='layer',
        )(x_blk.reshape(tokens, dim), ln_scale[None], qn_scale[None], kn_scale[None], w_qkv.transpose(1, 0, 2), w_up,
          b_up[None], w_o, w_down, b_out[None])[0]
        return out.reshape(batch, patches, dim)

    return jax.shard_map(local_layer, mesh=mesh, in_specs=(P('dp', None, 'm1'), P(), P(), P(), P('m1', None, 'm2'), P('m1', 'm2'), P('m2'), P('m2', 'm1'), P('m2', 'm1'), P('m1')), out_specs=P('dp', None, 'm1'), check_vma=False)
```

```python
import functools

import jax
import jax.numpy as jnp
from jax import lax
from jax.experimental import pallas as pl
from jax.experimental.pallas import tpu as pltpu
from jax.sharding import PartitionSpec as P

LN_EPS = 1e-6
MESH = pl.DeviceIdType.MESH
LANES = 128
LAG = 3
AHEAD = 2


def xors(value):
    return (value, value + 1 - 2 * lax.rem(value, 2), value + 2 - 4 * lax.div(value, 2), 3 - value)


def ds(start, size):
    return pl.ds(pl.multiple_of(start, size if size < LANES else LANES), size)


def rows_at(start, size):
    return pl.ds(pl.multiple_of(start, 8), size)


def rcopy(src, dst, send_sem, recv_sem, device):
    return pltpu.make_async_remote_copy(src_ref=src, dst_ref=dst, send_sem=send_sem, recv_sem=recv_sem, device_id=device, device_id_type=MESH)


def dot(lhs, rhs):
    return jnp.dot(lhs, rhs, preferred_element_type=jnp.float32)


def head_norm(values, scale):
    mean = jnp.mean(values, axis=-1, keepdims=True)
    centered = values - mean
    variance = jnp.mean(centered * centered, axis=-1, keepdims=True)
    return (centered * lax.rsqrt(variance + LN_EPS) * scale).astype(jnp.bfloat16)


def kernel(sizes, x, lns, qns, kns, wq, wu, bu, wo, wd, bo,
           out, u, w1, w2, ra,
           xg, ubl, zq, h, rhs, lhs, w2b, pa, po, rav, ss, rb, rc, ud, rd, fin,
           xs, xr, w1s, w1r, f1s, f1r, us, ur, w2s, w2r, f2s, f2r,
           as_, ar, bs, br, cs, cr, dsm, drm, es, er, own_sem, rhs_sem, lhs_sem, ub_sem, w2b_sem, rav_sem, fin_sem):
    batch, patches, dim, qw, uw = sizes
    tokens = batch * patches
    rows = tokens // 4
    block = rows // 2
    half = dim // 2
    total = 4 * dim
    nub = uw // qw
    nc = dim // LANES
    wide = 4 * LANES
    heads = qw // LANES
    ln_rows = min(64, rows)

    g, i, j = lax.axis_index('dp'), lax.axis_index('m1'), lax.axis_index('m2')
    ip, jp = xors(i), xors(j)
    jy, jc = lax.div(j, 2), lax.rem(j, 2)

    barrier = pltpu.get_barrier_semaphore()
    peers = [{'m1': ip[e]} for e in (1, 2, 3)] + [{'m2': jp[e]} for e in (1, 2, 3)] + [{'dp': 1 - g}]
    for peer in peers:
        pl.semaphore_signal(barrier, inc=1, device_id=peer, device_id_type=MESH)
    with jax.named_scope('barrier'):
        pl.semaphore_wait(barrier, len(peers))

    mine = rows_at(j * rows, rows)
    x_far = rcopy(x.at[mine, :], xg.at[i], xs.at[0], xr.at[0], {'m1': ip[2]})
    x_near = rcopy(x.at[mine, :], xg.at[i], xs.at[1], xr.at[1], {'m1': ip[1]})
    x_own = pltpu.make_async_copy(x.at[mine, :], xg.at[i], own_sem.at[0])
    x_far.start()
    x_near.start()
    x_own.start()
    x_far_in = rcopy(xg.at[ip[2]], xg.at[ip[2]], xs.at[0], xr.at[0], {'m1': ip[2]})
    with jax.named_scope('w_xfar'):
        x_far_in.wait_recv()
    x_fwd = rcopy(xg.at[ip[2]], xg.at[ip[2]], xs.at[2], xr.at[2], {'m1': ip[1]})
    x_fwd.start()

    def z1(b, e):
        t = ip[e]
        if b < 3:
            src = wq.at[b, rows_at(g * half, half), ds(t * qw, qw)]
        else:
            src = wu.at[rows_at(g * half, half), ds(t * uw + (b - 3) * qw, qw)]
        return rcopy(src, w1.at[b, rows_at(i * dim + g * half, half), :], w1s.at[b, e - 1], w1r.at[b, e - 1], {'m1': t})

    def f1(b, e):
        part = w1.at[b, rows_at(ip[e] * dim + g * half, half), :]
        return rcopy(part, part, f1s.at[b, e - 1], f1r.at[b, e - 1], {'dp': 1 - g})

    def z1_in(b, e):
        part = w1.at[b, rows_at(ip[e] * dim + g * half, half), :]
        return rcopy(part, part, w1s.at[b, e - 1], w1r.at[b, e - 1], {'m1': ip[e]})

    def f1_in(b, e):
        part = w1.at[b, rows_at(ip[e] * dim + (1 - g) * half, half), :]
        return rcopy(part, part, f1s.at[b, e - 1], f1r.at[b, e - 1], {'dp': 1 - g})

    def forward1(b):
        for e in (2, 3, 1):
            with jax.named_scope(f'w_z1e{e}'):
                z1_in(b, e).wait_recv()
            f1(b, e).start()

    def issue1(b):
        for e in (2, 3, 1):
            z1(b, e).start()

    issue1(0)
    issue1(1)

    def parts2(c, e, group, kind):
        size, first = (qw // 2, 0) if kind == 0 else (uw // 2, qw)
        return size, first + group * size

    def z2(c, e, kind):
        size, at = parts2(c, e, g, kind)
        t = ip[e]
        src = wo if kind == 0 else wd
        start = t * (2 * size) + g * size
        return rcopy(src.at[rows_at(start, size), ds(c * LANES, LANES)], w2.at[c, rows_at(at, size), ds(i * LANES, LANES)],
                     w2s.at[c, e - 1, kind], w2r.at[c, e - 1, kind], {'m1': t})

    def region2(c, e, group, kind):
        size, at = parts2(c, e, group, kind)
        return w2.at[c, rows_at(at, size), ds(ip[e] * LANES, LANES)]

    def z2_in(c, e, kind):
        part = region2(c, e, g, kind)
        return rcopy(part, part, w2s.at[c, e - 1, kind], w2r.at[c, e - 1, kind], {'m1': ip[e]})

    def f2(c, e, kind):
        part = region2(c, e, g, kind)
        return rcopy(part, part, f2s.at[c, e - 1, kind], f2r.at[c, e - 1, kind], {'dp': 1 - g})

    def f2_in(c, e, kind):
        part = region2(c, e, 1 - g, kind)
        return rcopy(part, part, f2s.at[c, e - 1, kind], f2r.at[c, e - 1, kind], {'dp': 1 - g})

    def next2(c):
        forward2(c)

        @pl.when(c + AHEAD < nc)
        def _():
            issue2(c + AHEAD)

    pieces2 = [(e, kind) for e in (2, 3, 1) for kind in (1, 0)]

    def issue2(c):
        for e, kind in pieces2:
            z2(c, e, kind).start()

    def forward2(c):
        for e, kind in pieces2:
            with jax.named_scope(f'w_z2e{e}k{kind}'):
                z2_in(c, e, kind).wait_recv()
            f2(c, e, kind).start()

    with jax.named_scope('w_xown'):
        x_own.wait()
    with jax.named_scope('w_xnear'):
        rcopy(xg.at[ip[1]], xg.at[ip[1]], xs.at[1], xr.at[1], {'m1': ip[1]}).wait_recv()
    with jax.named_scope('w_xfwd'):
        rcopy(xg.at[ip[3]], xg.at[ip[3]], xs.at[2], xr.at[2], {'m1': ip[1]}).wait_recv()

    def u_out(r, slot):
        return pltpu.make_async_copy(ubl.at[slot], u.at[rows_at(j * rows + r * ln_rows, ln_rows), :], ub_sem.at[slot])

    @pl.loop(0, rows // ln_rows)
    def _(r):
        slot = lax.rem(r, 2)

        @pl.when(r >= 2)
        def _():
            u_out(r - 2, slot).wait()
        at = rows_at(r * ln_rows, ln_rows)
        parts = [xg[s, at, :].astype(jnp.float32) for s in range(4)]
        mean = sum(jnp.sum(part, axis=-1, keepdims=True) for part in parts) / total
        parts = [part - mean for part in parts]
        variance = sum(jnp.sum(part * part, axis=-1, keepdims=True) for part in parts) / total
        inverse = lax.rsqrt(variance + LN_EPS)
        for s in range(4):
            cols = slice(s * dim, (s + 1) * dim)
            ubl[slot, :, cols] = (parts[s] * inverse * lns[:, cols]).astype(jnp.bfloat16)
        u_out(r, slot).start()

    for r in range(max(0, rows // ln_rows - 2), rows // ln_rows):
        u_out(r, r % 2).wait()

    def u_rows(q):
        return u.at[rows_at(q * rows, rows), :]

    u_far = rcopy(u_rows(j), u_rows(j), us.at[0], ur.at[0], {'m2': jp[2]})
    u_near = rcopy(u_rows(j), u_rows(j), us.at[1], ur.at[1], {'m2': jp[1]})
    u_far.start()
    u_near.start()
    for b in range(4):
        forward1(b)
        issue1(b + 2)
    with jax.named_scope('w_ufar'):
        rcopy(u_rows(jp[2]), u_rows(jp[2]), us.at[0], ur.at[0], {'m2': jp[2]}).wait_recv()
    u_fwd = rcopy(u_rows(jp[2]), u_rows(jp[2]), us.at[2], ur.at[2], {'m2': jp[1]})
    u_fwd.start()
    rcopy(u_rows(jp[1]), u_rows(jp[1]), us.at[1], ur.at[1], {'m2': jp[1]}).wait_recv()
    with jax.named_scope('w_ufwd'):
        rcopy(u_rows(jp[3]), u_rows(jp[3]), us.at[2], ur.at[2], {'m2': jp[1]}).wait_recv()

    def lhs_in(m, slot):
        return pltpu.make_async_copy(u.at[rows_at(m * block, block), :], lhs.at[slot], lhs_sem.at[slot])

    def product1(b, own, store):
        with jax.named_scope('w_f1'):
            for e in (1, 2, 3):
                f1_in(b, e).wait_recv()
        loads = [pltpu.make_async_copy(own, rhs.at[rows_at(i * dim, dim), :], rhs_sem.at[0])]
        for e in (1, 2, 3):
            at = rows_at(ip[e] * dim, dim)
            loads.append(pltpu.make_async_copy(w1.at[b, at, :], rhs.at[at, :], rhs_sem.at[e]))
        for load in loads:
            load.start()
        lhs_in(0, 0).start()
        for load in loads:
            load.wait()

        @pl.loop(0, tokens // block)
        def _(m):
            slot = lax.rem(m, 2)
            lhs_in(m, slot).wait()

            @pl.when(m + 1 < tokens // block)
            def _():
                lhs_in(m + 1, 1 - slot).start()
            with jax.named_scope('mm1'):
                store(rows_at(m * block, block), dot(lhs[slot], rhs[...]))

    @pl.loop(0, 3)
    def _(b):
        def store(at, value):
            zq[b, at, :] = value.astype(jnp.bfloat16)
        product1(b, wq.at[b, :, ds(i * qw, qw)], store)

        @pl.when(b == 1)
        def _():
            forward1(4)
            issue1(6)

    @pl.loop(0, batch)
    def _(n):
        at = rows_at(n * patches, patches)
        for head in range(heads):
            cols = slice(head * LANES, (head + 1) * LANES)
            query = head_norm(zq[0, at, cols].astype(jnp.float32), qns[...])
            key = head_norm(zq[1, at, cols].astype(jnp.float32), kns[...])
            scores = lax.dot_general(query, key, (((1,), (1,)), ((), ())), preferred_element_type=jnp.float32) * LANES ** -0.5
            scores = jnp.exp(scores - jnp.max(scores, axis=-1, keepdims=True))
            probs = (scores / jnp.sum(scores, axis=-1, keepdims=True)).astype(jnp.bfloat16)
            with jax.named_scope('attn'):
                h[at, cols] = dot(probs, zq[2, at, cols]).astype(jnp.bfloat16)

    forward1(5)
    for c in range(AHEAD // 2):
        issue2(c)

    @pl.loop(0, nub)
    def _(b):
        def store(at, value):
            value = value.astype(jnp.bfloat16).astype(jnp.float32) + bu[:, ds(i * uw + b * qw, qw)]
            value = 0.5 * value * (1.0 + lax.erf(value * 2.0 ** -0.5))
            h[at, ds(qw + b * qw, qw)] = value.astype(jnp.bfloat16)
        product1(b + 3, wu.at[:, ds(i * uw + b * qw, qw)], store)

        @pl.when(b == 1)
        def _():
            forward1(6)
            for c in range(AHEAD // 2, AHEAD):
                issue2(c)

        @pl.when(b == 2)
        def _():
            next2(0)

        @pl.when(b == 3)
        def _():
            next2(1)

    def quarter(yy, core):
        return (2 * yy + core) * rows

    def send_a(c, yy):
        return rcopy(pa.at[lax.rem(c, 2), yy], ra.at[c, yy], as_.at[c, yy], ar.at[c, yy], {'m2': jp[1]})

    def send_b(c):
        return rcopy(ss.at[lax.rem(c, 2)], rb.at[c], bs.at[c], br.at[c], {'m2': jp[2]})

    def send_c(c, k):
        src = rb.at[c, :, ds(ip[1 + 2 * k] * LANES, LANES)]
        return rcopy(src, rc.at[c, k], cs.at[c, k], cr.at[c, k], {'m1': ip[1]})

    def send_d(c):
        return rcopy(ud.at[c], rd.at[c], dsm.at[c], drm.at[c], {'m1': ip[2]})

    def out_part(c, q):
        return out.at[rows_at(q * rows, rows), ds(c * LANES, LANES)]

    def send_e(c, e):
        return rcopy(fin.at[c], out_part(c, j), es.at[c, e - 1], er.at[c, e - 1], {'m2': jp[e]})

    def send_f(c):
        part = out_part(c, jp[2])
        return rcopy(part, part, es.at[c, 2], er.at[c, 2], {'m2': jp[1]})

    def out_own(c):
        return pltpu.make_async_copy(fin.at[c], out_part(c, j), fin_sem.at[c])

    def product2(c):
        slot = lax.rem(c, 2)
        cols = ds(i * LANES, LANES)
        loads = [pltpu.make_async_copy(wo.at[rows_at(i * qw, qw), ds(c * LANES, LANES)], w2b.at[slot, 0:qw, cols], w2b_sem.at[0]),
                 pltpu.make_async_copy(wd.at[rows_at(i * uw, uw), ds(c * LANES, LANES)], w2b.at[slot, qw:qw + uw, cols], w2b_sem.at[4])]
        for load in loads:
            load.start()
        with jax.named_scope('w_f2'):
            for e, kind in pieces2:
                f2_in(c, e, kind).wait_recv()
        for e in (1, 2, 3):
            cols = ds(ip[e] * LANES, LANES)
            loads.append(pltpu.make_async_copy(w2.at[c, :, cols], w2b.at[slot, :, cols], w2b_sem.at[e]))
            loads[-1].start()

        @pl.when(c >= 2)
        def _():
            for yy in range(2):
                send_a(c - 2, yy).wait_send()
        with jax.named_scope('w_w2b'):
            for load in loads:
                load.wait()
        for yy in range(2):
            for sub in range(2):
                at = rows_at(quarter(yy, 1 - jc) + sub * block, block)
                pa[slot, yy, sub * block:(sub + 1) * block, :] = dot(h[at, :], w2b[slot]).astype(jnp.bfloat16)
            send_a(c, yy).start()
        keep = lax.rem(c, 3)
        for yy in range(2):
            for sub in range(2):
                at = rows_at(quarter(yy, jc) + sub * block, block)
                po[keep, yy, sub * block:(sub + 1) * block, :] = dot(h[at, :], w2b[slot]).astype(jnp.bfloat16)

    def add(a, b):
        return (a.astype(jnp.float32) + b.astype(jnp.float32)).astype(jnp.bfloat16)

    def sum_core(d):
        keep = lax.rem(d, 3)
        with jax.named_scope('w_a'):
            for yy in range(2):
                part = ra.at[d, yy]
                rcopy(part, part, as_.at[d, yy], ar.at[d, yy], {'m2': jp[1]}).wait_recv()
        load = pltpu.make_async_copy(ra.at[d], rav, rav_sem.at[0])
        load.start()

        @pl.when(d >= 2)
        def _():
            send_b(d - 2).wait_send()
        load.wait()
        ss[lax.rem(d, 2)] = add(po[keep, 1 - jy], rav[1 - jy])
        send_b(d).start()
        po[keep, jy] = add(po[keep, jy], rav[jy])

    def sum_y(d):
        with jax.named_scope('w_b'):
            rcopy(rb.at[d], rb.at[d], bs.at[d], br.at[d], {'m2': jp[2]}).wait_recv()
        rb[d] = add(po[lax.rem(d, 3), jy], rb[d])
        for k in range(2):
            send_c(d, k).start()

    def sum_near(d):
        with jax.named_scope('w_c'):
            for k in range(2):
                rcopy(rc.at[d, k], rc.at[d, k], cs.at[d, k], cr.at[d, k], {'m1': ip[1]}).wait_recv()
        ud[d] = add(rb[d, :, ds(ip[2] * LANES, LANES)], rc[d, 1])
        send_d(d).start()

    def finish(d):
        with jax.named_scope('w_d'):
            rcopy(rd.at[d], rd.at[d], dsm.at[d], drm.at[d], {'m1': ip[2]}).wait_recv()
        cols = ds(d * LANES, LANES)
        value = rb[d, :, ds(i * LANES, LANES)].astype(jnp.float32) + rc[d, 0].astype(jnp.float32) + rd[d].astype(jnp.float32)
        value = xg[i, :, cols].astype(jnp.float32) + value + bo[:, cols]
        fin[d] = value.astype(jnp.bfloat16)
        send_e(d, 2).start()
        send_e(d, 1).start()
        out_own(d).start()

    def pass_on(d):
        with jax.named_scope('w_e'):
            part = out_part(d, jp[2])
            rcopy(part, part, es.at[d, 1], er.at[d, 1], {'m2': jp[2]}).wait_recv()
        send_f(d).start()

    def steps(c):
        for step, lag in ((pass_on, 3 + 2 * LAG), (finish, 2 + 2 * LAG), (sum_near, 2 + LAG), (sum_y, 2), (sum_core, 1)):
            @pl.when(c >= lag)
            def _(step=step, lag=lag):
                step(c - lag)

    @pl.loop(0, nc)
    def _(c):
        steps(c)

        @pl.when((c >= 1) & (c + 1 < nc))
        def _():
            next2(c + 1)
        product2(c)

    def run(step, first, last):
        @pl.loop(max(first, 0), last)
        def _(d):
            step(d)

    sum_core(nc - 1)
    sum_y(nc - 2)
    run(sum_near, nc - 2 - LAG, nc - 2)
    run(finish, nc - 2 - 2 * LAG, nc - 2 - LAG)
    run(pass_on, nc - 3 - 2 * LAG, nc - 3 - LAG)
    sum_y(nc - 1)
    run(sum_near, nc - 2, nc)
    run(finish, nc - 2 - LAG, nc)
    run(pass_on, nc - 3 - LAG, nc)

    with jax.named_scope('drain0'):
      for copy in (x_far, x_near, x_fwd, u_far, u_near, u_fwd):
        copy.wait_send()
    for b in range(3 + nub):
        for e in (2, 3, 1):
            z1(b, e).wait_send()
            f1(b, e).wait_send()

    @pl.loop(0, nc)
    def _(c):
        with jax.named_scope('drain_z2'):
          for e, kind in pieces2:
            z2(c, e, kind).wait_send()
            f2(c, e, kind).wait_send()
        for k in range(2):
            send_c(c, k).wait_send()
        send_d(c).wait_send()
        out_own(c).wait()
        send_e(c, 1).wait_send()
        send_e(c, 2).wait_send()
        send_f(c).wait_send()
        for e, q in ((1, jp[1]), (3, jp[3])):
            part = out_part(c, q)
            with jax.named_scope('w_f'):
                rcopy(part, part, es.at[c, e - 1], er.at[c, e - 1], {'m2': jp[1]}).wait_recv()

        @pl.when(c >= nc - 2)
        def _():
            for yy in range(2):
                send_a(c, yy).wait_send()
            send_b(c).wait_send()


def solution(mesh):
    assert mesh.shape['m1'] == 4 and mesh.shape['m2'] == 4 and mesh.shape['dp'] == 2

    def local_layer(x_blk, ln_scale, qn_scale, kn_scale, w_qkv, w_up, b_up, w_o, w_down, b_out):
        batch, patches, dim = x_blk.shape
        tokens = batch * patches
        qw, uw = w_qkv.shape[2] // 4, w_up.shape[1] // 4
        rows, block, nc, nb = tokens // 4, tokens // 8, dim // LANES, 3 + uw // qw
        assert qn_scale.shape[0] == LANES and uw % qw == 0 and nb == 7
        wide = 4 * LANES
        bf16 = jnp.bfloat16
        dma = pltpu.SemaphoreType.DMA
        hbm = pl.BlockSpec(memory_space=pltpu.HBM)
        vmem = pl.BlockSpec(memory_space=pltpu.VMEM)
        ln_rows = min(64, rows)
        out = pl.pallas_call(
            functools.partial(kernel, (batch, patches, dim, qw, uw)),
            out_shape=[
                jax.ShapeDtypeStruct((tokens, dim), bf16),
                jax.ShapeDtypeStruct((tokens, 4 * dim), bf16),
                jax.ShapeDtypeStruct((nb, 4 * dim, qw), bf16),
                jax.ShapeDtypeStruct((nc, qw + uw, wide), bf16),
                jax.ShapeDtypeStruct((nc, 2, rows, wide), bf16)],
            in_specs=[hbm, vmem, vmem, vmem, hbm, hbm, vmem, hbm, hbm, vmem],
            out_specs=[hbm] * 5,
            scratch_shapes=[
                pltpu.VMEM((4, rows, dim), bf16),
                pltpu.VMEM((2, ln_rows, 4 * dim), bf16),
                pltpu.VMEM((3, tokens, qw), bf16),
                pltpu.VMEM((tokens, qw + uw), bf16),
                pltpu.VMEM((4 * dim, qw), bf16),
                pltpu.VMEM((2, block, 4 * dim), bf16),
                pltpu.VMEM((2, qw + uw, wide), bf16),
                pltpu.VMEM((2, 2, rows, wide), bf16),
                pltpu.VMEM((3, 2, rows, wide), bf16),
                pltpu.VMEM((2, rows, wide), bf16),
                pltpu.VMEM((2, rows, wide), bf16),
                pltpu.VMEM((nc, rows, wide), bf16),
                pltpu.VMEM((nc, 2, rows, LANES), bf16),
                pltpu.VMEM((nc, rows, LANES), bf16),
                pltpu.VMEM((nc, rows, LANES), bf16),
                pltpu.VMEM((nc, rows, LANES), bf16),
                dma((3,)), dma((3,)),
                dma((nb, 3)), dma((nb, 3)), dma((nb, 3)), dma((nb, 3)),
                dma((3,)), dma((3,)),
                dma((nc, 3, 2)), dma((nc, 3, 2)), dma((nc, 3, 2)), dma((nc, 3, 2)),
                dma((nc, 2)), dma((nc, 2)), dma((nc,)), dma((nc,)), dma((nc, 2)), dma((nc, 2)), dma((nc,)), dma((nc,)),
                dma((nc, 3)), dma((nc, 3)),
                dma((1,)), dma((4,)), dma((2,)), dma((2,)), dma((5,)), dma((1,)), dma((nc,))],
            compiler_params=pltpu.CompilerParams(collective_id=0, has_side_effects=True, vmem_limit_bytes=67_043_328),
            name='layer',
        )(x_blk.reshape(tokens, dim), ln_scale[None], qn_scale[None], kn_scale[None], w_qkv.transpose(1, 0, 2), w_up,
          b_up[None], w_o, w_down, b_out[None])[0]
        return out.reshape(batch, patches, dim)

    return jax.shard_map(local_layer, mesh=mesh, in_specs=(P('dp', None, 'm1'), P(), P(), P(), P('m1', None, 'm2'), P('m1', 'm2'), P('m2'), P('m2', 'm1'), P('m2', 'm1'), P('m1')), out_specs=P('dp', None, 'm1'), check_vma=False)
```

```python
import functools

import jax
import jax.numpy as jnp
from jax import lax
from jax.experimental import pallas as pl
from jax.experimental.pallas import tpu as pltpu
from jax.sharding import PartitionSpec as P

LN_EPS = 1e-6
MESH = pl.DeviceIdType.MESH
LANES = 128
NEAR_LAG = 8
FINISH_LAG = 9
AHEAD = 2


def xors(value):
    return (value, value + 1 - 2 * lax.rem(value, 2), value + 2 - 4 * lax.div(value, 2), 3 - value)


def ds(start, size):
    return pl.ds(pl.multiple_of(start, size if size < LANES else LANES), size)


def rows_at(start, size):
    return pl.ds(pl.multiple_of(start, 8), size)


def rcopy(src, dst, send_sem, recv_sem, device):
    return pltpu.make_async_remote_copy(src_ref=src, dst_ref=dst, send_sem=send_sem, recv_sem=recv_sem, device_id=device, device_id_type=MESH)


def dot(lhs, rhs):
    return jnp.dot(lhs, rhs, preferred_element_type=jnp.float32)


def head_norm(values, scale):
    mean = jnp.mean(values, axis=-1, keepdims=True)
    centered = values - mean
    variance = jnp.mean(centered * centered, axis=-1, keepdims=True)
    return (centered * lax.rsqrt(variance + LN_EPS) * scale).astype(jnp.bfloat16)


def kernel(sizes, x, lns, qns, kns, wq, wu, bu, wo, wd, bo,
           out, u, w1, w2, ra,
           xg, ubl, zq, h, rhs, lhs, w2b, pa, po, rav, ss, rb, rc, ud, rd, fin,
           xs, xr, w1s, w1r, f1s, f1r, us, ur, w2s, w2r, f2s, f2r,
           as_, ar, bs, br, cs, cr, dsm, drm, es, er, own_sem, rhs_sem, lhs_sem, ub_sem, w2b_sem, rav_sem, fin_sem):
    batch, patches, dim, qw, uw = sizes
    tokens = batch * patches
    rows = tokens // 4
    block = rows // 2
    half = dim // 2
    total = 4 * dim
    nub = uw // qw
    nc = dim // LANES
    wide = 4 * LANES
    heads = qw // LANES
    ln_rows = min(64, rows)

    g, i, j = lax.axis_index('dp'), lax.axis_index('m1'), lax.axis_index('m2')
    ip, jp = xors(i), xors(j)
    jy, jc = lax.div(j, 2), lax.rem(j, 2)

    barrier = pltpu.get_barrier_semaphore()
    peers = [{'m1': ip[e]} for e in (1, 2, 3)] + [{'m2': jp[e]} for e in (1, 2, 3)] + [{'dp': 1 - g}]
    for peer in peers:
        pl.semaphore_signal(barrier, inc=1, device_id=peer, device_id_type=MESH)
    with jax.named_scope('barrier'):
        pl.semaphore_wait(barrier, len(peers))

    mine = rows_at(j * rows, rows)
    x_far = rcopy(x.at[mine, :], xg.at[i], xs.at[0], xr.at[0], {'m1': ip[2]})
    x_near = rcopy(x.at[mine, :], xg.at[i], xs.at[1], xr.at[1], {'m1': ip[1]})
    x_own = pltpu.make_async_copy(x.at[mine, :], xg.at[i], own_sem.at[0])
    x_far.start()
    x_near.start()
    x_own.start()
    x_far_in = rcopy(xg.at[ip[2]], xg.at[ip[2]], xs.at[0], xr.at[0], {'m1': ip[2]})
    with jax.named_scope('w_xfar'):
        x_far_in.wait_recv()
    x_fwd = rcopy(xg.at[ip[2]], xg.at[ip[2]], xs.at[2], xr.at[2], {'m1': ip[1]})
    x_fwd.start()

    def z1(b, e):
        t = ip[e]
        if b < 3:
            src = wq.at[b, rows_at(g * half, half), ds(t * qw, qw)]
        else:
            src = wu.at[rows_at(g * half, half), ds(t * uw + (b - 3) * qw, qw)]
        return rcopy(src, w1.at[b, rows_at(i * dim + g * half, half), :], w1s.at[b, e - 1], w1r.at[b, e - 1], {'m1': t})

    def f1(b, e):
        part = w1.at[b, rows_at(ip[e] * dim + g * half, half), :]
        return rcopy(part, part, f1s.at[b, e - 1], f1r.at[b, e - 1], {'dp': 1 - g})

    def z1_in(b, e):
        part = w1.at[b, rows_at(ip[e] * dim + g * half, half), :]
        return rcopy(part, part, w1s.at[b, e - 1], w1r.at[b, e - 1], {'m1': ip[e]})

    def f1_in(b, e):
        part = w1.at[b, rows_at(ip[e] * dim + (1 - g) * half, half), :]
        return rcopy(part, part, f1s.at[b, e - 1], f1r.at[b, e - 1], {'dp': 1 - g})

    def forward1(b):
        for e in (2, 3, 1):
            with jax.named_scope(f'w_z1e{e}'):
                z1_in(b, e).wait_recv()
            f1(b, e).start()

    def issue1(b):
        for e in (2, 3, 1):
            z1(b, e).start()

    issue1(0)
    issue1(1)

    def parts2(c, e, group, kind):
        size, first = (qw // 2, 0) if kind == 0 else (uw // 2, qw)
        return size, first + group * size

    def z2(c, e, kind):
        size, at = parts2(c, e, g, kind)
        t = ip[e]
        src = wo if kind == 0 else wd
        start = t * (2 * size) + g * size
        return rcopy(src.at[rows_at(start, size), ds(c * LANES, LANES)], w2.at[c, rows_at(at, size), ds(i * LANES, LANES)],
                     w2s.at[c, e - 1, kind], w2r.at[c, e - 1, kind], {'m1': t})

    def region2(c, e, group, kind):
        size, at = parts2(c, e, group, kind)
        return w2.at[c, rows_at(at, size), ds(ip[e] * LANES, LANES)]

    def z2_in(c, e, kind):
        part = region2(c, e, g, kind)
        return rcopy(part, part, w2s.at[c, e - 1, kind], w2r.at[c, e - 1, kind], {'m1': ip[e]})

    def f2(c, e, kind):
        part = region2(c, e, g, kind)
        return rcopy(part, part, f2s.at[c, e - 1, kind], f2r.at[c, e - 1, kind], {'dp': 1 - g})

    def f2_in(c, e, kind):
        part = region2(c, e, 1 - g, kind)
        return rcopy(part, part, f2s.at[c, e - 1, kind], f2r.at[c, e - 1, kind], {'dp': 1 - g})

    def next2(c):
        forward2(c)

        @pl.when(c + AHEAD < nc)
        def _():
            issue2(c + AHEAD)

    pieces2 = [(e, kind) for e in (2, 3, 1) for kind in (1, 0)]

    def issue2(c):
        for e, kind in pieces2:
            z2(c, e, kind).start()

    def forward2(c):
        for e, kind in pieces2:
            with jax.named_scope(f'w_z2e{e}k{kind}'):
                z2_in(c, e, kind).wait_recv()
            f2(c, e, kind).start()

    with jax.named_scope('w_xown'):
        x_own.wait()
    with jax.named_scope('w_xnear'):
        rcopy(xg.at[ip[1]], xg.at[ip[1]], xs.at[1], xr.at[1], {'m1': ip[1]}).wait_recv()
    with jax.named_scope('w_xfwd'):
        rcopy(xg.at[ip[3]], xg.at[ip[3]], xs.at[2], xr.at[2], {'m1': ip[1]}).wait_recv()

    def u_out(r, slot):
        return pltpu.make_async_copy(ubl.at[slot], u.at[rows_at(j * rows + r * ln_rows, ln_rows), :], ub_sem.at[slot])

    @pl.loop(0, rows // ln_rows)
    def _(r):
        slot = lax.rem(r, 2)

        @pl.when(r >= 2)
        def _():
            u_out(r - 2, slot).wait()
        at = rows_at(r * ln_rows, ln_rows)
        parts = [xg[s, at, :].astype(jnp.float32) for s in range(4)]
        mean = sum(jnp.sum(part, axis=-1, keepdims=True) for part in parts) / total
        parts = [part - mean for part in parts]
        variance = sum(jnp.sum(part * part, axis=-1, keepdims=True) for part in parts) / total
        inverse = lax.rsqrt(variance + LN_EPS)
        for s in range(4):
            cols = slice(s * dim, (s + 1) * dim)
            ubl[slot, :, cols] = (parts[s] * inverse * lns[:, cols]).astype(jnp.bfloat16)
        u_out(r, slot).start()

    for r in range(max(0, rows // ln_rows - 2), rows // ln_rows):
        u_out(r, r % 2).wait()

    def u_rows(q):
        return u.at[rows_at(q * rows, rows), :]

    u_far = rcopy(u_rows(j), u_rows(j), us.at[0], ur.at[0], {'m2': jp[2]})
    u_near = rcopy(u_rows(j), u_rows(j), us.at[1], ur.at[1], {'m2': jp[1]})
    u_far.start()
    u_near.start()
    for b in range(4):
        forward1(b)
        issue1(b + 2)
    with jax.named_scope('w_ufar'):
        rcopy(u_rows(jp[2]), u_rows(jp[2]), us.at[0], ur.at[0], {'m2': jp[2]}).wait_recv()
    u_fwd = rcopy(u_rows(jp[2]), u_rows(jp[2]), us.at[2], ur.at[2], {'m2': jp[1]})
    u_fwd.start()
    rcopy(u_rows(jp[1]), u_rows(jp[1]), us.at[1], ur.at[1], {'m2': jp[1]}).wait_recv()
    with jax.named_scope('w_ufwd'):
        rcopy(u_rows(jp[3]), u_rows(jp[3]), us.at[2], ur.at[2], {'m2': jp[1]}).wait_recv()

    def lhs_in(m, slot):
        return pltpu.make_async_copy(u.at[rows_at(m * block, block), :], lhs.at[slot], lhs_sem.at[slot])

    def product1(b, own, store):
        with jax.named_scope('w_f1'):
            for e in (1, 2, 3):
                f1_in(b, e).wait_recv()
        loads = [pltpu.make_async_copy(own, rhs.at[rows_at(i * dim, dim), :], rhs_sem.at[0])]
        for e in (1, 2, 3):
            at = rows_at(ip[e] * dim, dim)
            loads.append(pltpu.make_async_copy(w1.at[b, at, :], rhs.at[at, :], rhs_sem.at[e]))
        for load in loads:
            load.start()
        lhs_in(0, 0).start()
        for load in loads:
            load.wait()

        @pl.loop(0, tokens // block)
        def _(m):
            slot = lax.rem(m, 2)
            lhs_in(m, slot).wait()

            @pl.when(m + 1 < tokens // block)
            def _():
                lhs_in(m + 1, 1 - slot).start()
            with jax.named_scope('mm1'):
                store(rows_at(m * block, block), dot(lhs[slot], rhs[...]))

    @pl.loop(0, 3)
    def _(b):
        def store(at, value):
            zq[b, at, :] = value.astype(jnp.bfloat16)
        product1(b, wq.at[b, :, ds(i * qw, qw)], store)

        @pl.when(b == 1)
        def _():
            forward1(4)
            issue1(6)

    @pl.loop(0, batch)
    def _(n):
        at = rows_at(n * patches, patches)
        for head in range(heads):
            cols = slice(head * LANES, (head + 1) * LANES)
            query = head_norm(zq[0, at, cols].astype(jnp.float32), qns[...])
            key = head_norm(zq[1, at, cols].astype(jnp.float32), kns[...])
            scores = lax.dot_general(query, key, (((1,), (1,)), ((), ())), preferred_element_type=jnp.float32) * LANES ** -0.5
            scores = jnp.exp(scores - jnp.max(scores, axis=-1, keepdims=True))
            probs = (scores / jnp.sum(scores, axis=-1, keepdims=True)).astype(jnp.bfloat16)
            with jax.named_scope('attn'):
                h[at, cols] = dot(probs, zq[2, at, cols]).astype(jnp.bfloat16)

    forward1(5)
    for c in range(AHEAD // 2):
        issue2(c)

    @pl.loop(0, nub)
    def _(b):
        def store(at, value):
            value = value.astype(jnp.bfloat16).astype(jnp.float32) + bu[:, ds(i * uw + b * qw, qw)]
            value = 0.5 * value * (1.0 + lax.erf(value * 2.0 ** -0.5))
            h[at, ds(qw + b * qw, qw)] = value.astype(jnp.bfloat16)
        product1(b + 3, wu.at[:, ds(i * uw + b * qw, qw)], store)

        @pl.when(b == 1)
        def _():
            forward1(6)
            for c in range(AHEAD // 2, AHEAD):
                issue2(c)

        @pl.when(b == 2)
        def _():
            next2(0)

        @pl.when(b == 3)
        def _():
            next2(1)

    def quarter(yy, core):
        return (2 * yy + core) * rows

    def send_a(c, yy):
        return rcopy(pa.at[lax.rem(c, 2), yy], ra.at[c, yy], as_.at[c, yy], ar.at[c, yy], {'m2': jp[1]})

    def send_b(c):
        return rcopy(ss.at[lax.rem(c, 2)], rb.at[c], bs.at[c], br.at[c], {'m2': jp[2]})

    def send_c(c, k):
        src = rb.at[c, :, ds(ip[1 + 2 * k] * LANES, LANES)]
        return rcopy(src, rc.at[c, k], cs.at[c, k], cr.at[c, k], {'m1': ip[1]})

    def send_d(c):
        return rcopy(ud.at[c], rd.at[c], dsm.at[c], drm.at[c], {'m1': ip[2]})

    def out_part(c, q):
        return out.at[rows_at(q * rows, rows), ds(c * LANES, LANES)]

    def send_e(c, e):
        return rcopy(fin.at[c], out_part(c, j), es.at[c, e - 1], er.at[c, e - 1], {'m2': jp[e]})

    def send_f(c):
        part = out_part(c, jp[2])
        return rcopy(part, part, es.at[c, 2], er.at[c, 2], {'m2': jp[1]})

    def out_own(c):
        return pltpu.make_async_copy(fin.at[c], out_part(c, j), fin_sem.at[c])

    def product2(c):
        slot = lax.rem(c, 2)
        cols = ds(i * LANES, LANES)
        loads = [pltpu.make_async_copy(wo.at[rows_at(i * qw, qw), ds(c * LANES, LANES)], w2b.at[slot, 0:qw, cols], w2b_sem.at[0]),
                 pltpu.make_async_copy(wd.at[rows_at(i * uw, uw), ds(c * LANES, LANES)], w2b.at[slot, qw:qw + uw, cols], w2b_sem.at[4])]
        for load in loads:
            load.start()
        with jax.named_scope('w_f2'):
            for e, kind in pieces2:
                f2_in(c, e, kind).wait_recv()
        for e in (1, 2, 3):
            cols = ds(ip[e] * LANES, LANES)
            loads.append(pltpu.make_async_copy(w2.at[c, :, cols], w2b.at[slot, :, cols], w2b_sem.at[e]))
            loads[-1].start()

        @pl.when(c >= 2)
        def _():
            for yy in range(2):
                send_a(c - 2, yy).wait_send()
        with jax.named_scope('w_w2b'):
            for load in loads:
                load.wait()
        for yy in range(2):
            for sub in range(2):
                at = rows_at(quarter(yy, 1 - jc) + sub * block, block)
                pa[slot, yy, sub * block:(sub + 1) * block, :] = dot(h[at, :], w2b[slot]).astype(jnp.bfloat16)
            send_a(c, yy).start()
        keep = lax.rem(c, 3)
        for yy in range(2):
            for sub in range(2):
                at = rows_at(quarter(yy, jc) + sub * block, block)
                po[keep, yy, sub * block:(sub + 1) * block, :] = dot(h[at, :], w2b[slot]).astype(jnp.bfloat16)

    def add(a, b):
        return (a.astype(jnp.float32) + b.astype(jnp.float32)).astype(jnp.bfloat16)

    def sum_core(d):
        keep = lax.rem(d, 3)
        with jax.named_scope('w_a'):
            for yy in range(2):
                part = ra.at[d, yy]
                rcopy(part, part, as_.at[d, yy], ar.at[d, yy], {'m2': jp[1]}).wait_recv()
        load = pltpu.make_async_copy(ra.at[d], rav, rav_sem.at[0])
        load.start()

        @pl.when(d >= 2)
        def _():
            send_b(d - 2).wait_send()
        load.wait()
        ss[lax.rem(d, 2)] = add(po[keep, 1 - jy], rav[1 - jy])
        send_b(d).start()
        po[keep, jy] = add(po[keep, jy], rav[jy])

    def sum_y(d):
        with jax.named_scope('w_b'):
            rcopy(rb.at[d], rb.at[d], bs.at[d], br.at[d], {'m2': jp[2]}).wait_recv()
        rb[d] = add(po[lax.rem(d, 3), jy], rb[d])
        for k in range(2):
            send_c(d, k).start()

    def sum_near(d):
        with jax.named_scope('w_c'):
            for k in range(2):
                rcopy(rc.at[d, k], rc.at[d, k], cs.at[d, k], cr.at[d, k], {'m1': ip[1]}).wait_recv()
        ud[d] = add(rb[d, :, ds(ip[2] * LANES, LANES)], rc[d, 1])
        send_d(d).start()

    def finish(d):
        with jax.named_scope('w_d'):
            rcopy(rd.at[d], rd.at[d], dsm.at[d], drm.at[d], {'m1': ip[2]}).wait_recv()
        cols = ds(d * LANES, LANES)
        value = rb[d, :, ds(i * LANES, LANES)].astype(jnp.float32) + rc[d, 0].astype(jnp.float32) + rd[d].astype(jnp.float32)
        value = xg[i, :, cols].astype(jnp.float32) + value + bo[:, cols]
        fin[d] = value.astype(jnp.bfloat16)
        send_e(d, 2).start()
        send_e(d, 1).start()
        out_own(d).start()

    def pass_on(d):
        with jax.named_scope('w_e'):
            part = out_part(d, jp[2])
            rcopy(part, part, es.at[d, 1], er.at[d, 1], {'m2': jp[2]}).wait_recv()
        send_f(d).start()

    def run(step, first, last):
        @pl.loop(max(first, 0), max(last, 0))
        def _(d):
            step(d)

    def late(c, lag, step, last=nc):
        @pl.when((c >= lag) & (c < last))
        def _():
            step(c - lag)

    @pl.loop(0, nc)
    def _(c):
        late(c, FINISH_LAG, finish)
        late(c, NEAR_LAG, sum_near, nc - 1)
        late(c, 2, sum_y)
        late(c, 1, sum_core)

        @pl.when((c >= 1) & (c + 1 < nc))
        def _():
            next2(c + 1)

        @pl.when(c == nc - 2)
        def _():
            run(sum_near, nc - 1 - NEAR_LAG, nc - 4)

        @pl.when(c == nc - 1)
        def _():
            sum_near(nc - 4)
        product2(c)

    sum_core(nc - 1)
    sum_y(nc - 2)
    sum_near(nc - 3)
    run(finish, nc - FINISH_LAG, nc - 6)
    sum_y(nc - 1)
    sum_near(nc - 2)
    run(finish, max(nc - FINISH_LAG, nc - 6), nc - 3)
    sum_near(nc - 1)
    run(finish, nc - 3, nc)
    run(pass_on, 0, nc)

    with jax.named_scope('drain0'):
      for copy in (x_far, x_near, x_fwd, u_far, u_near, u_fwd):
        copy.wait_send()
    for b in range(3 + nub):
        for e in (2, 3, 1):
            z1(b, e).wait_send()
            f1(b, e).wait_send()

    @pl.loop(0, nc)
    def _(c):
        with jax.named_scope('drain_z2'):
          for e, kind in pieces2:
            z2(c, e, kind).wait_send()
            f2(c, e, kind).wait_send()
        for k in range(2):
            send_c(c, k).wait_send()
        send_d(c).wait_send()
        out_own(c).wait()
        send_e(c, 1).wait_send()
        send_e(c, 2).wait_send()
        send_f(c).wait_send()
        for e, q in ((1, jp[1]), (3, jp[3])):
            part = out_part(c, q)
            with jax.named_scope('w_f'):
                rcopy(part, part, es.at[c, e - 1], er.at[c, e - 1], {'m2': jp[1]}).wait_recv()

        @pl.when(c >= nc - 2)
        def _():
            for yy in range(2):
                send_a(c, yy).wait_send()
            send_b(c).wait_send()


def solution(mesh):
    assert mesh.shape['m1'] == 4 and mesh.shape['m2'] == 4 and mesh.shape['dp'] == 2

    def local_layer(x_blk, ln_scale, qn_scale, kn_scale, w_qkv, w_up, b_up, w_o, w_down, b_out):
        batch, patches, dim = x_blk.shape
        tokens = batch * patches
        qw, uw = w_qkv.shape[2] // 4, w_up.shape[1] // 4
        rows, block, nc, nb = tokens // 4, tokens // 8, dim // LANES, 3 + uw // qw
        assert qn_scale.shape[0] == LANES and uw % qw == 0 and nb == 7
        wide = 4 * LANES
        bf16 = jnp.bfloat16
        dma = pltpu.SemaphoreType.DMA
        hbm = pl.BlockSpec(memory_space=pltpu.HBM)
        vmem = pl.BlockSpec(memory_space=pltpu.VMEM)
        ln_rows = min(64, rows)
        out = pl.pallas_call(
            functools.partial(kernel, (batch, patches, dim, qw, uw)),
            out_shape=[
                jax.ShapeDtypeStruct((tokens, dim), bf16),
                jax.ShapeDtypeStruct((tokens, 4 * dim), bf16),
                jax.ShapeDtypeStruct((nb, 4 * dim, qw), bf16),
                jax.ShapeDtypeStruct((nc, qw + uw, wide), bf16),
                jax.ShapeDtypeStruct((nc, 2, rows, wide), bf16)],
            in_specs=[hbm, vmem, vmem, vmem, hbm, hbm, vmem, hbm, hbm, vmem],
            out_specs=[hbm] * 5,
            scratch_shapes=[
                pltpu.VMEM((4, rows, dim), bf16),
                pltpu.VMEM((2, ln_rows, 4 * dim), bf16),
                pltpu.VMEM((3, tokens, qw), bf16),
                pltpu.VMEM((tokens, qw + uw), bf16),
                pltpu.VMEM((4 * dim, qw), bf16),
                pltpu.VMEM((2, block, 4 * dim), bf16),
                pltpu.VMEM((2, qw + uw, wide), bf16),
                pltpu.VMEM((2, 2, rows, wide), bf16),
                pltpu.VMEM((3, 2, rows, wide), bf16),
                pltpu.VMEM((2, rows, wide), bf16),
                pltpu.VMEM((2, rows, wide), bf16),
                pltpu.VMEM((nc, rows, wide), bf16),
                pltpu.VMEM((nc, 2, rows, LANES), bf16),
                pltpu.VMEM((nc, rows, LANES), bf16),
                pltpu.VMEM((nc, rows, LANES), bf16),
                pltpu.VMEM((nc, rows, LANES), bf16),
                dma((3,)), dma((3,)),
                dma((nb, 3)), dma((nb, 3)), dma((nb, 3)), dma((nb, 3)),
                dma((3,)), dma((3,)),
                dma((nc, 3, 2)), dma((nc, 3, 2)), dma((nc, 3, 2)), dma((nc, 3, 2)),
                dma((nc, 2)), dma((nc, 2)), dma((nc,)), dma((nc,)), dma((nc, 2)), dma((nc, 2)), dma((nc,)), dma((nc,)),
                dma((nc, 3)), dma((nc, 3)),
                dma((1,)), dma((4,)), dma((2,)), dma((2,)), dma((5,)), dma((1,)), dma((nc,))],
            compiler_params=pltpu.CompilerParams(collective_id=0, has_side_effects=True, vmem_limit_bytes=67_043_328),
            name='layer',
        )(x_blk.reshape(tokens, dim), ln_scale[None], qn_scale[None], kn_scale[None], w_qkv.transpose(1, 0, 2), w_up,
          b_up[None], w_o, w_down, b_out[None])[0]
        return out.reshape(batch, patches, dim)

    return jax.shard_map(local_layer, mesh=mesh, in_specs=(P('dp', None, 'm1'), P(), P(), P(), P('m1', None, 'm2'), P('m1', 'm2'), P('m2'), P('m2', 'm1'), P('m2', 'm1'), P('m1')), out_specs=P('dp', None, 'm1'), check_vma=False)
```

```python
import functools

import jax
import jax.numpy as jnp
from jax import lax
from jax.experimental import pallas as pl
from jax.experimental.pallas import tpu as pltpu
from jax.sharding import PartitionSpec as P

LN_EPS = 1e-6
MESH = pl.DeviceIdType.MESH
LANES = 128
NEAR_LAG = 8
AHEAD = 2


def xors(value):
    return (value, value + 1 - 2 * lax.rem(value, 2), value + 2 - 4 * lax.div(value, 2), 3 - value)


def ds(start, size):
    return pl.ds(pl.multiple_of(start, size if size < LANES else LANES), size)


def rows_at(start, size):
    return pl.ds(pl.multiple_of(start, 8), size)


def rcopy(src, dst, send_sem, recv_sem, device):
    return pltpu.make_async_remote_copy(src_ref=src, dst_ref=dst, send_sem=send_sem, recv_sem=recv_sem, device_id=device, device_id_type=MESH)


def dot(lhs, rhs):
    return jnp.dot(lhs, rhs, preferred_element_type=jnp.float32)


def head_norm(values, scale):
    mean = jnp.mean(values, axis=-1, keepdims=True)
    centered = values - mean
    variance = jnp.mean(centered * centered, axis=-1, keepdims=True)
    return (centered * lax.rsqrt(variance + LN_EPS) * scale).astype(jnp.bfloat16)


def kernel(sizes, x, lns, qns, kns, wq, wu, bu, wo, wd, bo,
           out, u, w1, w2, ra,
           xg, ubl, zq, h, rhs, lhs, w2b, pa, po, rav, ss, rb, rc, ud, rd,
           xs, xr, w1s, w1r, f1s, f1r, us, ur, w2s, w2r, f2s, f2r,
           as_, ar, bs, br, cs, cr, dsm, drm, es, er, fr, own_sem, rhs_sem, lhs_sem, ub_sem, w2b_sem, rav_sem):
    batch, patches, dim, qw, uw = sizes
    tokens = batch * patches
    rows = tokens // 4
    block = rows // 2
    half = dim // 2
    total = 4 * dim
    nub = uw // qw
    nc = dim // LANES
    wide = 4 * LANES
    heads = qw // LANES
    ln_rows = min(64, rows)

    g, i, j = lax.axis_index('dp'), lax.axis_index('m1'), lax.axis_index('m2')
    ip, jp = xors(i), xors(j)
    jy, jc = lax.div(j, 2), lax.rem(j, 2)
    mid = lax.div(lax.rem(i + 1, 4), 2)
    peers1 = ((0, ip[1]), (2 - mid, ip[3] + mid * (ip[2] - ip[3])), (1 + mid, ip[2] + mid * (ip[3] - ip[2])))

    barrier = pltpu.get_barrier_semaphore()
    peers = [{'m1': ip[e]} for e in (1, 2, 3)] + [{'m2': jp[e]} for e in (1, 2, 3)] + [{'dp': 1 - g}]
    for peer in peers:
        pl.semaphore_signal(barrier, inc=1, device_id=peer, device_id_type=MESH)
    with jax.named_scope('barrier'):
        pl.semaphore_wait(barrier, len(peers))

    mine = rows_at(j * rows, rows)
    x_far = rcopy(x.at[mine, :], xg.at[i], xs.at[0], xr.at[0], {'m1': ip[2]})
    x_near = rcopy(x.at[mine, :], xg.at[i], xs.at[1], xr.at[1], {'m1': ip[1]})
    x_own = pltpu.make_async_copy(x.at[mine, :], xg.at[i], own_sem.at[0])
    x_far.start()
    x_near.start()
    x_own.start()
    x_far_in = rcopy(xg.at[ip[2]], xg.at[ip[2]], xs.at[0], xr.at[0], {'m1': ip[2]})
    with jax.named_scope('w_xfar'):
        x_far_in.wait_recv()
    x_fwd = rcopy(xg.at[ip[2]], xg.at[ip[2]], xs.at[2], xr.at[2], {'m1': ip[1]})
    x_fwd.start()

    def z1(b, e):
        t = ip[e]
        if b < 3:
            src = wq.at[b, rows_at(g * half, half), ds(t * qw, qw)]
        else:
            src = wu.at[rows_at(g * half, half), ds(t * uw + (b - 3) * qw, qw)]
        return rcopy(src, w1.at[b, rows_at(i * dim + g * half, half), :], w1s.at[0], w1r.at[b, e - 1], {'m1': t})

    def piece1(b, k, s):
        part = w1.at[b, rows_at(s * dim + g * half, half), :]
        return (rcopy(part, part, w1s.at[0], w1r.at[b, k], {'m1': s}), rcopy(part, part, f1s.at[0], f1r.at[b], {'dp': 1 - g}))

    def forward1(b):
        for k, s in peers1:
            arrival, swap = piece1(b, k, s)
            with jax.named_scope('w_z1'):
                arrival.wait_recv()
            swap.start()

    def swapped1(b):
        part = w1.at[b, 0:3 * half, :]
        return rcopy(part, part, f1s.at[0], f1r.at[b], {'dp': 1 - g})

    def issue1(b):
        for e in (2, 3, 1):
            z1(b, e).start()

    issue1(0)
    issue1(1)

    qh, uh = qw // 2, uw // 2

    def z2(c, e):
        t = ip[e]
        cols, to = ds(c * LANES, LANES), ds(i * LANES, LANES)
        return [rcopy(wd.at[rows_at(t * uw + g * uh, uh), cols], w2.at[c, g, qh:qh + uh, to], w2s.at[0], w2r.at[c, e - 1], {'m1': t}),
                rcopy(wo.at[rows_at(t * qw + g * qh, qh), cols], w2.at[c, g, 0:qh, to], w2s.at[0], w2r.at[c, e - 1], {'m1': t})]

    def issue2(c):
        for e in (2, 3, 1):
            for copy in z2(c, e):
                copy.start()

    def forward2(c):
        for k, s in peers1:
            part = w2.at[c, g, :, ds(s * LANES, LANES)]
            with jax.named_scope('w_z2'):
                rcopy(part, part, w2s.at[0], w2r.at[c, k], {'m1': s}).wait_recv()
            rcopy(part, part, f2s.at[0], f2r.at[c], {'dp': 1 - g}).start()

    def next2(c):
        forward2(c)

        @pl.when(c + AHEAD < nc)
        def _():
            issue2(c + AHEAD)

    with jax.named_scope('w_xown'):
        x_own.wait()
    with jax.named_scope('w_xnear'):
        rcopy(xg.at[ip[1]], xg.at[ip[1]], xs.at[1], xr.at[1], {'m1': ip[1]}).wait_recv()
    with jax.named_scope('w_xfwd'):
        rcopy(xg.at[ip[3]], xg.at[ip[3]], xs.at[2], xr.at[2], {'m1': ip[1]}).wait_recv()

    def u_out(r, slot):
        return pltpu.make_async_copy(ubl.at[slot], u.at[rows_at(j * rows + r * ln_rows, ln_rows), :], ub_sem.at[slot])

    @pl.loop(0, rows // ln_rows)
    def _(r):
        slot = lax.rem(r, 2)

        @pl.when(r >= 2)
        def _():
            u_out(r - 2, slot).wait()
        at = rows_at(r * ln_rows, ln_rows)
        parts = [xg[s, at, :].astype(jnp.float32) for s in range(4)]
        mean = sum(jnp.sum(part, axis=-1, keepdims=True) for part in parts) / total
        parts = [part - mean for part in parts]
        variance = sum(jnp.sum(part * part, axis=-1, keepdims=True) for part in parts) / total
        inverse = lax.rsqrt(variance + LN_EPS)
        for s in range(4):
            cols = slice(s * dim, (s + 1) * dim)
            ubl[slot, :, cols] = (parts[s] * inverse * lns[:, cols]).astype(jnp.bfloat16)
        u_out(r, slot).start()

    for r in range(max(0, rows // ln_rows - 2), rows // ln_rows):
        u_out(r, r % 2).wait()

    def u_rows(q):
        return u.at[rows_at(q * rows, rows), :]

    u_far = rcopy(u_rows(j), u_rows(j), us.at[0], ur.at[0], {'m2': jp[2]})
    u_near = rcopy(u_rows(j), u_rows(j), us.at[1], ur.at[1], {'m2': jp[1]})
    u_far.start()
    u_near.start()
    for b in range(4):
        forward1(b)
        issue1(b + 2)
    with jax.named_scope('w_ufar'):
        rcopy(u_rows(jp[2]), u_rows(jp[2]), us.at[0], ur.at[0], {'m2': jp[2]}).wait_recv()
    u_fwd = rcopy(u_rows(jp[2]), u_rows(jp[2]), us.at[2], ur.at[2], {'m2': jp[1]})
    u_fwd.start()
    rcopy(u_rows(jp[1]), u_rows(jp[1]), us.at[1], ur.at[1], {'m2': jp[1]}).wait_recv()
    with jax.named_scope('w_ufwd'):
        rcopy(u_rows(jp[3]), u_rows(jp[3]), us.at[2], ur.at[2], {'m2': jp[1]}).wait_recv()

    def lhs_in(m, slot):
        return pltpu.make_async_copy(u.at[rows_at(m * block, block), :], lhs.at[slot], lhs_sem.at[slot])

    def product1(b, own, store):
        with jax.named_scope('w_f1'):
            swapped1(b).wait_recv()
        loads = [pltpu.make_async_copy(own, rhs.at[rows_at(i * dim, dim), :], rhs_sem.at[0])]
        for e in (1, 2, 3):
            at = rows_at(ip[e] * dim, dim)
            loads.append(pltpu.make_async_copy(w1.at[b, at, :], rhs.at[at, :], rhs_sem.at[e]))
        for load in loads:
            load.start()
        lhs_in(0, 0).start()
        for load in loads:
            load.wait()

        @pl.loop(0, tokens // block)
        def _(m):
            slot = lax.rem(m, 2)
            lhs_in(m, slot).wait()

            @pl.when(m + 1 < tokens // block)
            def _():
                lhs_in(m + 1, 1 - slot).start()
            with jax.named_scope('mm1'):
                store(rows_at(m * block, block), dot(lhs[slot], rhs[...]))

    @pl.loop(0, 3)
    def _(b):
        def store(at, value):
            zq[b, at, :] = value.astype(jnp.bfloat16)
        product1(b, wq.at[b, :, ds(i * qw, qw)], store)

        @pl.when(b == 1)
        def _():
            forward1(4)
            issue1(6)

    @pl.loop(0, batch)
    def _(n):
        at = rows_at(n * patches, patches)
        for head in range(heads):
            cols = slice(head * LANES, (head + 1) * LANES)
            query = head_norm(zq[0, at, cols].astype(jnp.float32), qns[...])
            key = head_norm(zq[1, at, cols].astype(jnp.float32), kns[...])
            scores = lax.dot_general(query, key, (((1,), (1,)), ((), ())), preferred_element_type=jnp.float32) * LANES ** -0.5
            scores = jnp.exp(scores - jnp.max(scores, axis=-1, keepdims=True))
            probs = (scores / jnp.sum(scores, axis=-1, keepdims=True)).astype(jnp.bfloat16)
            with jax.named_scope('attn'):
                h[at, cols] = dot(probs, zq[2, at, cols]).astype(jnp.bfloat16)

    forward1(5)
    for c in range(AHEAD // 2):
        issue2(c)

    @pl.loop(0, nub)
    def _(b):
        def store(at, value):
            value = value.astype(jnp.bfloat16).astype(jnp.float32) + bu[:, ds(i * uw + b * qw, qw)]
            value = 0.5 * value * (1.0 + lax.erf(value * 2.0 ** -0.5))
            h[at, ds(qw + b * qw, qw)] = value.astype(jnp.bfloat16)
        product1(b + 3, wu.at[:, ds(i * uw + b * qw, qw)], store)

        @pl.when(b == 1)
        def _():
            forward1(6)
            for c in range(AHEAD // 2, AHEAD):
                issue2(c)

        @pl.when(b == 2)
        def _():
            next2(0)

        @pl.when(b == 3)
        def _():
            next2(1)

    def quarter(yy, core):
        return (2 * yy + core) * rows

    def send_a(c, yy):
        return rcopy(pa.at[lax.rem(c, 2), yy], ra.at[c, yy], as_.at[lax.rem(c, 2)], ar.at[c], {'m2': jp[1]})

    def all_a(c):
        return rcopy(pa.at[lax.rem(c, 2)], ra.at[c], as_.at[lax.rem(c, 2)], ar.at[c], {'m2': jp[1]})

    def send_b(c):
        return rcopy(ss.at[lax.rem(c, 2)], rb.at[c], bs.at[lax.rem(c, 2)], br.at[c], {'m2': jp[2]})

    def send_c(c, k):
        src = rb.at[c, :, ds(ip[1 + 2 * k] * LANES, LANES)]
        return rcopy(src, rc.at[c, k], cs.at[0], cr.at[c], {'m1': ip[1]})

    def send_d(c):
        return rcopy(ud.at[c], rd.at[c], dsm.at[0], drm.at[c], {'m1': ip[2]})

    def out_part(c, q):
        return out.at[rows_at(q * rows, rows), ds(c * LANES, LANES)]

    def result(c, q, sem, recv, device):
        part = out_part(c, q)
        return rcopy(part, part, es.at[sem], recv, device)

    def product2(c):
        slot = lax.rem(c, 2)
        cols, to = ds(c * LANES, LANES), ds(i * LANES, LANES)
        loads = [pltpu.make_async_copy(wo.at[rows_at(i * qw, qw), cols], w2b.at[slot, 0:qw, to], w2b_sem.at[0]),
                 pltpu.make_async_copy(wd.at[rows_at(i * uw, uw), cols], w2b.at[slot, qw:qw + uw, to], w2b_sem.at[1])]
        for load in loads:
            load.start()
        with jax.named_scope('w_f2'):
            part = w2.at[c, 0, :, 0:3 * LANES]
            rcopy(part, part, f2s.at[0], f2r.at[c], {'dp': 1 - g}).wait_recv()
        for e in (1, 2, 3):
            to = ds(ip[e] * LANES, LANES)
            for k in range(2):
                sems = 2 + 4 * (e - 1) + 2 * k
                loads.append(pltpu.make_async_copy(w2.at[c, k, 0:qh, to], w2b.at[slot, k * qh:(k + 1) * qh, to], w2b_sem.at[sems]))
                loads.append(pltpu.make_async_copy(w2.at[c, k, qh:qh + uh, to], w2b.at[slot, qw + k * uh:qw + (k + 1) * uh, to], w2b_sem.at[sems + 1]))
        for load in loads[2:]:
            load.start()

        @pl.when(c >= 2)
        def _():
            all_a(c - 2).wait_send()
        with jax.named_scope('w_w2b'):
            for load in loads:
                load.wait()
        for yy in range(2):
            for sub in range(2):
                at = rows_at(quarter(yy, 1 - jc) + sub * block, block)
                pa[slot, yy, sub * block:(sub + 1) * block, :] = dot(h[at, :], w2b[slot]).astype(jnp.bfloat16)
            send_a(c, yy).start()
        keep = lax.rem(c, 3)
        for yy in range(2):
            for sub in range(2):
                at = rows_at(quarter(yy, jc) + sub * block, block)
                po[keep, yy, sub * block:(sub + 1) * block, :] = dot(h[at, :], w2b[slot]).astype(jnp.bfloat16)

    def add(a, b):
        return (a.astype(jnp.float32) + b.astype(jnp.float32)).astype(jnp.bfloat16)

    def sum_core(d):
        keep = lax.rem(d, 3)
        with jax.named_scope('w_a'):
            rcopy(ra.at[d], ra.at[d], as_.at[0], ar.at[d], {'m2': jp[1]}).wait_recv()
        load = pltpu.make_async_copy(ra.at[d], rav, rav_sem.at[0])
        load.start()

        @pl.when(d >= 2)
        def _():
            send_b(d - 2).wait_send()
        load.wait()
        ss[lax.rem(d, 2)] = add(po[keep, 1 - jy], rav[1 - jy])
        send_b(d).start()
        po[keep, jy] = add(po[keep, jy], rav[jy])

    def sum_y(d):
        with jax.named_scope('w_b'):
            rcopy(rb.at[d], rb.at[d], bs.at[0], br.at[d], {'m2': jp[2]}).wait_recv()
        rb[d] = add(po[lax.rem(d, 3), jy], rb[d])
        for k in range(2):
            send_c(d, k).start()

    def sum_near(d):
        with jax.named_scope('w_c'):
            rcopy(rc.at[d], rc.at[d], cs.at[0], cr.at[d], {'m1': ip[1]}).wait_recv()
        ud[d] = add(rb[d, :, ds(ip[2] * LANES, LANES)], rc[d, 1])
        send_d(d).start()

    def finish(d):
        with jax.named_scope('w_d'):
            rcopy(rd.at[d], rd.at[d], dsm.at[0], drm.at[d], {'m1': ip[2]}).wait_recv()
        cols = ds(d * LANES, LANES)
        value = rb[d, :, ds(i * LANES, LANES)].astype(jnp.float32) + rc[d, 0].astype(jnp.float32) + rd[d].astype(jnp.float32)
        value = xg[i, :, cols].astype(jnp.float32) + value + bo[cols][None, :]
        out[rows_at(j * rows, rows), cols] = value.astype(jnp.bfloat16)
        result(d, j, 0, er.at[d], {'m2': jp[2]}).start()
        result(d, j, 1, fr.at[0], {'m2': jp[1]}).start()

    def pass_on(d):
        with jax.named_scope('w_e'):
            result(d, jp[2], 0, er.at[d], {'m2': jp[2]}).wait_recv()
        result(d, jp[2], 2, fr.at[1], {'m2': jp[1]}).start()

    def run(step, first, last):
        @pl.loop(max(first, 0), max(last, 0))
        def _(d):
            step(d)

    def late(c, lag, step, last=nc):
        @pl.when((c >= lag) & (c < last))
        def _():
            step(c - lag)

    @pl.loop(0, nc)
    def _(c):
        late(c, NEAR_LAG, sum_near, nc - 1)
        late(c, 2, sum_y)
        late(c, 1, sum_core)

        @pl.when((c >= 1) & (c + 1 < nc))
        def _():
            next2(c + 1)

        @pl.when(c == nc - 2)
        def _():
            run(sum_near, nc - 1 - NEAR_LAG, nc - 4)

        @pl.when(c == nc - 1)
        def _():
            sum_near(nc - 4)
        product2(c)

    sum_core(nc - 1)
    sum_y(nc - 2)
    sum_near(nc - 3)
    run(finish, 0, nc - 6)
    sum_y(nc - 1)
    sum_near(nc - 2)
    run(finish, nc - 6, nc - 3)
    sum_near(nc - 1)
    run(finish, nc - 3, nc)
    run(pass_on, 0, nc)

    with jax.named_scope('drain0'):
      for copy in (x_far, x_near, x_fwd, u_far, u_near, u_fwd):
        copy.wait_send()
    for sem in (w1s, f1s):
        part = w1.at[:, 0:3 * half, :]
        rcopy(part, part, sem.at[0], w1r.at[0, 0], {'dp': 1 - g}).wait_send()
    for sem in (w2s, f2s):
        part = w2.at[:, 0, :, 0:3 * LANES]
        rcopy(part, part, sem.at[0], f2r.at[0], {'dp': 1 - g}).wait_send()
    for c in (nc - 2, nc - 1):
        all_a(c).wait_send()
        send_b(c).wait_send()
    rcopy(rc, rc, cs.at[0], cr.at[0], {'m1': ip[1]}).wait_send()
    for sem in (dsm.at[0], es.at[0], es.at[1], es.at[2]):
        rcopy(rd, rd, sem, drm.at[0], {'m1': ip[2]}).wait_send()
    for k in range(2):
        with jax.named_scope('w_f'):
            rcopy(rd, rd, es.at[1], fr.at[k], {'m2': jp[1]}).wait_recv()


def solution(mesh):
    assert mesh.shape['m1'] == 4 and mesh.shape['m2'] == 4 and mesh.shape['dp'] == 2

    def local_layer(x_blk, ln_scale, qn_scale, kn_scale, w_qkv, w_up, b_up, w_o, w_down, b_out):
        batch, patches, dim = x_blk.shape
        tokens = batch * patches
        qw, uw = w_qkv.shape[2] // 4, w_up.shape[1] // 4
        rows, block, nc, nb = tokens // 4, tokens // 8, dim // LANES, 3 + uw // qw
        assert qn_scale.shape[0] == LANES and uw % qw == 0 and nb == 7
        wide = 4 * LANES
        bf16 = jnp.bfloat16
        dma = pltpu.SemaphoreType.DMA
        hbm = pl.BlockSpec(memory_space=pltpu.HBM)
        vmem = pl.BlockSpec(memory_space=pltpu.VMEM)
        ln_rows = min(64, rows)
        out = pl.pallas_call(
            functools.partial(kernel, (batch, patches, dim, qw, uw)),
            out_shape=[
                pltpu.VMEM((tokens, dim), bf16),
                jax.ShapeDtypeStruct((tokens, 4 * dim), bf16),
                jax.ShapeDtypeStruct((nb, 4 * dim, qw), bf16),
                jax.ShapeDtypeStruct((nc, 2, (qw + uw) // 2, wide), bf16),
                jax.ShapeDtypeStruct((nc, 2, rows, wide), bf16)],
            in_specs=[hbm, vmem, vmem, vmem, hbm, hbm, vmem, hbm, hbm, vmem],
            out_specs=[vmem] + [hbm] * 4,
            scratch_shapes=[
                pltpu.VMEM((4, rows, dim), bf16),
                pltpu.VMEM((2, ln_rows, 4 * dim), bf16),
                pltpu.VMEM((3, tokens, qw), bf16),
                pltpu.VMEM((tokens, qw + uw), bf16),
                pltpu.VMEM((4 * dim, qw), bf16),
                pltpu.VMEM((2, block, 4 * dim), bf16),
                pltpu.VMEM((2, qw + uw, wide), bf16),
                pltpu.VMEM((2, 2, rows, wide), bf16),
                pltpu.VMEM((3, 2, rows, wide), bf16),
                pltpu.VMEM((2, rows, wide), bf16),
                pltpu.VMEM((2, rows, wide), bf16),
                pltpu.VMEM((nc, rows, wide), bf16),
                pltpu.VMEM((nc, 2, rows, LANES), bf16),
                pltpu.VMEM((nc, rows, LANES), bf16),
                pltpu.VMEM((nc, rows, LANES), bf16),
                dma((3,)), dma((3,)),
                dma((1,)), dma((nb, 3)), dma((1,)), dma((nb,)),
                dma((3,)), dma((3,)),
                dma((1,)), dma((nc, 3)), dma((1,)), dma((nc,)),
                dma((2,)), dma((nc,)), dma((2,)), dma((nc,)), dma((1,)), dma((nc,)), dma((1,)), dma((nc,)),
                dma((3,)), dma((nc,)), dma((2,)),
                dma((1,)), dma((4,)), dma((2,)), dma((2,)), dma((14,)), dma((1,))],
            compiler_params=pltpu.CompilerParams(collective_id=0, has_side_effects=True, vmem_limit_bytes=60_000_000),
            name='layer',
        )(x_blk.reshape(tokens, dim), ln_scale[None], qn_scale[None], kn_scale[None], w_qkv.transpose(1, 0, 2), w_up,
          b_up[None], w_o, w_down, b_out)[0]
        return out.reshape(batch, patches, dim)

    return jax.shard_map(local_layer, mesh=mesh, in_specs=(P('dp', None, 'm1'), P(), P(), P(), P('m1', None, 'm2'), P('m1', 'm2'), P('m2'), P('m2', 'm1'), P('m2', 'm1'), P('m1')), out_specs=P('dp', None, 'm1'), check_vma=False)
```

```python
import functools

import jax
import jax.numpy as jnp
from jax import lax
from jax.experimental import pallas as pl
from jax.experimental.pallas import tpu as pltpu
from jax.sharding import PartitionSpec as P

LN_EPS = 1e-6
MESH = pl.DeviceIdType.MESH
LANES = 128
AHEAD = 2


def xors(value):
    return (value, value + 1 - 2 * lax.rem(value, 2), value + 2 - 4 * lax.div(value, 2), 3 - value)


def ds(start, size):
    return pl.ds(pl.multiple_of(start, size if size < LANES else LANES), size)


def rows_at(start, size):
    return pl.ds(pl.multiple_of(start, 8), size)


def rcopy(src, dst, send_sem, recv_sem, device):
    return pltpu.make_async_remote_copy(src_ref=src, dst_ref=dst, send_sem=send_sem, recv_sem=recv_sem, device_id=device, device_id_type=MESH)


def dot(lhs, rhs):
    return jnp.dot(lhs, rhs, preferred_element_type=jnp.float32)


def head_norm(values, scale):
    mean = jnp.mean(values, axis=-1, keepdims=True)
    centered = values - mean
    variance = jnp.mean(centered * centered, axis=-1, keepdims=True)
    return (centered * lax.rsqrt(variance + LN_EPS) * scale).astype(jnp.bfloat16)


def kernel(sizes, x, lns, qns, kns, wq, wu, bu, wo, wd, bo,
           out, u, w1, w2, ra,
           xg, ubl, zq, h, rhs, lhs, w2b, pa, po, rav, ss, rb, rc, ud, rd,
           xs, xr, w1s, w1r, f1s, f1r, us, ur, w2s, w2r, f2s, f2r,
           as_, ar, bs, br, cs, cr, dsm, drm, es, er, fr, own_sem, rhs_sem, lhs_sem, ub_sem, w2b_sem, rav_sem):
    batch, patches, dim, qw, uw = sizes
    tokens = batch * patches
    rows = tokens // 4
    block = rows // 2
    half = dim // 2
    total = 4 * dim
    nub = uw // qw
    nc = dim // LANES
    wide = 4 * LANES
    heads = qw // LANES
    ln_rows = min(64, rows)

    g, i, j = lax.axis_index('dp'), lax.axis_index('m1'), lax.axis_index('m2')
    ip, jp = xors(i), xors(j)
    jy, jc = lax.div(j, 2), lax.rem(j, 2)
    mid = lax.div(lax.rem(i + 1, 4), 2)
    peers1 = ((0, ip[1]), (2 - mid, ip[3] + mid * (ip[2] - ip[3])), (1 + mid, ip[2] + mid * (ip[3] - ip[2])))

    barrier = pltpu.get_barrier_semaphore()
    peers = [{'m1': ip[e]} for e in (1, 2, 3)] + [{'m2': jp[e]} for e in (1, 2, 3)] + [{'dp': 1 - g}]
    for peer in peers:
        pl.semaphore_signal(barrier, inc=1, device_id=peer, device_id_type=MESH)
    with jax.named_scope('barrier'):
        pl.semaphore_wait(barrier, len(peers))

    mine = rows_at(j * rows, rows)
    x_far = rcopy(x.at[mine, :], xg.at[i], xs.at[0], xr.at[0], {'m1': ip[2]})
    x_near = rcopy(x.at[mine, :], xg.at[i], xs.at[1], xr.at[1], {'m1': ip[1]})
    x_own = pltpu.make_async_copy(x.at[mine, :], xg.at[i], own_sem.at[0])
    x_far.start()
    x_near.start()
    x_own.start()
    x_far_in = rcopy(xg.at[ip[2]], xg.at[ip[2]], xs.at[0], xr.at[0], {'m1': ip[2]})
    with jax.named_scope('w_xfar'):
        x_far_in.wait_recv()
    x_fwd = rcopy(xg.at[ip[2]], xg.at[ip[2]], xs.at[2], xr.at[2], {'m1': ip[1]})
    x_fwd.start()

    def z1(b, e):
        t = ip[e]
        if b < 3:
            src = wq.at[b, rows_at(g * half, half), ds(t * qw, qw)]
        else:
            src = wu.at[rows_at(g * half, half), ds(t * uw + (b - 3) * qw, qw)]
        return rcopy(src, w1.at[b, rows_at(i * dim + g * half, half), :], w1s.at[0], w1r.at[b, e - 1], {'m1': t})

    def piece1(b, k, s):
        part = w1.at[b, rows_at(s * dim + g * half, half), :]
        return (rcopy(part, part, w1s.at[0], w1r.at[b, k], {'m1': s}), rcopy(part, part, f1s.at[0], f1r.at[b], {'dp': 1 - g}))

    def forward1(b):
        for k, s in peers1:
            arrival, swap = piece1(b, k, s)
            with jax.named_scope('w_z1'):
                arrival.wait_recv()
            swap.start()

    def swapped1(b):
        part = w1.at[b, 0:3 * half, :]
        return rcopy(part, part, f1s.at[0], f1r.at[b], {'dp': 1 - g})

    def issue1(b):
        for e in (2, 3, 1):
            z1(b, e).start()

    issue1(0)
    issue1(1)

    qh, uh = qw // 2, uw // 2

    def z2(c, e):
        t = ip[e]
        cols, to = ds(c * LANES, LANES), ds(i * LANES, LANES)
        return [rcopy(wd.at[rows_at(t * uw + g * uh, uh), cols], w2.at[c, g, qh:qh + uh, to], w2s.at[0], w2r.at[c, e - 1], {'m1': t}),
                rcopy(wo.at[rows_at(t * qw + g * qh, qh), cols], w2.at[c, g, 0:qh, to], w2s.at[0], w2r.at[c, e - 1], {'m1': t})]

    def issue2(c):
        for e in (2, 3, 1):
            for copy in z2(c, e):
                copy.start()

    def forward2(c):
        for k, s in peers1:
            part = w2.at[c, g, :, ds(s * LANES, LANES)]
            with jax.named_scope('w_z2'):
                rcopy(part, part, w2s.at[0], w2r.at[c, k], {'m1': s}).wait_recv()
            rcopy(part, part, f2s.at[0], f2r.at[c], {'dp': 1 - g}).start()

    def next2(c):
        forward2(c)

        @pl.when(c + AHEAD < nc)
        def _():
            issue2(c + AHEAD)

    with jax.named_scope('w_xown'):
        x_own.wait()
    with jax.named_scope('w_xnear'):
        rcopy(xg.at[ip[1]], xg.at[ip[1]], xs.at[1], xr.at[1], {'m1': ip[1]}).wait_recv()
    with jax.named_scope('w_xfwd'):
        rcopy(xg.at[ip[3]], xg.at[ip[3]], xs.at[2], xr.at[2], {'m1': ip[1]}).wait_recv()

    def u_out(r, slot):
        return pltpu.make_async_copy(ubl.at[slot], u.at[rows_at(j * rows + r * ln_rows, ln_rows), :], ub_sem.at[slot])

    @pl.loop(0, rows // ln_rows)
    def _(r):
        slot = lax.rem(r, 2)

        @pl.when(r >= 2)
        def _():
            u_out(r - 2, slot).wait()
        at = rows_at(r * ln_rows, ln_rows)
        parts = [xg[s, at, :].astype(jnp.float32) for s in range(4)]
        mean = sum(jnp.sum(part, axis=-1, keepdims=True) for part in parts) / total
        parts = [part - mean for part in parts]
        variance = sum(jnp.sum(part * part, axis=-1, keepdims=True) for part in parts) / total
        inverse = lax.rsqrt(variance + LN_EPS)
        for s in range(4):
            cols = slice(s * dim, (s + 1) * dim)
            ubl[slot, :, cols] = (parts[s] * inverse * lns[:, cols]).astype(jnp.bfloat16)
        u_out(r, slot).start()

    for r in range(max(0, rows // ln_rows - 2), rows // ln_rows):
        u_out(r, r % 2).wait()

    def u_rows(q):
        return u.at[rows_at(q * rows, rows), :]

    u_far = rcopy(u_rows(j), u_rows(j), us.at[0], ur.at[0], {'m2': jp[2]})
    u_near = rcopy(u_rows(j), u_rows(j), us.at[1], ur.at[1], {'m2': jp[1]})
    u_far.start()
    u_near.start()
    for b in range(4):
        forward1(b)
        issue1(b + 2)
    with jax.named_scope('w_ufar'):
        rcopy(u_rows(jp[2]), u_rows(jp[2]), us.at[0], ur.at[0], {'m2': jp[2]}).wait_recv()
    u_fwd = rcopy(u_rows(jp[2]), u_rows(jp[2]), us.at[2], ur.at[2], {'m2': jp[1]})
    u_fwd.start()
    rcopy(u_rows(jp[1]), u_rows(jp[1]), us.at[1], ur.at[1], {'m2': jp[1]}).wait_recv()
    with jax.named_scope('w_ufwd'):
        rcopy(u_rows(jp[3]), u_rows(jp[3]), us.at[2], ur.at[2], {'m2': jp[1]}).wait_recv()

    def lhs_in(m, slot):
        return pltpu.make_async_copy(u.at[rows_at(m * block, block), :], lhs.at[slot], lhs_sem.at[slot])

    def product1(b, own, store):
        with jax.named_scope('w_f1'):
            swapped1(b).wait_recv()
        loads = [pltpu.make_async_copy(own, rhs.at[rows_at(i * dim, dim), :], rhs_sem.at[0])]
        for e in (1, 2, 3):
            at = rows_at(ip[e] * dim, dim)
            loads.append(pltpu.make_async_copy(w1.at[b, at, :], rhs.at[at, :], rhs_sem.at[e]))
        for load in loads:
            load.start()
        lhs_in(0, 0).start()
        for load in loads:
            load.wait()

        @pl.loop(0, tokens // block)
        def _(m):
            slot = lax.rem(m, 2)
            lhs_in(m, slot).wait()

            @pl.when(m + 1 < tokens // block)
            def _():
                lhs_in(m + 1, 1 - slot).start()
            with jax.named_scope('mm1'):
                store(rows_at(m * block, block), dot(lhs[slot], rhs[...]))

    @pl.loop(0, 3)
    def _(b):
        def store(at, value):
            zq[b, at, :] = value.astype(jnp.bfloat16)
        product1(b, wq.at[b, :, ds(i * qw, qw)], store)

        @pl.when(b == 1)
        def _():
            forward1(4)
            issue1(6)

    @pl.loop(0, batch)
    def _(n):
        at = rows_at(n * patches, patches)
        for head in range(heads):
            cols = slice(head * LANES, (head + 1) * LANES)
            query = head_norm(zq[0, at, cols].astype(jnp.float32), qns[...])
            key = head_norm(zq[1, at, cols].astype(jnp.float32), kns[...])
            scores = lax.dot_general(query, key, (((1,), (1,)), ((), ())), preferred_element_type=jnp.float32) * LANES ** -0.5
            scores = jnp.exp(scores - jnp.max(scores, axis=-1, keepdims=True))
            probs = (scores / jnp.sum(scores, axis=-1, keepdims=True)).astype(jnp.bfloat16)
            with jax.named_scope('attn'):
                h[at, cols] = dot(probs, zq[2, at, cols]).astype(jnp.bfloat16)

    forward1(5)
    for c in range(AHEAD // 2):
        issue2(c)

    @pl.loop(0, nub)
    def _(b):
        def store(at, value):
            value = value.astype(jnp.bfloat16).astype(jnp.float32) + bu[:, ds(i * uw + b * qw, qw)]
            value = 0.5 * value * (1.0 + lax.erf(value * 2.0 ** -0.5))
            h[at, ds(qw + b * qw, qw)] = value.astype(jnp.bfloat16)
        product1(b + 3, wu.at[:, ds(i * uw + b * qw, qw)], store)

        @pl.when(b == 1)
        def _():
            forward1(6)
            for c in range(AHEAD // 2, AHEAD):
                issue2(c)

        @pl.when(b == 2)
        def _():
            next2(0)

        @pl.when(b == 3)
        def _():
            next2(1)

    def quarter(yy, core):
        return (2 * yy + core) * rows

    def send_a(c, yy):
        return rcopy(pa.at[lax.rem(c, 2), yy], ra.at[c, yy], as_.at[lax.rem(c, 2)], ar.at[c], {'m2': jp[1]})

    def all_a(c):
        return rcopy(pa.at[lax.rem(c, 2)], ra.at[c], as_.at[lax.rem(c, 2)], ar.at[c], {'m2': jp[1]})

    def send_b(c):
        return rcopy(ss.at[lax.rem(c, 2)], rb.at[c], bs.at[lax.rem(c, 2)], br.at[c], {'m2': jp[2]})

    def send_c(c, k):
        src = rb.at[c, :, ds(ip[1 + 2 * k] * LANES, LANES)]
        return rcopy(src, rc.at[c, k], cs.at[0], cr.at[c], {'m1': ip[1]})

    def send_d(c):
        return rcopy(ud.at[c], rd.at[c], dsm.at[0], drm.at[c], {'m1': ip[2]})

    def out_part(c, q):
        return out.at[rows_at(q * rows, rows), ds(c * LANES, LANES)]

    def result(c, q, sem, recv, device):
        part = out_part(c, q)
        return rcopy(part, part, es.at[sem], recv, device)

    def product2(c):
        slot = lax.rem(c, 2)
        cols, to = ds(c * LANES, LANES), ds(i * LANES, LANES)
        loads = [pltpu.make_async_copy(wo.at[rows_at(i * qw, qw), cols], w2b.at[slot, 0:qw, to], w2b_sem.at[0]),
                 pltpu.make_async_copy(wd.at[rows_at(i * uw, uw), cols], w2b.at[slot, qw:qw + uw, to], w2b_sem.at[1])]
        for load in loads:
            load.start()
        with jax.named_scope('w_f2'):
            part = w2.at[c, 0, :, 0:3 * LANES]
            rcopy(part, part, f2s.at[0], f2r.at[c], {'dp': 1 - g}).wait_recv()
        for e in (1, 2, 3):
            to = ds(ip[e] * LANES, LANES)
            for k in range(2):
                sems = 2 + 4 * (e - 1) + 2 * k
                loads.append(pltpu.make_async_copy(w2.at[c, k, 0:qh, to], w2b.at[slot, k * qh:(k + 1) * qh, to], w2b_sem.at[sems]))
                loads.append(pltpu.make_async_copy(w2.at[c, k, qh:qh + uh, to], w2b.at[slot, qw + k * uh:qw + (k + 1) * uh, to], w2b_sem.at[sems + 1]))
        for load in loads[2:]:
            load.start()

        @pl.when(c >= 2)
        def _():
            all_a(c - 2).wait_send()
        with jax.named_scope('w_w2b'):
            for load in loads:
                load.wait()
        for yy in range(2):
            for sub in range(2):
                at = rows_at(quarter(yy, 1 - jc) + sub * block, block)
                pa[slot, yy, sub * block:(sub + 1) * block, :] = dot(h[at, :], w2b[slot]).astype(jnp.bfloat16)
            send_a(c, yy).start()
        keep = lax.rem(c, 3)
        for yy in range(2):
            for sub in range(2):
                at = rows_at(quarter(yy, jc) + sub * block, block)
                po[keep, yy, sub * block:(sub + 1) * block, :] = dot(h[at, :], w2b[slot]).astype(jnp.bfloat16)

    def add(a, b):
        return (a.astype(jnp.float32) + b.astype(jnp.float32)).astype(jnp.bfloat16)

    def sum_core(d):
        keep = lax.rem(d, 3)
        with jax.named_scope('w_a'):
            rcopy(ra.at[d], ra.at[d], as_.at[0], ar.at[d], {'m2': jp[1]}).wait_recv()
        load = pltpu.make_async_copy(ra.at[d], rav, rav_sem.at[0])
        load.start()

        @pl.when(d >= 2)
        def _():
            send_b(d - 2).wait_send()
        load.wait()
        ss[lax.rem(d, 2)] = add(po[keep, 1 - jy], rav[1 - jy])
        send_b(d).start()
        po[keep, jy] = add(po[keep, jy], rav[jy])

    def sum_y(d):
        with jax.named_scope('w_b'):
            rcopy(rb.at[d], rb.at[d], bs.at[0], br.at[d], {'m2': jp[2]}).wait_recv()
        rb[d] = add(po[lax.rem(d, 3), jy], rb[d])
        for k in range(2):
            send_c(d, k).start()

    def sum_near(d):
        with jax.named_scope('w_c'):
            rcopy(rc.at[d], rc.at[d], cs.at[0], cr.at[d], {'m1': ip[1]}).wait_recv()
        ud[d] = add(rb[d, :, ds(ip[2] * LANES, LANES)], rc[d, 1])
        send_d(d).start()

    def finish(d):
        with jax.named_scope('w_d'):
            rcopy(rd.at[d], rd.at[d], dsm.at[0], drm.at[d], {'m1': ip[2]}).wait_recv()
        cols = ds(d * LANES, LANES)
        value = rb[d, :, ds(i * LANES, LANES)].astype(jnp.float32) + rc[d, 0].astype(jnp.float32) + rd[d].astype(jnp.float32)
        value = xg[i, :, cols].astype(jnp.float32) + value + bo[cols][None, :]
        out[rows_at(j * rows, rows), cols] = value.astype(jnp.bfloat16)
        result(d, j, 0, er.at[d], {'m2': jp[2]}).start()
        result(d, j, 1, fr.at[0], {'m2': jp[1]}).start()

    def pass_on(d):
        with jax.named_scope('w_e'):
            result(d, jp[2], 0, er.at[d], {'m2': jp[2]}).wait_recv()
        result(d, jp[2], 2, fr.at[1], {'m2': jp[1]}).start()

    def run(step, first, last):
        @pl.loop(max(first, 0), max(last, 0))
        def _(d):
            step(d)

    def late(c, lag, step, last=nc):
        @pl.when((c >= lag) & (c < last))
        def _():
            step(c - lag)

    @pl.loop(0, nc)
    def _(c):
        late(c, 2, sum_y)
        late(c, 1, sum_core)

        @pl.when((c >= 1) & (c + 1 < nc))
        def _():
            next2(c + 1)

        @pl.when((c == nc - 2) & (mid == 1))
        def _():
            run(sum_near, 0, nc - 4)

        @pl.when((c == nc - 1) & (mid == 0))
        def _():
            run(sum_near, 0, nc - 4)

        @pl.when(c == nc - 1)
        def _():
            sum_near(nc - 4)
            run(finish, 0, 2)
        product2(c)

    sum_core(nc - 1)
    sum_y(nc - 2)
    sum_near(nc - 3)
    run(finish, 2, nc - 6)
    sum_y(nc - 1)
    sum_near(nc - 2)
    run(finish, max(nc - 6, 2), nc - 3)
    sum_near(nc - 1)
    run(finish, max(nc - 3, 2), nc)
    run(pass_on, 0, nc)

    with jax.named_scope('drain0'):
      for copy in (x_far, x_near, x_fwd, u_far, u_near, u_fwd):
        copy.wait_send()
    for sem in (w1s, f1s):
        part = w1.at[:, 0:3 * half, :]
        rcopy(part, part, sem.at[0], w1r.at[0, 0], {'dp': 1 - g}).wait_send()
    for sem in (w2s, f2s):
        part = w2.at[:, 0, :, 0:3 * LANES]
        rcopy(part, part, sem.at[0], f2r.at[0], {'dp': 1 - g}).wait_send()
    for c in (nc - 2, nc - 1):
        all_a(c).wait_send()
        send_b(c).wait_send()
    rcopy(rc, rc, cs.at[0], cr.at[0], {'m1': ip[1]}).wait_send()
    for sem in (dsm.at[0], es.at[0], es.at[1], es.at[2]):
        rcopy(rd, rd, sem, drm.at[0], {'m1': ip[2]}).wait_send()
    for k in range(2):
        with jax.named_scope('w_f'):
            rcopy(rd, rd, es.at[1], fr.at[k], {'m2': jp[1]}).wait_recv()


def solution(mesh):
    assert mesh.shape['m1'] == 4 and mesh.shape['m2'] == 4 and mesh.shape['dp'] == 2

    def local_layer(x_blk, ln_scale, qn_scale, kn_scale, w_qkv, w_up, b_up, w_o, w_down, b_out):
        batch, patches, dim = x_blk.shape
        tokens = batch * patches
        qw, uw = w_qkv.shape[2] // 4, w_up.shape[1] // 4
        rows, block, nc, nb = tokens // 4, tokens // 8, dim // LANES, 3 + uw // qw
        assert qn_scale.shape[0] == LANES and uw % qw == 0 and nb == 7
        wide = 4 * LANES
        bf16 = jnp.bfloat16
        dma = pltpu.SemaphoreType.DMA
        hbm = pl.BlockSpec(memory_space=pltpu.HBM)
        vmem = pl.BlockSpec(memory_space=pltpu.VMEM)
        ln_rows = min(64, rows)
        out = pl.pallas_call(
            functools.partial(kernel, (batch, patches, dim, qw, uw)),
            out_shape=[
                pltpu.VMEM((tokens, dim), bf16),
                jax.ShapeDtypeStruct((tokens, 4 * dim), bf16),
                jax.ShapeDtypeStruct((nb, 4 * dim, qw), bf16),
                jax.ShapeDtypeStruct((nc, 2, (qw + uw) // 2, wide), bf16),
                jax.ShapeDtypeStruct((nc, 2, rows, wide), bf16)],
            in_specs=[hbm, vmem, vmem, vmem, hbm, hbm, vmem, hbm, hbm, vmem],
            out_specs=[vmem] + [hbm] * 4,
            scratch_shapes=[
                pltpu.VMEM((4, rows, dim), bf16),
                pltpu.VMEM((2, ln_rows, 4 * dim), bf16),
                pltpu.VMEM((3, tokens, qw), bf16),
                pltpu.VMEM((tokens, qw + uw), bf16),
                pltpu.VMEM((4 * dim, qw), bf16),
                pltpu.VMEM((2, block, 4 * dim), bf16),
                pltpu.VMEM((2, qw + uw, wide), bf16),
                pltpu.VMEM((2, 2, rows, wide), bf16),
                pltpu.VMEM((3, 2, rows, wide), bf16),
                pltpu.VMEM((2, rows, wide), bf16),
                pltpu.VMEM((2, rows, wide), bf16),
                pltpu.VMEM((nc, rows, wide), bf16),
                pltpu.VMEM((nc, 2, rows, LANES), bf16),
                pltpu.VMEM((nc, rows, LANES), bf16),
                pltpu.VMEM((nc, rows, LANES), bf16),
                dma((3,)), dma((3,)),
                dma((1,)), dma((nb, 3)), dma((1,)), dma((nb,)),
                dma((3,)), dma((3,)),
                dma((1,)), dma((nc, 3)), dma((1,)), dma((nc,)),
                dma((2,)), dma((nc,)), dma((2,)), dma((nc,)), dma((1,)), dma((nc,)), dma((1,)), dma((nc,)),
                dma((3,)), dma((nc,)), dma((2,)),
                dma((1,)), dma((4,)), dma((2,)), dma((2,)), dma((14,)), dma((1,))],
            compiler_params=pltpu.CompilerParams(collective_id=0, has_side_effects=True, vmem_limit_bytes=60_000_000),
            name='layer',
        )(x_blk.reshape(tokens, dim), ln_scale[None], qn_scale[None], kn_scale[None], w_qkv.transpose(1, 0, 2), w_up,
          b_up[None], w_o, w_down, b_out)[0]
        return out.reshape(batch, patches, dim)

    return jax.shard_map(local_layer, mesh=mesh, in_specs=(P('dp', None, 'm1'), P(), P(), P(), P('m1', None, 'm2'), P('m1', 'm2'), P('m2'), P('m2', 'm1'), P('m2', 'm1'), P('m1')), out_specs=P('dp', None, 'm1'), check_vma=False)
```

```python
import functools

import jax
import jax.numpy as jnp
from jax import lax
from jax.experimental import pallas as pl
from jax.experimental.pallas import tpu as pltpu
from jax.sharding import PartitionSpec as P

LN_EPS = 1e-6
MESH = pl.DeviceIdType.MESH
LANES = 128
AHEAD = 2


def xors(value):
    return (value, value + 1 - 2 * lax.rem(value, 2), value + 2 - 4 * lax.div(value, 2), 3 - value)


def ds(start, size):
    return pl.ds(pl.multiple_of(start, size if size < LANES else LANES), size)


def rows_at(start, size):
    return pl.ds(pl.multiple_of(start, 8), size)


def rcopy(src, dst, send_sem, recv_sem, device):
    return pltpu.make_async_remote_copy(src_ref=src, dst_ref=dst, send_sem=send_sem, recv_sem=recv_sem, device_id=device, device_id_type=MESH)


def dot(lhs, rhs):
    return jnp.dot(lhs, rhs, preferred_element_type=jnp.float32)


def head_norm(values, scale):
    mean = jnp.mean(values, axis=-1, keepdims=True)
    centered = values - mean
    variance = jnp.mean(centered * centered, axis=-1, keepdims=True)
    return (centered * lax.rsqrt(variance + LN_EPS) * scale).astype(jnp.bfloat16)


def kernel(sizes, x, lns, qns, kns, wq, wu, bu, wo, wd, bo,
           out, u, w1, w2, ra,
           xg, ubl, zq, h, rhs, lhs, w2b, pa, po, rav, ss, rb, rc, ud, rd,
           xs, xr, w1s, w1r, f1s, f1r, us, ur, w2s, w2r, f2s, f2r,
           as_, ar, bs, br, cs, cr, dsm, drm, es, er, fr, own_sem, rhs_sem, lhs_sem, ub_sem, w2b_sem, rav_sem):
    batch, patches, dim, qw, uw = sizes
    tokens = batch * patches
    rows = tokens // 4
    block = rows // 2
    half = dim // 2
    total = 4 * dim
    nub = uw // qw
    nc = dim // LANES
    wide = 4 * LANES
    heads = qw // LANES
    ln_rows = min(64, rows)

    g, i, j = lax.axis_index('dp'), lax.axis_index('m1'), lax.axis_index('m2')
    ip, jp = xors(i), xors(j)
    jy, jc = lax.div(j, 2), lax.rem(j, 2)
    mid = lax.div(lax.rem(i + 1, 4), 2)
    peers1 = ((0, ip[1]), (2 - mid, ip[3] + mid * (ip[2] - ip[3])), (1 + mid, ip[2] + mid * (ip[3] - ip[2])))

    barrier = pltpu.get_barrier_semaphore()
    peers = [{'m1': ip[e]} for e in (1, 2, 3)] + [{'m2': jp[e]} for e in (1, 2, 3)] + [{'dp': 1 - g}]
    for peer in peers:
        pl.semaphore_signal(barrier, inc=1, device_id=peer, device_id_type=MESH)
    with jax.named_scope('barrier'):
        pl.semaphore_wait(barrier, len(peers))

    mine = rows_at(j * rows, rows)
    x_far = rcopy(x.at[mine, :], xg.at[i], xs.at[0], xr.at[0], {'m1': ip[2]})
    x_near = rcopy(x.at[mine, :], xg.at[i], xs.at[1], xr.at[1], {'m1': ip[1]})
    x_own = pltpu.make_async_copy(x.at[mine, :], xg.at[i], own_sem.at[0])
    x_far.start()
    x_near.start()
    x_own.start()
    x_far_in = rcopy(xg.at[ip[2]], xg.at[ip[2]], xs.at[0], xr.at[0], {'m1': ip[2]})
    with jax.named_scope('w_xfar'):
        x_far_in.wait_recv()
    x_fwd = rcopy(xg.at[ip[2]], xg.at[ip[2]], xs.at[2], xr.at[2], {'m1': ip[1]})
    x_fwd.start()

    def z1(b, e):
        t = ip[e]
        if b < 3:
            src = wq.at[b, rows_at(g * half, half), ds(t * qw, qw)]
        else:
            src = wu.at[rows_at(g * half, half), ds(t * uw + (b - 3) * qw, qw)]
        return rcopy(src, w1.at[b, rows_at(i * dim + g * half, half), :], w1s.at[0], w1r.at[b, e - 1], {'m1': t})

    def piece1(b, k, s):
        part = w1.at[b, rows_at(s * dim + g * half, half), :]
        return (rcopy(part, part, w1s.at[0], w1r.at[b, k], {'m1': s}), rcopy(part, part, f1s.at[0], f1r.at[b], {'dp': 1 - g}))

    def forward1(b):
        for k, s in peers1:
            arrival, swap = piece1(b, k, s)
            with jax.named_scope('w_z1'):
                arrival.wait_recv()
            swap.start()

    def swapped1(b):
        part = w1.at[b, 0:3 * half, :]
        return rcopy(part, part, f1s.at[0], f1r.at[b], {'dp': 1 - g})

    def issue1(b):
        for e in (2, 3, 1):
            z1(b, e).start()

    issue1(0)
    issue1(1)

    qh, uh = qw // 2, uw // 2

    def z2(c, e):
        t = ip[e]
        cols, to = ds(c * LANES, LANES), ds(i * LANES, LANES)
        return [rcopy(wd.at[rows_at(t * uw + g * uh, uh), cols], w2.at[c, g, qh:qh + uh, to], w2s.at[0], w2r.at[c, e - 1], {'m1': t}),
                rcopy(wo.at[rows_at(t * qw + g * qh, qh), cols], w2.at[c, g, 0:qh, to], w2s.at[0], w2r.at[c, e - 1], {'m1': t})]

    def issue2(c):
        for e in (2, 3, 1):
            for copy in z2(c, e):
                copy.start()

    def forward2(c):
        for k, s in peers1:
            part = w2.at[c, g, :, ds(s * LANES, LANES)]
            with jax.named_scope('w_z2'):
                rcopy(part, part, w2s.at[0], w2r.at[c, k], {'m1': s}).wait_recv()
            rcopy(part, part, f2s.at[0], f2r.at[c], {'dp': 1 - g}).start()

    def next2(c):
        forward2(c)

        @pl.when(c + AHEAD < nc)
        def _():
            issue2(c + AHEAD)

    with jax.named_scope('w_xown'):
        x_own.wait()
    with jax.named_scope('w_xnear'):
        rcopy(xg.at[ip[1]], xg.at[ip[1]], xs.at[1], xr.at[1], {'m1': ip[1]}).wait_recv()
    with jax.named_scope('w_xfwd'):
        rcopy(xg.at[ip[3]], xg.at[ip[3]], xs.at[2], xr.at[2], {'m1': ip[1]}).wait_recv()

    def u_out(r, slot):
        return pltpu.make_async_copy(ubl.at[slot], u.at[rows_at(j * rows + r * ln_rows, ln_rows), :], ub_sem.at[slot])

    @pl.loop(0, rows // ln_rows)
    def _(r):
        slot = lax.rem(r, 2)

        @pl.when(r >= 2)
        def _():
            u_out(r - 2, slot).wait()
        at = rows_at(r * ln_rows, ln_rows)
        parts = [xg[s, at, :].astype(jnp.float32) for s in range(4)]
        mean = sum(jnp.sum(part, axis=-1, keepdims=True) for part in parts) / total
        parts = [part - mean for part in parts]
        variance = sum(jnp.sum(part * part, axis=-1, keepdims=True) for part in parts) / total
        inverse = lax.rsqrt(variance + LN_EPS)
        for s in range(4):
            cols = slice(s * dim, (s + 1) * dim)
            ubl[slot, :, cols] = (parts[s] * inverse * lns[:, cols]).astype(jnp.bfloat16)
        u_out(r, slot).start()

    for r in range(max(0, rows // ln_rows - 2), rows // ln_rows):
        u_out(r, r % 2).wait()

    def u_rows(q):
        return u.at[rows_at(q * rows, rows), :]

    u_far = rcopy(u_rows(j), u_rows(j), us.at[0], ur.at[0], {'m2': jp[2]})
    u_near = rcopy(u_rows(j), u_rows(j), us.at[1], ur.at[1], {'m2': jp[1]})
    u_far.start()
    u_near.start()
    for b in range(4):
        forward1(b)
        issue1(b + 2)
    with jax.named_scope('w_ufar'):
        rcopy(u_rows(jp[2]), u_rows(jp[2]), us.at[0], ur.at[0], {'m2': jp[2]}).wait_recv()
    u_fwd = rcopy(u_rows(jp[2]), u_rows(jp[2]), us.at[2], ur.at[2], {'m2': jp[1]})
    u_fwd.start()
    rcopy(u_rows(jp[1]), u_rows(jp[1]), us.at[1], ur.at[1], {'m2': jp[1]}).wait_recv()
    with jax.named_scope('w_ufwd'):
        rcopy(u_rows(jp[3]), u_rows(jp[3]), us.at[2], ur.at[2], {'m2': jp[1]}).wait_recv()

    def lhs_in(m, slot):
        return pltpu.make_async_copy(u.at[rows_at(m * block, block), :], lhs.at[slot], lhs_sem.at[slot])

    def product1(b, own, store):
        with jax.named_scope('w_f1'):
            swapped1(b).wait_recv()
        loads = [pltpu.make_async_copy(own, rhs.at[rows_at(i * dim, dim), :], rhs_sem.at[0])]
        for e in (1, 2, 3):
            at = rows_at(ip[e] * dim, dim)
            loads.append(pltpu.make_async_copy(w1.at[b, at, :], rhs.at[at, :], rhs_sem.at[e]))
        for load in loads:
            load.start()
        lhs_in(0, 0).start()
        for load in loads:
            load.wait()

        @pl.loop(0, tokens // block)
        def _(m):
            slot = lax.rem(m, 2)
            lhs_in(m, slot).wait()

            @pl.when(m + 1 < tokens // block)
            def _():
                lhs_in(m + 1, 1 - slot).start()
            with jax.named_scope('mm1'):
                store(rows_at(m * block, block), dot(lhs[slot], rhs[...]))

    @pl.loop(0, 3)
    def _(b):
        def store(at, value):
            zq[b, at, :] = value.astype(jnp.bfloat16)
        product1(b, wq.at[b, :, ds(i * qw, qw)], store)

        @pl.when(b == 1)
        def _():
            forward1(4)
            issue1(6)

    @pl.loop(0, batch)
    def _(n):
        at = rows_at(n * patches, patches)
        for head in range(heads):
            cols = slice(head * LANES, (head + 1) * LANES)
            query = head_norm(zq[0, at, cols].astype(jnp.float32), qns[...])
            key = head_norm(zq[1, at, cols].astype(jnp.float32), kns[...])
            scores = lax.dot_general(query, key, (((1,), (1,)), ((), ())), preferred_element_type=jnp.float32) * LANES ** -0.5
            scores = jnp.exp(scores - jnp.max(scores, axis=-1, keepdims=True))
            probs = (scores / jnp.sum(scores, axis=-1, keepdims=True)).astype(jnp.bfloat16)
            with jax.named_scope('attn'):
                h[at, cols] = dot(probs, zq[2, at, cols]).astype(jnp.bfloat16)

    forward1(5)
    for c in range(AHEAD // 2):
        issue2(c)

    @pl.loop(0, nub)
    def _(b):
        def store(at, value):
            value = value.astype(jnp.bfloat16).astype(jnp.float32) + bu[:, ds(i * uw + b * qw, qw)]
            value = 0.5 * value * (1.0 + lax.erf(value * 2.0 ** -0.5))
            h[at, ds(qw + b * qw, qw)] = value.astype(jnp.bfloat16)
        product1(b + 3, wu.at[:, ds(i * uw + b * qw, qw)], store)

        @pl.when(b == 1)
        def _():
            forward1(6)
            for c in range(AHEAD // 2, AHEAD):
                issue2(c)

        @pl.when(b == 2)
        def _():
            next2(0)

        @pl.when(b == 3)
        def _():
            next2(1)

    def quarter(yy, core):
        return (2 * yy + core) * rows

    def send_a(c, yy):
        return rcopy(pa.at[lax.rem(c, 2), yy], ra.at[c, yy], as_.at[lax.rem(c, 2)], ar.at[c], {'m2': jp[1]})

    def all_a(c):
        return rcopy(pa.at[lax.rem(c, 2)], ra.at[c], as_.at[lax.rem(c, 2)], ar.at[c], {'m2': jp[1]})

    def send_b(c):
        return rcopy(ss.at[lax.rem(c, 2)], rb.at[c], bs.at[lax.rem(c, 2)], br.at[c], {'m2': jp[2]})

    def send_c(c, k):
        src = rb.at[c, :, ds(ip[1 + 2 * k] * LANES, LANES)]
        return rcopy(src, rc.at[c, k], cs.at[0], cr.at[c], {'m1': ip[1]})

    def send_d(c):
        return rcopy(ud.at[c], rd.at[c], dsm.at[0], drm.at[c], {'m1': ip[2]})

    def out_part(c, q):
        return out.at[rows_at(q * rows, rows), ds(c * LANES, LANES)]

    def result(c, q, sem, recv, device):
        part = out_part(c, q)
        return rcopy(part, part, es.at[sem], recv, device)

    def product2(c):
        slot = lax.rem(c, 2)
        cols, to = ds(c * LANES, LANES), ds(i * LANES, LANES)
        loads = [pltpu.make_async_copy(wo.at[rows_at(i * qw, qw), cols], w2b.at[slot, 0:qw, to], w2b_sem.at[0]),
                 pltpu.make_async_copy(wd.at[rows_at(i * uw, uw), cols], w2b.at[slot, qw:qw + uw, to], w2b_sem.at[1])]
        for load in loads:
            load.start()
        with jax.named_scope('w_f2'):
            part = w2.at[c, 0, :, 0:3 * LANES]
            rcopy(part, part, f2s.at[0], f2r.at[c], {'dp': 1 - g}).wait_recv()
        for e in (1, 2, 3):
            to = ds(ip[e] * LANES, LANES)
            for k in range(2):
                sems = 2 + 4 * (e - 1) + 2 * k
                loads.append(pltpu.make_async_copy(w2.at[c, k, 0:qh, to], w2b.at[slot, k * qh:(k + 1) * qh, to], w2b_sem.at[sems]))
                loads.append(pltpu.make_async_copy(w2.at[c, k, qh:qh + uh, to], w2b.at[slot, qw + k * uh:qw + (k + 1) * uh, to], w2b_sem.at[sems + 1]))
        for load in loads[2:]:
            load.start()

        @pl.when(c >= 2)
        def _():
            all_a(c - 2).wait_send()
        with jax.named_scope('w_w2b'):
            for load in loads:
                load.wait()
        for yy in range(2):
            for sub in range(2):
                at = rows_at(quarter(yy, 1 - jc) + sub * block, block)
                pa[slot, yy, sub * block:(sub + 1) * block, :] = dot(h[at, :], w2b[slot]).astype(jnp.bfloat16)
            send_a(c, yy).start()
        keep = lax.rem(c, 3)
        for yy in range(2):
            for sub in range(2):
                at = rows_at(quarter(yy, jc) + sub * block, block)
                po[keep, yy, sub * block:(sub + 1) * block, :] = dot(h[at, :], w2b[slot]).astype(jnp.bfloat16)

    def add(a, b):
        return (a.astype(jnp.float32) + b.astype(jnp.float32)).astype(jnp.bfloat16)

    def sum_core(d):
        keep = lax.rem(d, 3)
        with jax.named_scope('w_a'):
            rcopy(ra.at[d], ra.at[d], as_.at[0], ar.at[d], {'m2': jp[1]}).wait_recv()
        load = pltpu.make_async_copy(ra.at[d], rav, rav_sem.at[0])
        load.start()

        @pl.when(d >= 2)
        def _():
            send_b(d - 2).wait_send()
        load.wait()
        ss[lax.rem(d, 2)] = add(po[keep, 1 - jy], rav[1 - jy])
        send_b(d).start()
        po[keep, jy] = add(po[keep, jy], rav[jy])

    def sum_y(d):
        with jax.named_scope('w_b'):
            rcopy(rb.at[d], rb.at[d], bs.at[0], br.at[d], {'m2': jp[2]}).wait_recv()
        rb[d] = add(po[lax.rem(d, 3), jy], rb[d])
        for k in range(2):
            send_c(d, k).start()

    def sum_near(d):
        with jax.named_scope('w_c'):
            rcopy(rc.at[d], rc.at[d], cs.at[0], cr.at[d], {'m1': ip[1]}).wait_recv()
        ud[d] = add(rb[d, :, ds(ip[2] * LANES, LANES)], rc[d, 1])
        send_d(d).start()

    def finish(d):
        with jax.named_scope('w_d'):
            rcopy(rd.at[d], rd.at[d], dsm.at[0], drm.at[d], {'m1': ip[2]}).wait_recv()
        cols = ds(d * LANES, LANES)
        value = rb[d, :, ds(i * LANES, LANES)].astype(jnp.float32) + rc[d, 0].astype(jnp.float32) + rd[d].astype(jnp.float32)
        value = xg[i, :, cols].astype(jnp.float32) + value + bo[cols][None, :]
        out[rows_at(j * rows, rows), cols] = value.astype(jnp.bfloat16)
        result(d, j, 0, er.at[d], {'m2': jp[2]}).start()
        result(d, j, 1, fr.at[0], {'m2': jp[1]}).start()

    def pass_on(d):
        with jax.named_scope('w_e'):
            result(d, jp[2], 0, er.at[d], {'m2': jp[2]}).wait_recv()
        result(d, jp[2], 2, fr.at[1], {'m2': jp[1]}).start()

    def run(step, first, last):
        @pl.loop(max(first, 0), max(last, 0))
        def _(d):
            step(d)

    def late(c, lag, step, last=nc):
        @pl.when((c >= lag) & (c < last))
        def _():
            step(c - lag)

    @pl.loop(0, nc)
    def _(c):
        late(c, 2, sum_y)
        late(c, 1, sum_core)

        @pl.when((c >= 1) & (c + 1 < nc))
        def _():
            next2(c + 1)

        @pl.when((c == nc - 2) & (mid == 1))
        def _():
            run(sum_near, 0, 2)

        @pl.when((c == nc - 1) & (mid == 0))
        def _():
            run(sum_near, 0, 2)

        @pl.when(c == nc - 1)
        def _():
            run(sum_near, 2, nc - 6)
            finish(0)
        product2(c)

    sum_core(nc - 1)
    run(sum_near, max(nc - 6, 2), nc - 3)
    sum_y(nc - 2)
    sum_near(nc - 3)
    run(finish, 1, nc - 6)
    sum_y(nc - 1)
    sum_near(nc - 2)
    run(finish, max(nc - 6, 1), nc - 3)
    sum_near(nc - 1)
    run(finish, max(nc - 3, 1), nc)
    run(pass_on, 0, nc)

    with jax.named_scope('drain0'):
      for copy in (x_far, x_near, x_fwd, u_far, u_near, u_fwd):
        copy.wait_send()
    for sem in (w1s, f1s):
        part = w1.at[:, 0:3 * half, :]
        rcopy(part, part, sem.at[0], w1r.at[0, 0], {'dp': 1 - g}).wait_send()
    for sem in (w2s, f2s):
        part = w2.at[:, 0, :, 0:3 * LANES]
        rcopy(part, part, sem.at[0], f2r.at[0], {'dp': 1 - g}).wait_send()
    for c in (nc - 2, nc - 1):
        all_a(c).wait_send()
        send_b(c).wait_send()
    rcopy(rc, rc, cs.at[0], cr.at[0], {'m1': ip[1]}).wait_send()
    for sem in (dsm.at[0], es.at[0], es.at[1], es.at[2]):
        rcopy(rd, rd, sem, drm.at[0], {'m1': ip[2]}).wait_send()
    for k in range(2):
        with jax.named_scope('w_f'):
            rcopy(rd, rd, es.at[1], fr.at[k], {'m2': jp[1]}).wait_recv()


def solution(mesh):
    assert mesh.shape['m1'] == 4 and mesh.shape['m2'] == 4 and mesh.shape['dp'] == 2

    def local_layer(x_blk, ln_scale, qn_scale, kn_scale, w_qkv, w_up, b_up, w_o, w_down, b_out):
        batch, patches, dim = x_blk.shape
        tokens = batch * patches
        qw, uw = w_qkv.shape[2] // 4, w_up.shape[1] // 4
        rows, block, nc, nb = tokens // 4, tokens // 8, dim // LANES, 3 + uw // qw
        assert qn_scale.shape[0] == LANES and uw % qw == 0 and nb == 7
        wide = 4 * LANES
        bf16 = jnp.bfloat16
        dma = pltpu.SemaphoreType.DMA
        hbm = pl.BlockSpec(memory_space=pltpu.HBM)
        vmem = pl.BlockSpec(memory_space=pltpu.VMEM)
        ln_rows = min(64, rows)
        out = pl.pallas_call(
            functools.partial(kernel, (batch, patches, dim, qw, uw)),
            out_shape=[
                pltpu.VMEM((tokens, dim), bf16),
                jax.ShapeDtypeStruct((tokens, 4 * dim), bf16),
                jax.ShapeDtypeStruct((nb, 4 * dim, qw), bf16),
                jax.ShapeDtypeStruct((nc, 2, (qw + uw) // 2, wide), bf16),
                jax.ShapeDtypeStruct((nc, 2, rows, wide), bf16)],
            in_specs=[hbm, vmem, vmem, vmem, hbm, hbm, vmem, hbm, hbm, vmem],
            out_specs=[vmem] + [hbm] * 4,
            scratch_shapes=[
                pltpu.VMEM((4, rows, dim), bf16),
                pltpu.VMEM((2, ln_rows, 4 * dim), bf16),
                pltpu.VMEM((3, tokens, qw), bf16),
                pltpu.VMEM((tokens, qw + uw), bf16),
                pltpu.VMEM((4 * dim, qw), bf16),
                pltpu.VMEM((2, block, 4 * dim), bf16),
                pltpu.VMEM((2, qw + uw, wide), bf16),
                pltpu.VMEM((2, 2, rows, wide), bf16),
                pltpu.VMEM((3, 2, rows, wide), bf16),
                pltpu.VMEM((2, rows, wide), bf16),
                pltpu.VMEM((2, rows, wide), bf16),
                pltpu.VMEM((nc, rows, wide), bf16),
                pltpu.VMEM((nc, 2, rows, LANES), bf16),
                pltpu.VMEM((nc, rows, LANES), bf16),
                pltpu.VMEM((nc, rows, LANES), bf16),
                dma((3,)), dma((3,)),
                dma((1,)), dma((nb, 3)), dma((1,)), dma((nb,)),
                dma((3,)), dma((3,)),
                dma((1,)), dma((nc, 3)), dma((1,)), dma((nc,)),
                dma((2,)), dma((nc,)), dma((2,)), dma((nc,)), dma((1,)), dma((nc,)), dma((1,)), dma((nc,)),
                dma((3,)), dma((nc,)), dma((2,)),
                dma((1,)), dma((4,)), dma((2,)), dma((2,)), dma((14,)), dma((1,))],
            compiler_params=pltpu.CompilerParams(collective_id=0, has_side_effects=True, vmem_limit_bytes=60_000_000),
            name='layer',
        )(x_blk.reshape(tokens, dim), ln_scale[None], qn_scale[None], kn_scale[None], w_qkv.transpose(1, 0, 2), w_up,
          b_up[None], w_o, w_down, b_out)[0]
        return out.reshape(batch, patches, dim)

    return jax.shard_map(local_layer, mesh=mesh, in_specs=(P('dp', None, 'm1'), P(), P(), P(), P('m1', None, 'm2'), P('m1', 'm2'), P('m2'), P('m2', 'm1'), P('m2', 'm1'), P('m1')), out_specs=P('dp', None, 'm1'), check_vma=False)
```

```python
import functools

import jax
import jax.numpy as jnp
from jax import lax
from jax.experimental import pallas as pl
from jax.experimental.pallas import tpu as pltpu
from jax.sharding import PartitionSpec as P

LN_EPS = 1e-6
MESH = pl.DeviceIdType.MESH
LANES = 128
AHEAD = 2


def xors(value):
    return (value, value + 1 - 2 * lax.rem(value, 2), value + 2 - 4 * lax.div(value, 2), 3 - value)


def ds(start, size):
    return pl.ds(pl.multiple_of(start, size if size < LANES else LANES), size)


def rows_at(start, size):
    return pl.ds(pl.multiple_of(start, 8), size)


def rcopy(src, dst, send_sem, recv_sem, device):
    return pltpu.make_async_remote_copy(src_ref=src, dst_ref=dst, send_sem=send_sem, recv_sem=recv_sem, device_id=device, device_id_type=MESH)


def dot(lhs, rhs):
    return jnp.dot(lhs, rhs, preferred_element_type=jnp.float32)


def head_norm(values, scale):
    mean = jnp.mean(values, axis=-1, keepdims=True)
    centered = values - mean
    variance = jnp.mean(centered * centered, axis=-1, keepdims=True)
    return (centered * lax.rsqrt(variance + LN_EPS) * scale).astype(jnp.bfloat16)


def kernel(sizes, x, lns, qns, kns, wq, wu, bu, wo, wd, bo,
           out, u, w1, w2, ra,
           xg, ubl, zq, h, rhs, lhs, w2b, pa, po, rav, ss, rb, rc, ud, rd,
           xs, xr, w1s, w1r, f1s, f1r, us, ur, w2s, w2r, f2s, f2r,
           as_, ar, bs, br, cs, cr, dsm, drm, es, er, fr, own_sem, rhs_sem, lhs_sem, ub_sem, w2b_sem, rav_sem):
    batch, patches, dim, qw, uw = sizes
    tokens = batch * patches
    rows = tokens // 4
    block = rows // 2
    half = dim // 2
    total = 4 * dim
    nub = uw // qw
    nc = dim // LANES
    wide = 4 * LANES
    heads = qw // LANES
    ln_rows = min(64, rows)

    g, i, j = lax.axis_index('dp'), lax.axis_index('m1'), lax.axis_index('m2')
    ip, jp = xors(i), xors(j)
    jy, jc = lax.div(j, 2), lax.rem(j, 2)
    mid = lax.div(lax.rem(i + 1, 4), 2)
    peers1 = ((0, ip[1]), (2 - mid, ip[3] + mid * (ip[2] - ip[3])), (1 + mid, ip[2] + mid * (ip[3] - ip[2])))

    barrier = pltpu.get_barrier_semaphore()
    peers = [{'m1': ip[e]} for e in (1, 2, 3)] + [{'m2': jp[e]} for e in (1, 2, 3)] + [{'dp': 1 - g}]
    for peer in peers:
        pl.semaphore_signal(barrier, inc=1, device_id=peer, device_id_type=MESH)
    with jax.named_scope('barrier'):
        pl.semaphore_wait(barrier, len(peers))

    mine = rows_at(j * rows, rows)
    x_far = rcopy(x.at[mine, :], xg.at[i], xs.at[0], xr.at[0], {'m1': ip[2]})
    x_near = rcopy(x.at[mine, :], xg.at[i], xs.at[1], xr.at[1], {'m1': ip[1]})
    x_own = pltpu.make_async_copy(x.at[mine, :], xg.at[i], own_sem.at[0])
    x_far.start()
    x_near.start()
    x_own.start()
    x_far_in = rcopy(xg.at[ip[2]], xg.at[ip[2]], xs.at[0], xr.at[0], {'m1': ip[2]})
    with jax.named_scope('w_xfar'):
        x_far_in.wait_recv()
    x_fwd = rcopy(xg.at[ip[2]], xg.at[ip[2]], xs.at[2], xr.at[2], {'m1': ip[1]})
    x_fwd.start()

    def z1(b, e):
        t = ip[e]
        if b < 3:
            src = wq.at[b, rows_at(g * half, half), ds(t * qw, qw)]
        else:
            src = wu.at[rows_at(g * half, half), ds(t * uw + (b - 3) * qw, qw)]
        return rcopy(src, w1.at[b, rows_at(i * dim + g * half, half), :], w1s.at[0], w1r.at[b, e - 1], {'m1': t})

    def piece1(b, k, s):
        part = w1.at[b, rows_at(s * dim + g * half, half), :]
        return (rcopy(part, part, w1s.at[0], w1r.at[b, k], {'m1': s}), rcopy(part, part, f1s.at[0], f1r.at[b], {'dp': 1 - g}))

    def forward1(b):
        for k, s in peers1:
            arrival, swap = piece1(b, k, s)
            with jax.named_scope('w_z1'):
                arrival.wait_recv()
            swap.start()

    def swapped1(b):
        part = w1.at[b, 0:3 * half, :]
        return rcopy(part, part, f1s.at[0], f1r.at[b], {'dp': 1 - g})

    def issue1(b):
        for e in (2, 3, 1):
            z1(b, e).start()

    issue1(0)
    issue1(1)

    qh, uh = qw // 2, uw // 2

    def z2(c, e):
        t = ip[e]
        cols, to = ds(c * LANES, LANES), ds(i * LANES, LANES)
        return [rcopy(wd.at[rows_at(t * uw + g * uh, uh), cols], w2.at[c, g, qh:qh + uh, to], w2s.at[0], w2r.at[c, e - 1], {'m1': t}),
                rcopy(wo.at[rows_at(t * qw + g * qh, qh), cols], w2.at[c, g, 0:qh, to], w2s.at[0], w2r.at[c, e - 1], {'m1': t})]

    def issue2(c):
        for e in (2, 3, 1):
            for copy in z2(c, e):
                copy.start()

    def forward2(c):
        for k, s in peers1:
            part = w2.at[c, g, :, ds(s * LANES, LANES)]
            with jax.named_scope('w_z2'):
                rcopy(part, part, w2s.at[0], w2r.at[c, k], {'m1': s}).wait_recv()
            rcopy(part, part, f2s.at[0], f2r.at[c], {'dp': 1 - g}).start()

    def next2(c):
        forward2(c)

        @pl.when(c + AHEAD < nc)
        def _():
            issue2(c + AHEAD)

    with jax.named_scope('w_xown'):
        x_own.wait()
    with jax.named_scope('w_xnear'):
        rcopy(xg.at[ip[1]], xg.at[ip[1]], xs.at[1], xr.at[1], {'m1': ip[1]}).wait_recv()
    with jax.named_scope('w_xfwd'):
        rcopy(xg.at[ip[3]], xg.at[ip[3]], xs.at[2], xr.at[2], {'m1': ip[1]}).wait_recv()

    def u_out(r, slot):
        return pltpu.make_async_copy(ubl.at[slot], u.at[rows_at(j * rows + r * ln_rows, ln_rows), :], ub_sem.at[slot])

    @pl.loop(0, rows // ln_rows)
    def _(r):
        slot = lax.rem(r, 2)

        @pl.when(r >= 2)
        def _():
            u_out(r - 2, slot).wait()
        at = rows_at(r * ln_rows, ln_rows)
        parts = [xg[s, at, :].astype(jnp.float32) for s in range(4)]
        mean = sum(jnp.sum(part, axis=-1, keepdims=True) for part in parts) / total
        parts = [part - mean for part in parts]
        variance = sum(jnp.sum(part * part, axis=-1, keepdims=True) for part in parts) / total
        inverse = lax.rsqrt(variance + LN_EPS)
        for s in range(4):
            cols = slice(s * dim, (s + 1) * dim)
            ubl[slot, :, cols] = (parts[s] * inverse * lns[:, cols]).astype(jnp.bfloat16)
        u_out(r, slot).start()

    for r in range(max(0, rows // ln_rows - 2), rows // ln_rows):
        u_out(r, r % 2).wait()

    def u_rows(q):
        return u.at[rows_at(q * rows, rows), :]

    u_far = rcopy(u_rows(j), u_rows(j), us.at[0], ur.at[0], {'m2': jp[2]})
    u_near = rcopy(u_rows(j), u_rows(j), us.at[1], ur.at[1], {'m2': jp[1]})
    u_far.start()
    u_near.start()
    for b in range(4):
        forward1(b)
        issue1(b + 2)
    with jax.named_scope('w_ufar'):
        rcopy(u_rows(jp[2]), u_rows(jp[2]), us.at[0], ur.at[0], {'m2': jp[2]}).wait_recv()
    u_fwd = rcopy(u_rows(jp[2]), u_rows(jp[2]), us.at[2], ur.at[2], {'m2': jp[1]})
    u_fwd.start()
    rcopy(u_rows(jp[1]), u_rows(jp[1]), us.at[1], ur.at[1], {'m2': jp[1]}).wait_recv()
    with jax.named_scope('w_ufwd'):
        rcopy(u_rows(jp[3]), u_rows(jp[3]), us.at[2], ur.at[2], {'m2': jp[1]}).wait_recv()

    def lhs_in(m, slot):
        return pltpu.make_async_copy(u.at[rows_at(m * block, block), :], lhs.at[slot], lhs_sem.at[slot])

    def product1(b, own, store):
        with jax.named_scope('w_f1'):
            swapped1(b).wait_recv()
        loads = [pltpu.make_async_copy(own, rhs.at[rows_at(i * dim, dim), :], rhs_sem.at[0])]
        for e in (1, 2, 3):
            at = rows_at(ip[e] * dim, dim)
            loads.append(pltpu.make_async_copy(w1.at[b, at, :], rhs.at[at, :], rhs_sem.at[e]))
        for load in loads:
            load.start()
        lhs_in(0, 0).start()
        for load in loads:
            load.wait()

        @pl.loop(0, tokens // block)
        def _(m):
            slot = lax.rem(m, 2)
            lhs_in(m, slot).wait()

            @pl.when(m + 1 < tokens // block)
            def _():
                lhs_in(m + 1, 1 - slot).start()
            with jax.named_scope('mm1'):
                store(rows_at(m * block, block), dot(lhs[slot], rhs[...]))

    @pl.loop(0, 3)
    def _(b):
        def store(at, value):
            zq[b, at, :] = value.astype(jnp.bfloat16)
        product1(b, wq.at[b, :, ds(i * qw, qw)], store)

        @pl.when(b == 1)
        def _():
            forward1(4)
            issue1(6)

    @pl.loop(0, batch)
    def _(n):
        at = rows_at(n * patches, patches)
        for head in range(heads):
            cols = slice(head * LANES, (head + 1) * LANES)
            query = head_norm(zq[0, at, cols].astype(jnp.float32), qns[...])
            key = head_norm(zq[1, at, cols].astype(jnp.float32), kns[...])
            scores = lax.dot_general(query, key, (((1,), (1,)), ((), ())), preferred_element_type=jnp.float32) * LANES ** -0.5
            scores = jnp.exp(scores - jnp.max(scores, axis=-1, keepdims=True))
            probs = (scores / jnp.sum(scores, axis=-1, keepdims=True)).astype(jnp.bfloat16)
            with jax.named_scope('attn'):
                h[at, cols] = dot(probs, zq[2, at, cols]).astype(jnp.bfloat16)

    forward1(5)
    for c in range(AHEAD // 2):
        issue2(c)

    @pl.loop(0, nub)
    def _(b):
        def store(at, value):
            value = value.astype(jnp.bfloat16).astype(jnp.float32) + bu[:, ds(i * uw + b * qw, qw)]
            value = 0.5 * value * (1.0 + lax.erf(value * 2.0 ** -0.5))
            h[at, ds(qw + b * qw, qw)] = value.astype(jnp.bfloat16)
        product1(b + 3, wu.at[:, ds(i * uw + b * qw, qw)], store)

        @pl.when(b == 1)
        def _():
            forward1(6)
            for c in range(AHEAD // 2, AHEAD):
                issue2(c)

        @pl.when(b == 2)
        def _():
            next2(0)

        @pl.when(b == 3)
        def _():
            next2(1)

    def quarter(yy, core):
        return (2 * yy + core) * rows

    def send_a(c, yy):
        return rcopy(pa.at[lax.rem(c, 2), yy], ra.at[c, yy], as_.at[lax.rem(c, 2)], ar.at[c], {'m2': jp[1]})

    def all_a(c):
        return rcopy(pa.at[lax.rem(c, 2)], ra.at[c], as_.at[lax.rem(c, 2)], ar.at[c], {'m2': jp[1]})

    def send_b(c):
        return rcopy(ss.at[lax.rem(c, 2)], rb.at[c], bs.at[lax.rem(c, 2)], br.at[c], {'m2': jp[2]})

    def send_c(c, k):
        src = rb.at[c, :, ds(ip[1 + 2 * k] * LANES, LANES)]
        return rcopy(src, rc.at[c, k], cs.at[0], cr.at[c], {'m1': ip[1]})

    def send_d(c):
        return rcopy(ud.at[c], rd.at[c], dsm.at[0], drm.at[c], {'m1': ip[2]})

    def out_part(c, q):
        return out.at[rows_at(q * rows, rows), ds(c * LANES, LANES)]

    def result(c, q, sem, recv, device):
        part = out_part(c, q)
        return rcopy(part, part, es.at[sem], recv, device)

    def product2(c):
        slot = lax.rem(c, 2)
        cols, to = ds(c * LANES, LANES), ds(i * LANES, LANES)
        loads = [pltpu.make_async_copy(wo.at[rows_at(i * qw, qw), cols], w2b.at[slot, 0:qw, to], w2b_sem.at[0]),
                 pltpu.make_async_copy(wd.at[rows_at(i * uw, uw), cols], w2b.at[slot, qw:qw + uw, to], w2b_sem.at[1])]
        for load in loads:
            load.start()
        with jax.named_scope('w_f2'):
            part = w2.at[c, 0, :, 0:3 * LANES]
            rcopy(part, part, f2s.at[0], f2r.at[c], {'dp': 1 - g}).wait_recv()
        for e in (1, 2, 3):
            to = ds(ip[e] * LANES, LANES)
            for k in range(2):
                sems = 2 + 4 * (e - 1) + 2 * k
                loads.append(pltpu.make_async_copy(w2.at[c, k, 0:qh, to], w2b.at[slot, k * qh:(k + 1) * qh, to], w2b_sem.at[sems]))
                loads.append(pltpu.make_async_copy(w2.at[c, k, qh:qh + uh, to], w2b.at[slot, qw + k * uh:qw + (k + 1) * uh, to], w2b_sem.at[sems + 1]))
        for load in loads[2:]:
            load.start()

        @pl.when(c >= 2)
        def _():
            all_a(c - 2).wait_send()
        with jax.named_scope('w_w2b'):
            for load in loads:
                load.wait()
        for yy in range(2):
            for sub in range(2):
                at = rows_at(quarter(yy, 1 - jc) + sub * block, block)
                pa[slot, yy, sub * block:(sub + 1) * block, :] = dot(h[at, :], w2b[slot]).astype(jnp.bfloat16)
            send_a(c, yy).start()
        keep = lax.rem(c, 3)
        for yy in range(2):
            for sub in range(2):
                at = rows_at(quarter(yy, jc) + sub * block, block)
                po[keep, yy, sub * block:(sub + 1) * block, :] = dot(h[at, :], w2b[slot]).astype(jnp.bfloat16)

    def add(a, b):
        return (a.astype(jnp.float32) + b.astype(jnp.float32)).astype(jnp.bfloat16)

    def sum_core(d):
        keep = lax.rem(d, 3)
        with jax.named_scope('w_a'):
            rcopy(ra.at[d], ra.at[d], as_.at[0], ar.at[d], {'m2': jp[1]}).wait_recv()
        load = pltpu.make_async_copy(ra.at[d], rav, rav_sem.at[0])
        load.start()

        @pl.when(d >= 2)
        def _():
            send_b(d - 2).wait_send()
        load.wait()
        ss[lax.rem(d, 2)] = add(po[keep, 1 - jy], rav[1 - jy])
        send_b(d).start()
        po[keep, jy] = add(po[keep, jy], rav[jy])

    def sum_y(d):
        with jax.named_scope('w_b'):
            rcopy(rb.at[d], rb.at[d], bs.at[0], br.at[d], {'m2': jp[2]}).wait_recv()
        rb[d] = add(po[lax.rem(d, 3), jy], rb[d])
        for k in range(2):
            send_c(d, k).start()

    def sum_near(d):
        with jax.named_scope('w_c'):
            rcopy(rc.at[d], rc.at[d], cs.at[0], cr.at[d], {'m1': ip[1]}).wait_recv()
        ud[d] = add(rb[d, :, ds(ip[2] * LANES, LANES)], rc[d, 1])
        send_d(d).start()

    def finish(d):
        with jax.named_scope('w_d'):
            rcopy(rd.at[d], rd.at[d], dsm.at[0], drm.at[d], {'m1': ip[2]}).wait_recv()
        cols = ds(d * LANES, LANES)
        value = rb[d, :, ds(i * LANES, LANES)].astype(jnp.float32) + rc[d, 0].astype(jnp.float32) + rd[d].astype(jnp.float32)
        value = xg[i, :, cols].astype(jnp.float32) + value + bo[cols][None, :]
        out[rows_at(j * rows, rows), cols] = value.astype(jnp.bfloat16)
        result(d, j, 0, er.at[d], {'m2': jp[2]}).start()
        result(d, j, 1, fr.at[0], {'m2': jp[1]}).start()

    def pass_on(d):
        with jax.named_scope('w_e'):
            result(d, jp[2], 0, er.at[d], {'m2': jp[2]}).wait_recv()
        result(d, jp[2], 2, fr.at[1], {'m2': jp[1]}).start()

    def run(step, first, last):
        @pl.loop(max(first, 0), max(last, 0))
        def _(d):
            step(d)

    def late(c, lag, step, last=nc):
        @pl.when((c >= lag) & (c < last))
        def _():
            step(c - lag)

    @pl.loop(0, nc)
    def _(c):
        late(c, 2, sum_y)
        late(c, 1, sum_core)

        @pl.when((c >= 1) & (c + 1 < nc))
        def _():
            next2(c + 1)

        @pl.when(c == nc - 2)
        def _():
            run(sum_near, 0, min(4, nc - 4))

        @pl.when(c == nc - 1)
        def _():
            run(sum_near, min(4, nc - 4), max(nc - 6, 1))
            finish(0)
        product2(c)

    sum_core(nc - 1)
    run(sum_near, max(nc - 6, 1), nc - 3)
    sum_y(nc - 2)
    sum_near(nc - 3)
    run(finish, 1, nc - 6)
    sum_y(nc - 1)
    sum_near(nc - 2)
    run(finish, max(nc - 6, 1), nc - 3)
    sum_near(nc - 1)
    run(finish, max(nc - 3, 1), nc)
    run(pass_on, 0, nc)

    with jax.named_scope('drain0'):
      for copy in (x_far, x_near, x_fwd, u_far, u_near, u_fwd):
        copy.wait_send()
    for sem in (w1s, f1s):
        part = w1.at[:, 0:3 * half, :]
        rcopy(part, part, sem.at[0], w1r.at[0, 0], {'dp': 1 - g}).wait_send()
    for sem in (w2s, f2s):
        part = w2.at[:, 0, :, 0:3 * LANES]
        rcopy(part, part, sem.at[0], f2r.at[0], {'dp': 1 - g}).wait_send()
    for c in (nc - 2, nc - 1):
        all_a(c).wait_send()
        send_b(c).wait_send()
    rcopy(rc, rc, cs.at[0], cr.at[0], {'m1': ip[1]}).wait_send()
    for sem in (dsm.at[0], es.at[0], es.at[1], es.at[2]):
        rcopy(rd, rd, sem, drm.at[0], {'m1': ip[2]}).wait_send()
    for k in range(2):
        with jax.named_scope('w_f'):
            rcopy(rd, rd, es.at[1], fr.at[k], {'m2': jp[1]}).wait_recv()


def solution(mesh):
    assert mesh.shape['m1'] == 4 and mesh.shape['m2'] == 4 and mesh.shape['dp'] == 2

    def local_layer(x_blk, ln_scale, qn_scale, kn_scale, w_qkv, w_up, b_up, w_o, w_down, b_out):
        batch, patches, dim = x_blk.shape
        tokens = batch * patches
        qw, uw = w_qkv.shape[2] // 4, w_up.shape[1] // 4
        rows, block, nc, nb = tokens // 4, tokens // 8, dim // LANES, 3 + uw // qw
        assert qn_scale.shape[0] == LANES and uw % qw == 0 and nb == 7
        wide = 4 * LANES
        bf16 = jnp.bfloat16
        dma = pltpu.SemaphoreType.DMA
        hbm = pl.BlockSpec(memory_space=pltpu.HBM)
        vmem = pl.BlockSpec(memory_space=pltpu.VMEM)
        ln_rows = min(64, rows)
        out = pl.pallas_call(
            functools.partial(kernel, (batch, patches, dim, qw, uw)),
            out_shape=[
                pltpu.VMEM((tokens, dim), bf16),
                jax.ShapeDtypeStruct((tokens, 4 * dim), bf16),
                jax.ShapeDtypeStruct((nb, 4 * dim, qw), bf16),
                jax.ShapeDtypeStruct((nc, 2, (qw + uw) // 2, wide), bf16),
                jax.ShapeDtypeStruct((nc, 2, rows, wide), bf16)],
            in_specs=[hbm, vmem, vmem, vmem, hbm, hbm, vmem, hbm, hbm, vmem],
            out_specs=[vmem] + [hbm] * 4,
            scratch_shapes=[
                pltpu.VMEM((4, rows, dim), bf16),
                pltpu.VMEM((2, ln_rows, 4 * dim), bf16),
                pltpu.VMEM((3, tokens, qw), bf16),
                pltpu.VMEM((tokens, qw + uw), bf16),
                pltpu.VMEM((4 * dim, qw), bf16),
                pltpu.VMEM((2, block, 4 * dim), bf16),
                pltpu.VMEM((2, qw + uw, wide), bf16),
                pltpu.VMEM((2, 2, rows, wide), bf16),
                pltpu.VMEM((3, 2, rows, wide), bf16),
                pltpu.VMEM((2, rows, wide), bf16),
                pltpu.VMEM((2, rows, wide), bf16),
                pltpu.VMEM((nc, rows, wide), bf16),
                pltpu.VMEM((nc, 2, rows, LANES), bf16),
                pltpu.VMEM((nc, rows, LANES), bf16),
                pltpu.VMEM((nc, rows, LANES), bf16),
                dma((3,)), dma((3,)),
                dma((1,)), dma((nb, 3)), dma((1,)), dma((nb,)),
                dma((3,)), dma((3,)),
                dma((1,)), dma((nc, 3)), dma((1,)), dma((nc,)),
                dma((2,)), dma((nc,)), dma((2,)), dma((nc,)), dma((1,)), dma((nc,)), dma((1,)), dma((nc,)),
                dma((3,)), dma((nc,)), dma((2,)),
                dma((1,)), dma((4,)), dma((2,)), dma((2,)), dma((14,)), dma((1,))],
            compiler_params=pltpu.CompilerParams(collective_id=0, has_side_effects=True, vmem_limit_bytes=60_000_000),
            name='layer',
        )(x_blk.reshape(tokens, dim), ln_scale[None], qn_scale[None], kn_scale[None], w_qkv.transpose(1, 0, 2), w_up,
          b_up[None], w_o, w_down, b_out)[0]
        return out.reshape(batch, patches, dim)

    return jax.shard_map(local_layer, mesh=mesh, in_specs=(P('dp', None, 'm1'), P(), P(), P(), P('m1', None, 'm2'), P('m1', 'm2'), P('m2'), P('m2', 'm1'), P('m2', 'm1'), P('m1')), out_specs=P('dp', None, 'm1'), check_vma=False)
```

```python
import functools

import jax
import jax.numpy as jnp
from jax import lax
from jax.experimental import pallas as pl
from jax.experimental.pallas import tpu as pltpu
from jax.sharding import PartitionSpec as P

LN_EPS = 1e-6
MESH = pl.DeviceIdType.MESH
LANES = 128
AHEAD = 2


def xors(value):
    return (value, value + 1 - 2 * lax.rem(value, 2), value + 2 - 4 * lax.div(value, 2), 3 - value)


def ds(start, size):
    return pl.ds(pl.multiple_of(start, size if size < LANES else LANES), size)


def rows_at(start, size):
    return pl.ds(pl.multiple_of(start, 8), size)


def rcopy(src, dst, send_sem, recv_sem, device):
    return pltpu.make_async_remote_copy(src_ref=src, dst_ref=dst, send_sem=send_sem, recv_sem=recv_sem, device_id=device, device_id_type=MESH)


def dot(lhs, rhs):
    return jnp.dot(lhs, rhs, preferred_element_type=jnp.float32)


def head_norm(values, scale):
    mean = jnp.mean(values, axis=-1, keepdims=True)
    centered = values - mean
    variance = jnp.mean(centered * centered, axis=-1, keepdims=True)
    return (centered * lax.rsqrt(variance + LN_EPS) * scale).astype(jnp.bfloat16)


def kernel(sizes, x, lns, qns, kns, wq, wu, bu, wo, wd, bo,
           out, u, w1, w2, ra,
           xg, ubl, zq, h, rhs, lhs, w2b, pa, po, rav, ss, rb, rc, ud, rd,
           xs, xr, w1s, w1r, f1s, f1r, us, ur, w2s, w2r, f2s, f2r,
           as_, ar, bs, br, cs, cr, dsm, drm, es, er, fr, own_sem, rhs_sem, lhs_sem, ub_sem, w2b_sem, rav_sem):
    batch, patches, dim, qw, uw = sizes
    tokens = batch * patches
    rows = tokens // 4
    block = rows // 2
    half = dim // 2
    total = 4 * dim
    nub = uw // qw
    nc = dim // LANES
    wide = 4 * LANES
    heads = qw // LANES
    ln_rows = min(64, rows)

    g, i, j = lax.axis_index('dp'), lax.axis_index('m1'), lax.axis_index('m2')
    ip, jp = xors(i), xors(j)
    jy, jc = lax.div(j, 2), lax.rem(j, 2)
    mid = lax.div(lax.rem(i + 1, 4), 2)
    peers1 = ((0, ip[1]), (2 - mid, ip[3] + mid * (ip[2] - ip[3])), (1 + mid, ip[2] + mid * (ip[3] - ip[2])))

    barrier = pltpu.get_barrier_semaphore()
    peers = [{'m1': ip[e]} for e in (1, 2, 3)] + [{'m2': jp[e]} for e in (1, 2, 3)] + [{'dp': 1 - g}]
    for peer in peers:
        pl.semaphore_signal(barrier, inc=1, device_id=peer, device_id_type=MESH)
    with jax.named_scope('barrier'):
        pl.semaphore_wait(barrier, len(peers))

    mine = rows_at(j * rows, rows)
    x_far = rcopy(x.at[mine, :], xg.at[i], xs.at[0], xr.at[0], {'m1': ip[2]})
    x_near = rcopy(x.at[mine, :], xg.at[i], xs.at[1], xr.at[1], {'m1': ip[1]})
    x_own = pltpu.make_async_copy(x.at[mine, :], xg.at[i], own_sem.at[0])
    x_far.start()
    x_near.start()
    x_own.start()
    x_far_in = rcopy(xg.at[ip[2]], xg.at[ip[2]], xs.at[0], xr.at[0], {'m1': ip[2]})
    with jax.named_scope('w_xfar'):
        x_far_in.wait_recv()
    x_fwd = rcopy(xg.at[ip[2]], xg.at[ip[2]], xs.at[2], xr.at[2], {'m1': ip[1]})
    x_fwd.start()

    def z1(b, e):
        t = ip[e]
        if b < 3:
            src = wq.at[b, rows_at(g * half, half), ds(t * qw, qw)]
        else:
            src = wu.at[rows_at(g * half, half), ds(t * uw + (b - 3) * qw, qw)]
        return rcopy(src, w1.at[b, rows_at(i * dim + g * half, half), :], w1s.at[0], w1r.at[b, e - 1], {'m1': t})

    def piece1(b, k, s):
        part = w1.at[b, rows_at(s * dim + g * half, half), :]
        return (rcopy(part, part, w1s.at[0], w1r.at[b, k], {'m1': s}), rcopy(part, part, f1s.at[0], f1r.at[b], {'dp': 1 - g}))

    def forward1(b):
        for k, s in peers1:
            arrival, swap = piece1(b, k, s)
            with jax.named_scope('w_z1'):
                arrival.wait_recv()
            swap.start()

    def swapped1(b):
        part = w1.at[b, 0:3 * half, :]
        return rcopy(part, part, f1s.at[0], f1r.at[b], {'dp': 1 - g})

    def issue1(b):
        for e in (2, 3, 1):
            z1(b, e).start()

    issue1(0)
    issue1(1)

    qh, uh = qw // 2, uw // 2

    def z2(c, e):
        t = ip[e]
        cols, to = ds(c * LANES, LANES), ds(i * LANES, LANES)
        return [rcopy(wd.at[rows_at(t * uw + g * uh, uh), cols], w2.at[c, g, qh:qh + uh, to], w2s.at[0], w2r.at[c, e - 1], {'m1': t}),
                rcopy(wo.at[rows_at(t * qw + g * qh, qh), cols], w2.at[c, g, 0:qh, to], w2s.at[0], w2r.at[c, e - 1], {'m1': t})]

    def issue2(c):
        for e in (2, 3, 1):
            for copy in z2(c, e):
                copy.start()

    def forward2(c):
        for k, s in peers1:
            part = w2.at[c, g, :, ds(s * LANES, LANES)]
            with jax.named_scope('w_z2'):
                rcopy(part, part, w2s.at[0], w2r.at[c, k], {'m1': s}).wait_recv()
            rcopy(part, part, f2s.at[0], f2r.at[c], {'dp': 1 - g}).start()

    def next2(c):
        forward2(c)

        @pl.when(c + AHEAD < nc)
        def _():
            issue2(c + AHEAD)

    with jax.named_scope('w_xown'):
        x_own.wait()
    with jax.named_scope('w_xnear'):
        rcopy(xg.at[ip[1]], xg.at[ip[1]], xs.at[1], xr.at[1], {'m1': ip[1]}).wait_recv()
    with jax.named_scope('w_xfwd'):
        rcopy(xg.at[ip[3]], xg.at[ip[3]], xs.at[2], xr.at[2], {'m1': ip[1]}).wait_recv()

    def u_out(r, slot):
        return pltpu.make_async_copy(ubl.at[slot], u.at[rows_at(j * rows + r * ln_rows, ln_rows), :], ub_sem.at[slot])

    @pl.loop(0, rows // ln_rows)
    def _(r):
        slot = lax.rem(r, 2)

        @pl.when(r >= 2)
        def _():
            u_out(r - 2, slot).wait()
        at = rows_at(r * ln_rows, ln_rows)
        parts = [xg[s, at, :].astype(jnp.float32) for s in range(4)]
        mean = sum(jnp.sum(part, axis=-1, keepdims=True) for part in parts) / total
        parts = [part - mean for part in parts]
        variance = sum(jnp.sum(part * part, axis=-1, keepdims=True) for part in parts) / total
        inverse = lax.rsqrt(variance + LN_EPS)
        for s in range(4):
            cols = slice(s * dim, (s + 1) * dim)
            ubl[slot, :, cols] = (parts[s] * inverse * lns[:, cols]).astype(jnp.bfloat16)
        u_out(r, slot).start()

    for r in range(max(0, rows // ln_rows - 2), rows // ln_rows):
        u_out(r, r % 2).wait()

    def u_rows(q):
        return u.at[rows_at(q * rows, rows), :]

    u_far = rcopy(u_rows(j), u_rows(j), us.at[0], ur.at[0], {'m2': jp[2]})
    u_near = rcopy(u_rows(j), u_rows(j), us.at[1], ur.at[1], {'m2': jp[1]})
    u_far.start()
    u_near.start()
    for b in range(4):
        forward1(b)
        issue1(b + 2)
    with jax.named_scope('w_ufar'):
        rcopy(u_rows(jp[2]), u_rows(jp[2]), us.at[0], ur.at[0], {'m2': jp[2]}).wait_recv()
    u_fwd = rcopy(u_rows(jp[2]), u_rows(jp[2]), us.at[2], ur.at[2], {'m2': jp[1]})
    u_fwd.start()
    rcopy(u_rows(jp[1]), u_rows(jp[1]), us.at[1], ur.at[1], {'m2': jp[1]}).wait_recv()
    with jax.named_scope('w_ufwd'):
        rcopy(u_rows(jp[3]), u_rows(jp[3]), us.at[2], ur.at[2], {'m2': jp[1]}).wait_recv()

    def lhs_in(m, slot):
        return pltpu.make_async_copy(u.at[rows_at(m * block, block), :], lhs.at[slot], lhs_sem.at[slot])

    def product1(b, own, store):
        with jax.named_scope('w_f1'):
            swapped1(b).wait_recv()
        loads = [pltpu.make_async_copy(own, rhs.at[rows_at(i * dim, dim), :], rhs_sem.at[0])]
        for e in (1, 2, 3):
            at = rows_at(ip[e] * dim, dim)
            loads.append(pltpu.make_async_copy(w1.at[b, at, :], rhs.at[at, :], rhs_sem.at[e]))
        for load in loads:
            load.start()
        lhs_in(0, 0).start()
        for load in loads:
            load.wait()

        @pl.loop(0, tokens // block)
        def _(m):
            slot = lax.rem(m, 2)
            lhs_in(m, slot).wait()

            @pl.when(m + 1 < tokens // block)
            def _():
                lhs_in(m + 1, 1 - slot).start()
            with jax.named_scope('mm1'):
                store(rows_at(m * block, block), dot(lhs[slot], rhs[...]))

    @pl.loop(0, 3)
    def _(b):
        def store(at, value):
            zq[b, at, :] = value.astype(jnp.bfloat16)
        product1(b, wq.at[b, :, ds(i * qw, qw)], store)

        @pl.when(b == 1)
        def _():
            forward1(4)
            issue1(6)

    @pl.loop(0, batch)
    def _(n):
        at = rows_at(n * patches, patches)
        for head in range(heads):
            cols = slice(head * LANES, (head + 1) * LANES)
            query = head_norm(zq[0, at, cols].astype(jnp.float32), qns[...])
            key = head_norm(zq[1, at, cols].astype(jnp.float32), kns[...])
            scores = lax.dot_general(query, key, (((1,), (1,)), ((), ())), preferred_element_type=jnp.float32) * LANES ** -0.5
            scores = jnp.exp(scores - jnp.max(scores, axis=-1, keepdims=True))
            probs = (scores / jnp.sum(scores, axis=-1, keepdims=True)).astype(jnp.bfloat16)
            with jax.named_scope('attn'):
                h[at, cols] = dot(probs, zq[2, at, cols]).astype(jnp.bfloat16)

    forward1(5)
    for c in range(AHEAD // 2):
        issue2(c)

    @pl.loop(0, nub)
    def _(b):
        def store(at, value):
            value = value.astype(jnp.bfloat16).astype(jnp.float32) + bu[:, ds(i * uw + b * qw, qw)]
            value = 0.5 * value * (1.0 + lax.erf(value * 2.0 ** -0.5))
            h[at, ds(qw + b * qw, qw)] = value.astype(jnp.bfloat16)
        product1(b + 3, wu.at[:, ds(i * uw + b * qw, qw)], store)

        @pl.when(b == 1)
        def _():
            forward1(6)
            for c in range(AHEAD // 2, AHEAD):
                issue2(c)

        @pl.when(b == 2)
        def _():
            next2(0)

        @pl.when(b == 3)
        def _():
            next2(1)

    def quarter(yy, core):
        return (2 * yy + core) * rows

    def send_a(c, yy):
        return rcopy(pa.at[lax.rem(c, 2), yy], ra.at[c, yy], as_.at[lax.rem(c, 2)], ar.at[c], {'m2': jp[1]})

    def all_a(c):
        return rcopy(pa.at[lax.rem(c, 2)], ra.at[c], as_.at[lax.rem(c, 2)], ar.at[c], {'m2': jp[1]})

    def send_b(c):
        return rcopy(ss.at[lax.rem(c, 2)], rb.at[c], bs.at[lax.rem(c, 2)], br.at[c], {'m2': jp[2]})

    def send_c(c, k):
        src = rb.at[c, :, ds(ip[1 + 2 * k] * LANES, LANES)]
        return rcopy(src, rc.at[c, k], cs.at[0], cr.at[c], {'m1': ip[1]})

    def send_d(c):
        return rcopy(ud.at[c], rd.at[c], dsm.at[0], drm.at[c], {'m1': ip[2]})

    def out_part(c, q):
        return out.at[rows_at(q * rows, rows), ds(c * LANES, LANES)]

    def result(c, q, sem, recv, device):
        part = out_part(c, q)
        return rcopy(part, part, es.at[sem], recv, device)

    def product2(c):
        slot = lax.rem(c, 2)
        cols, to = ds(c * LANES, LANES), ds(i * LANES, LANES)
        loads = [pltpu.make_async_copy(wo.at[rows_at(i * qw, qw), cols], w2b.at[slot, 0:qw, to], w2b_sem.at[0]),
                 pltpu.make_async_copy(wd.at[rows_at(i * uw, uw), cols], w2b.at[slot, qw:qw + uw, to], w2b_sem.at[1])]
        for load in loads:
            load.start()
        with jax.named_scope('w_f2'):
            part = w2.at[c, 0, :, 0:3 * LANES]
            rcopy(part, part, f2s.at[0], f2r.at[c], {'dp': 1 - g}).wait_recv()
        for e in (1, 2, 3):
            to = ds(ip[e] * LANES, LANES)
            for k in range(2):
                sems = 2 + 4 * (e - 1) + 2 * k
                loads.append(pltpu.make_async_copy(w2.at[c, k, 0:qh, to], w2b.at[slot, k * qh:(k + 1) * qh, to], w2b_sem.at[sems]))
                loads.append(pltpu.make_async_copy(w2.at[c, k, qh:qh + uh, to], w2b.at[slot, qw + k * uh:qw + (k + 1) * uh, to], w2b_sem.at[sems + 1]))
        for load in loads[2:]:
            load.start()

        @pl.when(c >= 2)
        def _():
            all_a(c - 2).wait_send()
        with jax.named_scope('w_w2b'):
            for load in loads:
                load.wait()
        for yy in range(2):
            for sub in range(2):
                at = rows_at(quarter(yy, 1 - jc) + sub * block, block)
                pa[slot, yy, sub * block:(sub + 1) * block, :] = dot(h[at, :], w2b[slot]).astype(jnp.bfloat16)
            send_a(c, yy).start()
        keep = lax.rem(c, 3)
        for yy in range(2):
            for sub in range(2):
                at = rows_at(quarter(yy, jc) + sub * block, block)
                po[keep, yy, sub * block:(sub + 1) * block, :] = dot(h[at, :], w2b[slot]).astype(jnp.bfloat16)

    def add(a, b):
        return (a.astype(jnp.float32) + b.astype(jnp.float32)).astype(jnp.bfloat16)

    def sum_core(d):
        keep = lax.rem(d, 3)
        with jax.named_scope('w_a'):
            rcopy(ra.at[d], ra.at[d], as_.at[0], ar.at[d], {'m2': jp[1]}).wait_recv()
        load = pltpu.make_async_copy(ra.at[d], rav, rav_sem.at[0])
        load.start()

        @pl.when(d >= 2)
        def _():
            send_b(d - 2).wait_send()
        load.wait()
        ss[lax.rem(d, 2)] = add(po[keep, 1 - jy], rav[1 - jy])
        send_b(d).start()
        po[keep, jy] = add(po[keep, jy], rav[jy])

    def sum_y(d):
        with jax.named_scope('w_b'):
            rcopy(rb.at[d], rb.at[d], bs.at[0], br.at[d], {'m2': jp[2]}).wait_recv()
        rb[d] = add(po[lax.rem(d, 3), jy], rb[d])
        for k in range(2):
            send_c(d, k).start()

    def sum_near(d):
        with jax.named_scope('w_c'):
            rcopy(rc.at[d], rc.at[d], cs.at[0], cr.at[d], {'m1': ip[1]}).wait_recv()
        ud[d] = add(rb[d, :, ds(ip[2] * LANES, LANES)], rc[d, 1])
        send_d(d).start()

    def finish(d):
        with jax.named_scope('w_d'):
            rcopy(rd.at[d], rd.at[d], dsm.at[0], drm.at[d], {'m1': ip[2]}).wait_recv()
        cols = ds(d * LANES, LANES)
        value = rb[d, :, ds(i * LANES, LANES)].astype(jnp.float32) + rc[d, 0].astype(jnp.float32) + rd[d].astype(jnp.float32)
        value = xg[i, :, cols].astype(jnp.float32) + value + bo[cols][None, :]
        out[rows_at(j * rows, rows), cols] = value.astype(jnp.bfloat16)
        result(d, j, 0, er.at[d], {'m2': jp[2]}).start()
        result(d, j, 1, fr.at[0], {'m2': jp[1]}).start()

    def pass_on(d):
        with jax.named_scope('w_e'):
            result(d, jp[2], 0, er.at[d], {'m2': jp[2]}).wait_recv()
        result(d, jp[2], 2, fr.at[1], {'m2': jp[1]}).start()

    def run(step, first, last):
        @pl.loop(first, last)
        def _(d):
            step(d)

    early = 2 + 2 * mid

    def late(c, lag, step, last=nc):
        @pl.when((c >= lag) & (c < last))
        def _():
            step(c - lag)

    @pl.loop(0, nc)
    def _(c):
        late(c, 2, sum_y)
        late(c, 1, sum_core)

        @pl.when((c >= 1) & (c + 1 < nc))
        def _():
            next2(c + 1)

        @pl.when(c == nc - 2)
        def _():
            run(sum_near, 0, early)

        @pl.when(c == nc - 1)
        def _():
            run(sum_near, early, early + 2)
            finish(0)
        product2(c)

    sum_core(nc - 1)
    run(sum_near, early + 2, early + 5)
    sum_y(nc - 2)
    run(sum_near, early + 5, nc - 2)
    run(finish, 1, 4)
    sum_y(nc - 1)
    sum_near(nc - 2)
    run(finish, 4, nc - 3)
    sum_near(nc - 1)
    run(finish, nc - 3, nc)
    run(pass_on, 0, nc)

    with jax.named_scope('drain0'):
      for copy in (x_far, x_near, x_fwd, u_far, u_near, u_fwd):
        copy.wait_send()
    for sem in (w1s, f1s):
        part = w1.at[:, 0:3 * half, :]
        rcopy(part, part, sem.at[0], w1r.at[0, 0], {'dp': 1 - g}).wait_send()
    for sem in (w2s, f2s):
        part = w2.at[:, 0, :, 0:3 * LANES]
        rcopy(part, part, sem.at[0], f2r.at[0], {'dp': 1 - g}).wait_send()
    for c in (nc - 2, nc - 1):
        all_a(c).wait_send()
        send_b(c).wait_send()
    rcopy(rc, rc, cs.at[0], cr.at[0], {'m1': ip[1]}).wait_send()
    for sem in (dsm.at[0], es.at[0], es.at[1], es.at[2]):
        rcopy(rd, rd, sem, drm.at[0], {'m1': ip[2]}).wait_send()
    for k in range(2):
        with jax.named_scope('w_f'):
            rcopy(rd, rd, es.at[1], fr.at[k], {'m2': jp[1]}).wait_recv()


def solution(mesh):
    assert mesh.shape['m1'] == 4 and mesh.shape['m2'] == 4 and mesh.shape['dp'] == 2

    def local_layer(x_blk, ln_scale, qn_scale, kn_scale, w_qkv, w_up, b_up, w_o, w_down, b_out):
        batch, patches, dim = x_blk.shape
        tokens = batch * patches
        qw, uw = w_qkv.shape[2] // 4, w_up.shape[1] // 4
        rows, block, nc, nb = tokens // 4, tokens // 8, dim // LANES, 3 + uw // qw
        assert qn_scale.shape[0] == LANES and uw % qw == 0 and nb == 7
        wide = 4 * LANES
        bf16 = jnp.bfloat16
        dma = pltpu.SemaphoreType.DMA
        hbm = pl.BlockSpec(memory_space=pltpu.HBM)
        vmem = pl.BlockSpec(memory_space=pltpu.VMEM)
        ln_rows = min(64, rows)
        out = pl.pallas_call(
            functools.partial(kernel, (batch, patches, dim, qw, uw)),
            out_shape=[
                pltpu.VMEM((tokens, dim), bf16),
                jax.ShapeDtypeStruct((tokens, 4 * dim), bf16),
                jax.ShapeDtypeStruct((nb, 4 * dim, qw), bf16),
                jax.ShapeDtypeStruct((nc, 2, (qw + uw) // 2, wide), bf16),
                jax.ShapeDtypeStruct((nc, 2, rows, wide), bf16)],
            in_specs=[hbm, vmem, vmem, vmem, hbm, hbm, vmem, hbm, hbm, vmem],
            out_specs=[vmem] + [hbm] * 4,
            scratch_shapes=[
                pltpu.VMEM((4, rows, dim), bf16),
                pltpu.VMEM((2, ln_rows, 4 * dim), bf16),
                pltpu.VMEM((3, tokens, qw), bf16),
                pltpu.VMEM((tokens, qw + uw), bf16),
                pltpu.VMEM((4 * dim, qw), bf16),
                pltpu.VMEM((2, block, 4 * dim), bf16),
                pltpu.VMEM((2, qw + uw, wide), bf16),
                pltpu.VMEM((2, 2, rows, wide), bf16),
                pltpu.VMEM((3, 2, rows, wide), bf16),
                pltpu.VMEM((2, rows, wide), bf16),
                pltpu.VMEM((2, rows, wide), bf16),
                pltpu.VMEM((nc, rows, wide), bf16),
                pltpu.VMEM((nc, 2, rows, LANES), bf16),
                pltpu.VMEM((nc, rows, LANES), bf16),
                pltpu.VMEM((nc, rows, LANES), bf16),
                dma((3,)), dma((3,)),
                dma((1,)), dma((nb, 3)), dma((1,)), dma((nb,)),
                dma((3,)), dma((3,)),
                dma((1,)), dma((nc, 3)), dma((1,)), dma((nc,)),
                dma((2,)), dma((nc,)), dma((2,)), dma((nc,)), dma((1,)), dma((nc,)), dma((1,)), dma((nc,)),
                dma((3,)), dma((nc,)), dma((2,)),
                dma((1,)), dma((4,)), dma((2,)), dma((2,)), dma((14,)), dma((1,))],
            compiler_params=pltpu.CompilerParams(collective_id=0, has_side_effects=True, vmem_limit_bytes=60_000_000),
            name='layer',
        )(x_blk.reshape(tokens, dim), ln_scale[None], qn_scale[None], kn_scale[None], w_qkv.transpose(1, 0, 2), w_up,
          b_up[None], w_o, w_down, b_out)[0]
        return out.reshape(batch, patches, dim)

    return jax.shard_map(local_layer, mesh=mesh, in_specs=(P('dp', None, 'm1'), P(), P(), P(), P('m1', None, 'm2'), P('m1', 'm2'), P('m2'), P('m2', 'm1'), P('m2', 'm1'), P('m1')), out_specs=P('dp', None, 'm1'), check_vma=False)
```

```python
import functools

import jax
import jax.numpy as jnp
from jax import lax
from jax.experimental import pallas as pl
from jax.experimental.pallas import tpu as pltpu
from jax.sharding import PartitionSpec as P

LN_EPS = 1e-6
MESH = pl.DeviceIdType.MESH
LANES = 128
AHEAD = 2


def xors(value):
    return (value, value + 1 - 2 * lax.rem(value, 2), value + 2 - 4 * lax.div(value, 2), 3 - value)


def ds(start, size):
    return pl.ds(pl.multiple_of(start, size if size < LANES else LANES), size)


def rows_at(start, size):
    return pl.ds(pl.multiple_of(start, 8), size)


def rcopy(src, dst, send_sem, recv_sem, device):
    return pltpu.make_async_remote_copy(src_ref=src, dst_ref=dst, send_sem=send_sem, recv_sem=recv_sem, device_id=device, device_id_type=MESH)


def dot(lhs, rhs):
    return jnp.dot(lhs, rhs, preferred_element_type=jnp.float32)


def head_norm(values, scale):
    mean = jnp.mean(values, axis=-1, keepdims=True)
    centered = values - mean
    variance = jnp.mean(centered * centered, axis=-1, keepdims=True)
    return (centered * lax.rsqrt(variance + LN_EPS) * scale).astype(jnp.bfloat16)


def kernel(sizes, x, lns, qns, kns, wq, wu, bu, wo, wd, bo,
           out, u, w1, w2, ra,
           xg, ubl, zq, h, rhs, lhs, w2b, pa, po, rav, ss, rb, rc, ud, rd,
           xs, xr, w1s, w1r, f1s, f1r, us, ur, w2s, w2r, f2s, f2r,
           as_, ar, bs, br, cs, cr, dsm, drm, es, er, fr, own_sem, rhs_sem, lhs_sem, ub_sem, w2b_sem, rav_sem):
    batch, patches, dim, qw, uw = sizes
    tokens = batch * patches
    rows = tokens // 4
    block = rows // 2
    half = dim // 2
    total = 4 * dim
    nub = uw // qw
    nc = dim // LANES
    wide = 4 * LANES
    heads = qw // LANES
    ln_rows = min(64, rows)

    g, i, j = lax.axis_index('dp'), lax.axis_index('m1'), lax.axis_index('m2')
    ip, jp = xors(i), xors(j)
    jy, jc = lax.div(j, 2), lax.rem(j, 2)
    mid = lax.div(lax.rem(i + 1, 4), 2)
    peers1 = ((0, ip[1]), (2 - mid, ip[3] + mid * (ip[2] - ip[3])), (1 + mid, ip[2] + mid * (ip[3] - ip[2])))

    barrier = pltpu.get_barrier_semaphore()
    peers = [{'m1': ip[e]} for e in (1, 2, 3)] + [{'m2': jp[e]} for e in (1, 2, 3)] + [{'dp': 1 - g}]
    for peer in peers:
        pl.semaphore_signal(barrier, inc=1, device_id=peer, device_id_type=MESH)
    with jax.named_scope('barrier'):
        pl.semaphore_wait(barrier, len(peers))

    mine = rows_at(j * rows, rows)
    x_far = rcopy(x.at[mine, :], xg.at[i], xs.at[0], xr.at[0], {'m1': ip[2]})
    x_near = rcopy(x.at[mine, :], xg.at[i], xs.at[1], xr.at[1], {'m1': ip[1]})
    x_own = pltpu.make_async_copy(x.at[mine, :], xg.at[i], own_sem.at[0])
    x_far.start()
    x_near.start()
    x_own.start()
    x_far_in = rcopy(xg.at[ip[2]], xg.at[ip[2]], xs.at[0], xr.at[0], {'m1': ip[2]})
    with jax.named_scope('w_xfar'):
        x_far_in.wait_recv()
    x_fwd = rcopy(xg.at[ip[2]], xg.at[ip[2]], xs.at[2], xr.at[2], {'m1': ip[1]})
    x_fwd.start()

    def z1(b, e):
        t = ip[e]
        if b < 3:
            src = wq.at[b, rows_at(g * half, half), ds(t * qw, qw)]
        else:
            src = wu.at[rows_at(g * half, half), ds(t * uw + (b - 3) * qw, qw)]
        return rcopy(src, w1.at[b, rows_at(i * dim + g * half, half), :], w1s.at[0], w1r.at[b, e - 1], {'m1': t})

    def piece1(b, k, s):
        part = w1.at[b, rows_at(s * dim + g * half, half), :]
        return (rcopy(part, part, w1s.at[0], w1r.at[b, k], {'m1': s}), rcopy(part, part, f1s.at[0], f1r.at[b], {'dp': 1 - g}))

    def forward1(b):
        for k, s in peers1:
            arrival, swap = piece1(b, k, s)
            with jax.named_scope('w_z1'):
                arrival.wait_recv()
            swap.start()

    def swapped1(b):
        part = w1.at[b, 0:3 * half, :]
        return rcopy(part, part, f1s.at[0], f1r.at[b], {'dp': 1 - g})

    def issue1(b):
        for e in (2, 3, 1):
            z1(b, e).start()

    issue1(0)
    issue1(1)

    qh, uh = qw // 2, uw // 2

    def z2(c, e):
        t = ip[e]
        cols, to = ds(c * LANES, LANES), ds(i * LANES, LANES)
        return [rcopy(wd.at[rows_at(t * uw + g * uh, uh), cols], w2.at[c, g, qh:qh + uh, to], w2s.at[0], w2r.at[c, e - 1], {'m1': t}),
                rcopy(wo.at[rows_at(t * qw + g * qh, qh), cols], w2.at[c, g, 0:qh, to], w2s.at[0], w2r.at[c, e - 1], {'m1': t})]

    def issue2(c):
        for e in (2, 3, 1):
            for copy in z2(c, e):
                copy.start()

    def forward2(c):
        for k, s in peers1:
            part = w2.at[c, g, :, ds(s * LANES, LANES)]
            with jax.named_scope('w_z2'):
                rcopy(part, part, w2s.at[0], w2r.at[c, k], {'m1': s}).wait_recv()
            rcopy(part, part, f2s.at[0], f2r.at[c], {'dp': 1 - g}).start()

    def next2(c):
        forward2(c)

        @pl.when(c + AHEAD < nc)
        def _():
            issue2(c + AHEAD)

    with jax.named_scope('w_xown'):
        x_own.wait()
    with jax.named_scope('w_xnear'):
        rcopy(xg.at[ip[1]], xg.at[ip[1]], xs.at[1], xr.at[1], {'m1': ip[1]}).wait_recv()
    with jax.named_scope('w_xfwd'):
        rcopy(xg.at[ip[3]], xg.at[ip[3]], xs.at[2], xr.at[2], {'m1': ip[1]}).wait_recv()

    def u_out(r, slot):
        return pltpu.make_async_copy(ubl.at[slot], u.at[rows_at(j * rows + r * ln_rows, ln_rows), :], ub_sem.at[slot])

    @pl.loop(0, rows // ln_rows)
    def _(r):
        slot = lax.rem(r, 2)

        @pl.when(r >= 2)
        def _():
            u_out(r - 2, slot).wait()
        at = rows_at(r * ln_rows, ln_rows)
        parts = [xg[s, at, :].astype(jnp.float32) for s in range(4)]
        mean = sum(jnp.sum(part, axis=-1, keepdims=True) for part in parts) / total
        parts = [part - mean for part in parts]
        variance = sum(jnp.sum(part * part, axis=-1, keepdims=True) for part in parts) / total
        inverse = lax.rsqrt(variance + LN_EPS)
        for s in range(4):
            cols = slice(s * dim, (s + 1) * dim)
            ubl[slot, :, cols] = (parts[s] * inverse * lns[:, cols]).astype(jnp.bfloat16)
        u_out(r, slot).start()

    for r in range(max(0, rows // ln_rows - 2), rows // ln_rows):
        u_out(r, r % 2).wait()

    def u_rows(q):
        return u.at[rows_at(q * rows, rows), :]

    u_far = rcopy(u_rows(j), u_rows(j), us.at[0], ur.at[0], {'m2': jp[2]})
    u_near = rcopy(u_rows(j), u_rows(j), us.at[1], ur.at[1], {'m2': jp[1]})
    u_far.start()
    u_near.start()
    for b in range(4):
        forward1(b)
        issue1(b + 2)
    with jax.named_scope('w_ufar'):
        rcopy(u_rows(jp[2]), u_rows(jp[2]), us.at[0], ur.at[0], {'m2': jp[2]}).wait_recv()
    u_fwd = rcopy(u_rows(jp[2]), u_rows(jp[2]), us.at[2], ur.at[2], {'m2': jp[1]})
    u_fwd.start()
    rcopy(u_rows(jp[1]), u_rows(jp[1]), us.at[1], ur.at[1], {'m2': jp[1]}).wait_recv()
    with jax.named_scope('w_ufwd'):
        rcopy(u_rows(jp[3]), u_rows(jp[3]), us.at[2], ur.at[2], {'m2': jp[1]}).wait_recv()

    def lhs_in(m, slot):
        return pltpu.make_async_copy(u.at[rows_at(m * block, block), :], lhs.at[slot], lhs_sem.at[slot])

    def product1(b, own, store):
        with jax.named_scope('w_f1'):
            swapped1(b).wait_recv()
        loads = [pltpu.make_async_copy(own, rhs.at[rows_at(i * dim, dim), :], rhs_sem.at[0])]
        for e in (1, 2, 3):
            at = rows_at(ip[e] * dim, dim)
            loads.append(pltpu.make_async_copy(w1.at[b, at, :], rhs.at[at, :], rhs_sem.at[e]))
        for load in loads:
            load.start()
        lhs_in(0, 0).start()
        for load in loads:
            load.wait()

        @pl.loop(0, tokens // block)
        def _(m):
            slot = lax.rem(m, 2)
            lhs_in(m, slot).wait()

            @pl.when(m + 1 < tokens // block)
            def _():
                lhs_in(m + 1, 1 - slot).start()
            with jax.named_scope('mm1'):
                store(rows_at(m * block, block), dot(lhs[slot], rhs[...]))

    @pl.loop(0, 3)
    def _(b):
        def store(at, value):
            zq[b, at, :] = value.astype(jnp.bfloat16)
        product1(b, wq.at[b, :, ds(i * qw, qw)], store)

        @pl.when(b == 1)
        def _():
            forward1(4)
            issue1(6)

    @pl.loop(0, batch)
    def _(n):
        at = rows_at(n * patches, patches)
        for head in range(heads):
            cols = slice(head * LANES, (head + 1) * LANES)
            query = head_norm(zq[0, at, cols].astype(jnp.float32), qns[...])
            key = head_norm(zq[1, at, cols].astype(jnp.float32), kns[...])
            scores = lax.dot_general(query, key, (((1,), (1,)), ((), ())), preferred_element_type=jnp.float32) * LANES ** -0.5
            scores = jnp.exp(scores - jnp.max(scores, axis=-1, keepdims=True))
            probs = (scores / jnp.sum(scores, axis=-1, keepdims=True)).astype(jnp.bfloat16)
            with jax.named_scope('attn'):
                h[at, cols] = dot(probs, zq[2, at, cols]).astype(jnp.bfloat16)

    forward1(5)
    for c in range(AHEAD // 2):
        issue2(c)

    @pl.loop(0, nub)
    def _(b):
        def store(at, value):
            value = value.astype(jnp.bfloat16).astype(jnp.float32) + bu[:, ds(i * uw + b * qw, qw)]
            value = 0.5 * value * (1.0 + lax.erf(value * 2.0 ** -0.5))
            h[at, ds(qw + b * qw, qw)] = value.astype(jnp.bfloat16)
        product1(b + 3, wu.at[:, ds(i * uw + b * qw, qw)], store)

        @pl.when(b == 1)
        def _():
            forward1(6)
            for c in range(AHEAD // 2, AHEAD):
                issue2(c)

        @pl.when(b == 2)
        def _():
            next2(0)

        @pl.when(b == 3)
        def _():
            next2(1)

    def quarter(yy, core):
        return (2 * yy + core) * rows

    def send_a(c, yy):
        return rcopy(pa.at[lax.rem(c, 2), yy], ra.at[c, yy], as_.at[lax.rem(c, 2)], ar.at[c], {'m2': jp[1]})

    def all_a(c):
        return rcopy(pa.at[lax.rem(c, 2)], ra.at[c], as_.at[lax.rem(c, 2)], ar.at[c], {'m2': jp[1]})

    def send_b(c):
        return rcopy(ss.at[lax.rem(c, 2)], rb.at[c], bs.at[lax.rem(c, 2)], br.at[c], {'m2': jp[2]})

    def send_c(c, k):
        src = rb.at[c, :, ds(ip[1 + 2 * k] * LANES, LANES)]
        return rcopy(src, rc.at[c, k], cs.at[0], cr.at[c], {'m1': ip[1]})

    whole, halves = (0, rows, 0), ((0, block, 0), (block, block, 1))

    def send_d(c, part):
        first, size, k = part
        return rcopy(ud.at[c, first:first + size, :], rd.at[c, first:first + size, :], dsm.at[0], drm.at[c + k], {'m1': ip[2]})

    def result(c, q, part, sem, recv, device):
        first, size, _ = part
        region = out.at[rows_at(q * rows + first, size), ds(c * LANES, LANES)]
        return rcopy(region, region, es.at[sem], recv, device)

    def product2(c):
        slot = lax.rem(c, 2)
        cols, to = ds(c * LANES, LANES), ds(i * LANES, LANES)
        loads = [pltpu.make_async_copy(wo.at[rows_at(i * qw, qw), cols], w2b.at[slot, 0:qw, to], w2b_sem.at[0]),
                 pltpu.make_async_copy(wd.at[rows_at(i * uw, uw), cols], w2b.at[slot, qw:qw + uw, to], w2b_sem.at[1])]
        for load in loads:
            load.start()
        with jax.named_scope('w_f2'):
            part = w2.at[c, 0, :, 0:3 * LANES]
            rcopy(part, part, f2s.at[0], f2r.at[c], {'dp': 1 - g}).wait_recv()
        for e in (1, 2, 3):
            to = ds(ip[e] * LANES, LANES)
            for k in range(2):
                sems = 2 + 4 * (e - 1) + 2 * k
                loads.append(pltpu.make_async_copy(w2.at[c, k, 0:qh, to], w2b.at[slot, k * qh:(k + 1) * qh, to], w2b_sem.at[sems]))
                loads.append(pltpu.make_async_copy(w2.at[c, k, qh:qh + uh, to], w2b.at[slot, qw + k * uh:qw + (k + 1) * uh, to], w2b_sem.at[sems + 1]))
        for load in loads[2:]:
            load.start()

        @pl.when(c >= 2)
        def _():
            all_a(c - 2).wait_send()
        with jax.named_scope('w_w2b'):
            for load in loads:
                load.wait()
        for yy in range(2):
            for sub in range(2):
                at = rows_at(quarter(yy, 1 - jc) + sub * block, block)
                pa[slot, yy, sub * block:(sub + 1) * block, :] = dot(h[at, :], w2b[slot]).astype(jnp.bfloat16)
            send_a(c, yy).start()
        keep = lax.rem(c, 3)
        for yy in range(2):
            for sub in range(2):
                at = rows_at(quarter(yy, jc) + sub * block, block)
                po[keep, yy, sub * block:(sub + 1) * block, :] = dot(h[at, :], w2b[slot]).astype(jnp.bfloat16)

    def add(a, b):
        return (a.astype(jnp.float32) + b.astype(jnp.float32)).astype(jnp.bfloat16)

    def sum_core(d):
        keep = lax.rem(d, 3)
        with jax.named_scope('w_a'):
            rcopy(ra.at[d], ra.at[d], as_.at[0], ar.at[d], {'m2': jp[1]}).wait_recv()
        load = pltpu.make_async_copy(ra.at[d], rav, rav_sem.at[0])
        load.start()

        @pl.when(d >= 2)
        def _():
            send_b(d - 2).wait_send()
        load.wait()
        ss[lax.rem(d, 2)] = add(po[keep, 1 - jy], rav[1 - jy])
        send_b(d).start()
        po[keep, jy] = add(po[keep, jy], rav[jy])

    def sum_y(d):
        with jax.named_scope('w_b'):
            rcopy(rb.at[d], rb.at[d], bs.at[0], br.at[d], {'m2': jp[2]}).wait_recv()
        rb[d] = add(po[lax.rem(d, 3), jy], rb[d])
        for k in range(2):
            send_c(d, k).start()

    def sum_near(d, parts=(whole,)):
        with jax.named_scope('w_c'):
            rcopy(rc.at[d], rc.at[d], cs.at[0], cr.at[d], {'m1': ip[1]}).wait_recv()
        ud[d] = add(rb[d, :, ds(ip[2] * LANES, LANES)], rc[d, 1])
        for part in parts:
            send_d(d, part).start()

    def finish(d, parts=(whole,)):
        cols = ds(d * LANES, LANES)
        for part in parts:
            first, size, k = part
            with jax.named_scope('w_d'):
                send_d(d, part).wait_recv()
            at = slice(first, first + size)
            value = rb[d, at, ds(i * LANES, LANES)].astype(jnp.float32) + rc[d, 0, at].astype(jnp.float32) + rd[d, at].astype(jnp.float32)
            value = xg[i, at, cols].astype(jnp.float32) + value + bo[cols][None, :]
            out[rows_at(j * rows + first, size), cols] = value.astype(jnp.bfloat16)
            result(d, j, part, 0, er.at[d + k], {'m2': jp[2]}).start()
            result(d, j, part, 1, fr.at[0], {'m2': jp[1]}).start()

    def pass_on(d, parts=(whole,)):
        for part in parts:
            with jax.named_scope('w_e'):
                result(d, jp[2], part, 0, er.at[d + part[2]], {'m2': jp[2]}).wait_recv()
            result(d, jp[2], part, 2, fr.at[1], {'m2': jp[1]}).start()

    def run(step, first, last):
        @pl.loop(first, last)
        def _(d):
            step(d)

    early = 2 + 2 * mid

    def late(c, lag, step, last=nc):
        @pl.when((c >= lag) & (c < last))
        def _():
            step(c - lag)

    @pl.loop(0, nc)
    def _(c):
        late(c, 2, sum_y)
        late(c, 1, sum_core)

        @pl.when((c >= 1) & (c + 1 < nc))
        def _():
            next2(c + 1)

        @pl.when(c == nc - 2)
        def _():
            run(sum_near, 0, early)

        @pl.when(c == nc - 1)
        def _():
            run(sum_near, early, early + 2)
            finish(0)
        product2(c)

    sum_core(nc - 1)
    run(sum_near, early + 2, early + 5)
    sum_y(nc - 2)
    run(sum_near, early + 5, nc - 2)
    run(finish, 1, 4)
    sum_y(nc - 1)
    sum_near(nc - 2)
    ready = nc // 2 + 3 * mid
    run(finish, 4, ready)
    sum_near(nc - 1, halves)
    run(finish, ready, nc - 1)
    finish(nc - 1, halves)
    run(pass_on, 0, nc - 1)
    pass_on(nc - 1, halves)

    with jax.named_scope('drain0'):
      for copy in (x_far, x_near, x_fwd, u_far, u_near, u_fwd):
        copy.wait_send()
    for sem in (w1s, f1s):
        part = w1.at[:, 0:3 * half, :]
        rcopy(part, part, sem.at[0], w1r.at[0, 0], {'dp': 1 - g}).wait_send()
    for sem in (w2s, f2s):
        part = w2.at[:, 0, :, 0:3 * LANES]
        rcopy(part, part, sem.at[0], f2r.at[0], {'dp': 1 - g}).wait_send()
    for c in (nc - 2, nc - 1):
        all_a(c).wait_send()
        send_b(c).wait_send()
    rcopy(rc, rc, cs.at[0], cr.at[0], {'m1': ip[1]}).wait_send()
    for sem in (dsm.at[0], es.at[0], es.at[1], es.at[2]):
        rcopy(rd, rd, sem, drm.at[0], {'m1': ip[2]}).wait_send()
    for k in range(2):
        with jax.named_scope('w_f'):
            rcopy(rd, rd, es.at[1], fr.at[k], {'m2': jp[1]}).wait_recv()


def solution(mesh):
    assert mesh.shape['m1'] == 4 and mesh.shape['m2'] == 4 and mesh.shape['dp'] == 2

    def local_layer(x_blk, ln_scale, qn_scale, kn_scale, w_qkv, w_up, b_up, w_o, w_down, b_out):
        batch, patches, dim = x_blk.shape
        tokens = batch * patches
        qw, uw = w_qkv.shape[2] // 4, w_up.shape[1] // 4
        rows, block, nc, nb = tokens // 4, tokens // 8, dim // LANES, 3 + uw // qw
        assert qn_scale.shape[0] == LANES and uw % qw == 0 and nb == 7
        wide = 4 * LANES
        bf16 = jnp.bfloat16
        dma = pltpu.SemaphoreType.DMA
        hbm = pl.BlockSpec(memory_space=pltpu.HBM)
        vmem = pl.BlockSpec(memory_space=pltpu.VMEM)
        ln_rows = min(64, rows)
        out = pl.pallas_call(
            functools.partial(kernel, (batch, patches, dim, qw, uw)),
            out_shape=[
                pltpu.VMEM((tokens, dim), bf16),
                jax.ShapeDtypeStruct((tokens, 4 * dim), bf16),
                jax.ShapeDtypeStruct((nb, 4 * dim, qw), bf16),
                jax.ShapeDtypeStruct((nc, 2, (qw + uw) // 2, wide), bf16),
                jax.ShapeDtypeStruct((nc, 2, rows, wide), bf16)],
            in_specs=[hbm, vmem, vmem, vmem, hbm, hbm, vmem, hbm, hbm, vmem],
            out_specs=[vmem] + [hbm] * 4,
            scratch_shapes=[
                pltpu.VMEM((4, rows, dim), bf16),
                pltpu.VMEM((2, ln_rows, 4 * dim), bf16),
                pltpu.VMEM((3, tokens, qw), bf16),
                pltpu.VMEM((tokens, qw + uw), bf16),
                pltpu.VMEM((4 * dim, qw), bf16),
                pltpu.VMEM((2, block, 4 * dim), bf16),
                pltpu.VMEM((2, qw + uw, wide), bf16),
                pltpu.VMEM((2, 2, rows, wide), bf16),
                pltpu.VMEM((3, 2, rows, wide), bf16),
                pltpu.VMEM((2, rows, wide), bf16),
                pltpu.VMEM((2, rows, wide), bf16),
                pltpu.VMEM((nc, rows, wide), bf16),
                pltpu.VMEM((nc, 2, rows, LANES), bf16),
                pltpu.VMEM((nc, rows, LANES), bf16),
                pltpu.VMEM((nc, rows, LANES), bf16),
                dma((3,)), dma((3,)),
                dma((1,)), dma((nb, 3)), dma((1,)), dma((nb,)),
                dma((3,)), dma((3,)),
                dma((1,)), dma((nc, 3)), dma((1,)), dma((nc,)),
                dma((2,)), dma((nc,)), dma((2,)), dma((nc,)), dma((1,)), dma((nc,)), dma((1,)), dma((nc + 1,)),
                dma((3,)), dma((nc + 1,)), dma((2,)),
                dma((1,)), dma((4,)), dma((2,)), dma((2,)), dma((14,)), dma((1,))],
            compiler_params=pltpu.CompilerParams(collective_id=0, has_side_effects=True, vmem_limit_bytes=60_000_000),
            name='layer',
        )(x_blk.reshape(tokens, dim), ln_scale[None], qn_scale[None], kn_scale[None], w_qkv.transpose(1, 0, 2), w_up,
          b_up[None], w_o, w_down, b_out)[0]
        return out.reshape(batch, patches, dim)

    return jax.shard_map(local_layer, mesh=mesh, in_specs=(P('dp', None, 'm1'), P(), P(), P(), P('m1', None, 'm2'), P('m1', 'm2'), P('m2'), P('m2', 'm1'), P('m2', 'm1'), P('m1')), out_specs=P('dp', None, 'm1'), check_vma=False)
```

```python
import functools

import jax
import jax.numpy as jnp
from jax import lax
from jax.experimental import pallas as pl
from jax.experimental.pallas import tpu as pltpu
from jax.sharding import PartitionSpec as P

LN_EPS = 1e-6
MESH = pl.DeviceIdType.MESH
LANES = 128
AHEAD = 2


def xors(value):
    return (value, value + 1 - 2 * lax.rem(value, 2), value + 2 - 4 * lax.div(value, 2), 3 - value)


def ds(start, size):
    return pl.ds(pl.multiple_of(start, size if size < LANES else LANES), size)


def rows_at(start, size):
    return pl.ds(pl.multiple_of(start, 8), size)


def rcopy(src, dst, send_sem, recv_sem, device):
    return pltpu.make_async_remote_copy(src_ref=src, dst_ref=dst, send_sem=send_sem, recv_sem=recv_sem, device_id=device, device_id_type=MESH)


def dot(lhs, rhs):
    return jnp.dot(lhs, rhs, preferred_element_type=jnp.float32)


def head_norm(values, scale):
    mean = jnp.mean(values, axis=-1, keepdims=True)
    centered = values - mean
    variance = jnp.mean(centered * centered, axis=-1, keepdims=True)
    return (centered * lax.rsqrt(variance + LN_EPS) * scale).astype(jnp.bfloat16)


def kernel(sizes, x, lns, qns, kns, wq, wu, bu, wo, wd, bo,
           out, u, w1, w2, ra,
           xg, ubl, zq, h, rhs, lhs, w2b, pa, po, rav, ss, rb, rc, ud, rd,
           xs, xr, w1s, w1r, f1s, f1r, us, ur, w2s, w2r, f2s, f2r,
           as_, ar, bs, br, cs, cr, dsm, drm, es, er, fr, own_sem, rhs_sem, lhs_sem, ub_sem, w2b_sem, rav_sem):
    batch, patches, dim, qw, uw = sizes
    tokens = batch * patches
    rows = tokens // 4
    block = rows // 2
    half = dim // 2
    total = 4 * dim
    nub = uw // qw
    nc = dim // LANES
    wide = 4 * LANES
    heads = qw // LANES
    ln_rows = min(64, rows)

    g, i, j = lax.axis_index('dp'), lax.axis_index('m1'), lax.axis_index('m2')
    ip, jp = xors(i), xors(j)
    jy, jc = lax.div(j, 2), lax.rem(j, 2)
    mid = lax.div(lax.rem(i + 1, 4), 2)
    peers1 = ((0, ip[1]), (2 - mid, ip[3] + mid * (ip[2] - ip[3])), (1 + mid, ip[2] + mid * (ip[3] - ip[2])))

    barrier = pltpu.get_barrier_semaphore()
    peers = [{'m1': ip[e]} for e in (1, 2, 3)] + [{'m2': jp[e]} for e in (1, 2, 3)] + [{'dp': 1 - g}]
    for peer in peers:
        pl.semaphore_signal(barrier, inc=1, device_id=peer, device_id_type=MESH)
    with jax.named_scope('barrier'):
        pl.semaphore_wait(barrier, len(peers))

    mine = rows_at(j * rows, rows)
    x_far = rcopy(x.at[mine, :], xg.at[i], xs.at[0], xr.at[0], {'m1': ip[2]})
    x_near = rcopy(x.at[mine, :], xg.at[i], xs.at[1], xr.at[1], {'m1': ip[1]})
    x_own = pltpu.make_async_copy(x.at[mine, :], xg.at[i], own_sem.at[0])
    x_far.start()
    x_near.start()
    x_own.start()
    x_far_in = rcopy(xg.at[ip[2]], xg.at[ip[2]], xs.at[0], xr.at[0], {'m1': ip[2]})
    with jax.named_scope('w_xfar'):
        x_far_in.wait_recv()
    x_fwd = rcopy(xg.at[ip[2]], xg.at[ip[2]], xs.at[2], xr.at[2], {'m1': ip[1]})
    x_fwd.start()

    def z1(b, e):
        t = ip[e]
        if b < 3:
            src = wq.at[b, rows_at(g * half, half), ds(t * qw, qw)]
        else:
            src = wu.at[rows_at(g * half, half), ds(t * uw + (b - 3) * qw, qw)]
        return rcopy(src, w1.at[b, rows_at(i * dim + g * half, half), :], w1s.at[0], w1r.at[b, e - 1], {'m1': t})

    def piece1(b, k, s):
        part = w1.at[b, rows_at(s * dim + g * half, half), :]
        return (rcopy(part, part, w1s.at[0], w1r.at[b, k], {'m1': s}), rcopy(part, part, f1s.at[0], f1r.at[b], {'dp': 1 - g}))

    def forward1(b):
        for k, s in peers1:
            arrival, swap = piece1(b, k, s)
            with jax.named_scope('w_z1'):
                arrival.wait_recv()
            swap.start()

    def swapped1(b):
        part = w1.at[b, 0:3 * half, :]
        return rcopy(part, part, f1s.at[0], f1r.at[b], {'dp': 1 - g})

    def issue1(b):
        for e in (2, 3, 1):
            z1(b, e).start()

    issue1(0)
    issue1(1)

    qh, uh = qw // 2, uw // 2

    def z2(c, e):
        t = ip[e]
        cols, to = ds(c * LANES, LANES), ds(i * LANES, LANES)
        return [rcopy(wd.at[rows_at(t * uw + g * uh, uh), cols], w2.at[c, g, qh:qh + uh, to], w2s.at[0], w2r.at[c, e - 1], {'m1': t}),
                rcopy(wo.at[rows_at(t * qw + g * qh, qh), cols], w2.at[c, g, 0:qh, to], w2s.at[0], w2r.at[c, e - 1], {'m1': t})]

    def issue2(c):
        for e in (2, 3, 1):
            for copy in z2(c, e):
                copy.start()

    def forward2(c):
        for k, s in peers1:
            part = w2.at[c, g, :, ds(s * LANES, LANES)]
            with jax.named_scope('w_z2'):
                rcopy(part, part, w2s.at[0], w2r.at[c, k], {'m1': s}).wait_recv()
            rcopy(part, part, f2s.at[0], f2r.at[c], {'dp': 1 - g}).start()

    def next2(c):
        forward2(c)

        @pl.when(c + AHEAD < nc)
        def _():
            issue2(c + AHEAD)

    with jax.named_scope('w_xown'):
        x_own.wait()
    with jax.named_scope('w_xnear'):
        rcopy(xg.at[ip[1]], xg.at[ip[1]], xs.at[1], xr.at[1], {'m1': ip[1]}).wait_recv()
    with jax.named_scope('w_xfwd'):
        rcopy(xg.at[ip[3]], xg.at[ip[3]], xs.at[2], xr.at[2], {'m1': ip[1]}).wait_recv()

    def u_out(r, slot):
        return pltpu.make_async_copy(ubl.at[slot], u.at[rows_at(j * rows + r * ln_rows, ln_rows), :], ub_sem.at[slot])

    @pl.loop(0, rows // ln_rows)
    def _(r):
        slot = lax.rem(r, 2)

        @pl.when(r >= 2)
        def _():
            u_out(r - 2, slot).wait()
        at = rows_at(r * ln_rows, ln_rows)
        parts = [xg[s, at, :].astype(jnp.float32) for s in range(4)]
        mean = sum(jnp.sum(part, axis=-1, keepdims=True) for part in parts) / total
        parts = [part - mean for part in parts]
        variance = sum(jnp.sum(part * part, axis=-1, keepdims=True) for part in parts) / total
        inverse = lax.rsqrt(variance + LN_EPS)
        for s in range(4):
            cols = slice(s * dim, (s + 1) * dim)
            ubl[slot, :, cols] = (parts[s] * inverse * lns[:, cols]).astype(jnp.bfloat16)
        u_out(r, slot).start()

    for r in range(max(0, rows // ln_rows - 2), rows // ln_rows):
        u_out(r, r % 2).wait()

    def u_rows(q):
        return u.at[rows_at(q * rows, rows), :]

    u_far = rcopy(u_rows(j), u_rows(j), us.at[0], ur.at[0], {'m2': jp[2]})
    u_near = rcopy(u_rows(j), u_rows(j), us.at[1], ur.at[1], {'m2': jp[1]})
    u_far.start()
    u_near.start()
    for b in range(4):
        forward1(b)
        issue1(b + 2)
    with jax.named_scope('w_ufar'):
        rcopy(u_rows(jp[2]), u_rows(jp[2]), us.at[0], ur.at[0], {'m2': jp[2]}).wait_recv()
    u_fwd = rcopy(u_rows(jp[2]), u_rows(jp[2]), us.at[2], ur.at[2], {'m2': jp[1]})
    u_fwd.start()
    rcopy(u_rows(jp[1]), u_rows(jp[1]), us.at[1], ur.at[1], {'m2': jp[1]}).wait_recv()
    with jax.named_scope('w_ufwd'):
        rcopy(u_rows(jp[3]), u_rows(jp[3]), us.at[2], ur.at[2], {'m2': jp[1]}).wait_recv()

    def lhs_in(m, slot):
        return pltpu.make_async_copy(u.at[rows_at(m * block, block), :], lhs.at[slot], lhs_sem.at[slot])

    def product1(b, own, store):
        with jax.named_scope('w_f1'):
            swapped1(b).wait_recv()
        loads = [pltpu.make_async_copy(own, rhs.at[rows_at(i * dim, dim), :], rhs_sem.at[0])]
        for e in (1, 2, 3):
            at = rows_at(ip[e] * dim, dim)
            loads.append(pltpu.make_async_copy(w1.at[b, at, :], rhs.at[at, :], rhs_sem.at[e]))
        for load in loads:
            load.start()
        lhs_in(0, 0).start()
        for load in loads:
            load.wait()

        @pl.loop(0, tokens // block)
        def _(m):
            slot = lax.rem(m, 2)
            lhs_in(m, slot).wait()

            @pl.when(m + 1 < tokens // block)
            def _():
                lhs_in(m + 1, 1 - slot).start()
            with jax.named_scope('mm1'):
                store(rows_at(m * block, block), dot(lhs[slot], rhs[...]))

    @pl.loop(0, 3)
    def _(b):
        def store(at, value):
            zq[b, at, :] = value.astype(jnp.bfloat16)
        product1(b, wq.at[b, :, ds(i * qw, qw)], store)

        @pl.when(b == 1)
        def _():
            forward1(4)
            issue1(6)

    @pl.loop(0, batch)
    def _(n):
        at = rows_at(n * patches, patches)
        for head in range(heads):
            cols = slice(head * LANES, (head + 1) * LANES)
            query = head_norm(zq[0, at, cols].astype(jnp.float32), qns[...])
            key = head_norm(zq[1, at, cols].astype(jnp.float32), kns[...])
            scores = lax.dot_general(query, key, (((1,), (1,)), ((), ())), preferred_element_type=jnp.float32) * LANES ** -0.5
            scores = jnp.exp(scores - jnp.max(scores, axis=-1, keepdims=True))
            probs = (scores / jnp.sum(scores, axis=-1, keepdims=True)).astype(jnp.bfloat16)
            with jax.named_scope('attn'):
                h[at, cols] = dot(probs, zq[2, at, cols]).astype(jnp.bfloat16)

    forward1(5)
    for c in range(AHEAD // 2):
        issue2(c)

    @pl.loop(0, nub)
    def _(b):
        def store(at, value):
            value = value.astype(jnp.bfloat16).astype(jnp.float32) + bu[:, ds(i * uw + b * qw, qw)]
            value = 0.5 * value * (1.0 + lax.erf(value * 2.0 ** -0.5))
            h[at, ds(qw + b * qw, qw)] = value.astype(jnp.bfloat16)
        product1(b + 3, wu.at[:, ds(i * uw + b * qw, qw)], store)

        @pl.when(b == 1)
        def _():
            forward1(6)
            for c in range(AHEAD // 2, AHEAD):
                issue2(c)

        @pl.when(b == 2)
        def _():
            next2(0)

        @pl.when(b == 3)
        def _():
            next2(1)

    def quarter(yy, core):
        return (2 * yy + core) * rows

    def send_a(c, yy):
        return rcopy(pa.at[lax.rem(c, 2), yy], ra.at[c, yy], as_.at[lax.rem(c, 2)], ar.at[c], {'m2': jp[1]})

    def all_a(c):
        return rcopy(pa.at[lax.rem(c, 2)], ra.at[c], as_.at[lax.rem(c, 2)], ar.at[c], {'m2': jp[1]})

    def send_b(c):
        return rcopy(ss.at[lax.rem(c, 2)], rb.at[c], bs.at[lax.rem(c, 2)], br.at[c], {'m2': jp[2]})

    def send_c(c, k):
        src = rb.at[c, :, ds(ip[1 + 2 * k] * LANES, LANES)]
        return rcopy(src, rc.at[c, k], cs.at[0], cr.at[c], {'m1': ip[1]})

    def send_d(c):
        return rcopy(ud.at[c], rd.at[c], dsm.at[0], drm.at[c], {'m1': ip[2]})

    def out_part(c, q):
        return out.at[rows_at(q * rows, rows), ds(c * LANES, LANES)]

    def result(c, q, sem, recv, device):
        part = out_part(c, q)
        return rcopy(part, part, es.at[sem], recv, device)

    def product2(c):
        slot = lax.rem(c, 2)
        cols, to = ds(c * LANES, LANES), ds(i * LANES, LANES)
        loads = [pltpu.make_async_copy(wo.at[rows_at(i * qw, qw), cols], w2b.at[slot, 0:qw, to], w2b_sem.at[0]),
                 pltpu.make_async_copy(wd.at[rows_at(i * uw, uw), cols], w2b.at[slot, qw:qw + uw, to], w2b_sem.at[1])]
        for load in loads:
            load.start()
        with jax.named_scope('w_f2'):
            part = w2.at[c, 0, :, 0:3 * LANES]
            rcopy(part, part, f2s.at[0], f2r.at[c], {'dp': 1 - g}).wait_recv()
        for e in (1, 2, 3):
            to = ds(ip[e] * LANES, LANES)
            for k in range(2):
                sems = 2 + 4 * (e - 1) + 2 * k
                loads.append(pltpu.make_async_copy(w2.at[c, k, 0:qh, to], w2b.at[slot, k * qh:(k + 1) * qh, to], w2b_sem.at[sems]))
                loads.append(pltpu.make_async_copy(w2.at[c, k, qh:qh + uh, to], w2b.at[slot, qw + k * uh:qw + (k + 1) * uh, to], w2b_sem.at[sems + 1]))
        for load in loads[2:]:
            load.start()

        @pl.when(c >= 2)
        def _():
            all_a(c - 2).wait_send()
        with jax.named_scope('w_w2b'):
            for load in loads:
                load.wait()
        for yy in range(2):
            for sub in range(2):
                at = rows_at(quarter(yy, 1 - jc) + sub * block, block)
                pa[slot, yy, sub * block:(sub + 1) * block, :] = dot(h[at, :], w2b[slot]).astype(jnp.bfloat16)
            send_a(c, yy).start()
        keep = lax.rem(c, 3)
        for yy in range(2):
            for sub in range(2):
                at = rows_at(quarter(yy, jc) + sub * block, block)
                po[keep, yy, sub * block:(sub + 1) * block, :] = dot(h[at, :], w2b[slot]).astype(jnp.bfloat16)

    def add(a, b):
        return (a.astype(jnp.float32) + b.astype(jnp.float32)).astype(jnp.bfloat16)

    def sum_core(d):
        keep = lax.rem(d, 3)
        with jax.named_scope('w_a'):
            rcopy(ra.at[d], ra.at[d], as_.at[0], ar.at[d], {'m2': jp[1]}).wait_recv()
        load = pltpu.make_async_copy(ra.at[d], rav, rav_sem.at[0])
        load.start()

        @pl.when(d >= 2)
        def _():
            send_b(d - 2).wait_send()
        load.wait()
        ss[lax.rem(d, 2)] = add(po[keep, 1 - jy], rav[1 - jy])
        send_b(d).start()
        po[keep, jy] = add(po[keep, jy], rav[jy])

    def sum_y(d):
        with jax.named_scope('w_b'):
            rcopy(rb.at[d], rb.at[d], bs.at[0], br.at[d], {'m2': jp[2]}).wait_recv()
        rb[d] = add(po[lax.rem(d, 3), jy], rb[d])
        for k in range(2):
            send_c(d, k).start()

    def sum_near(d):
        with jax.named_scope('w_c'):
            rcopy(rc.at[d], rc.at[d], cs.at[0], cr.at[d], {'m1': ip[1]}).wait_recv()
        ud[d] = add(rb[d, :, ds(ip[2] * LANES, LANES)], rc[d, 1])
        send_d(d).start()

    def finish(d):
        with jax.named_scope('w_d'):
            rcopy(rd.at[d], rd.at[d], dsm.at[0], drm.at[d], {'m1': ip[2]}).wait_recv()
        cols = ds(d * LANES, LANES)
        value = rb[d, :, ds(i * LANES, LANES)].astype(jnp.float32) + rc[d, 0].astype(jnp.float32) + rd[d].astype(jnp.float32)
        value = xg[i, :, cols].astype(jnp.float32) + value + bo[cols][None, :]
        out[rows_at(j * rows, rows), cols] = value.astype(jnp.bfloat16)
        result(d, j, 0, er.at[d], {'m2': jp[2]}).start()
        result(d, j, 1, fr.at[0], {'m2': jp[1]}).start()

    def pass_on(d):
        with jax.named_scope('w_e'):
            result(d, jp[2], 0, er.at[d], {'m2': jp[2]}).wait_recv()
        result(d, jp[2], 2, fr.at[1], {'m2': jp[1]}).start()

    def run(step, first, last):
        @pl.loop(first, last)
        def _(d):
            step(d)

    early = 2 + 2 * mid

    def late(c, lag, step, last=nc):
        @pl.when((c >= lag) & (c < last))
        def _():
            step(c - lag)

    @pl.loop(0, nc)
    def _(c):
        late(c, 2, sum_y)
        late(c, 1, sum_core)

        @pl.when((c == nc - 2) & (mid == 1))
        def _():
            run(sum_near, 0, early)

        @pl.when((c >= 1) & (c + 1 < nc))
        def _():
            next2(c + 1)

        @pl.when((c == nc - 2) & (mid == 0))
        def _():
            run(sum_near, 0, early)

        @pl.when(c == nc - 1)
        def _():
            run(sum_near, early, early + 2)
            finish(0)
        product2(c)

    sum_core(nc - 1)
    run(sum_near, early + 2, early + 5)
    sum_y(nc - 2)
    run(sum_near, early + 5, nc - 2)
    run(finish, 1, 4)
    sum_y(nc - 1)
    sum_near(nc - 2)
    ready = nc // 2 + 3 * mid
    run(finish, 4, ready)
    sum_near(nc - 1)
    run(finish, ready, nc)
    run(pass_on, 0, nc)

    with jax.named_scope('drain0'):
      for copy in (x_far, x_near, x_fwd, u_far, u_near, u_fwd):
        copy.wait_send()
    for sem in (w1s, f1s):
        part = w1.at[:, 0:3 * half, :]
        rcopy(part, part, sem.at[0], w1r.at[0, 0], {'dp': 1 - g}).wait_send()
    for sem in (w2s, f2s):
        part = w2.at[:, 0, :, 0:3 * LANES]
        rcopy(part, part, sem.at[0], f2r.at[0], {'dp': 1 - g}).wait_send()
    for c in (nc - 2, nc - 1):
        all_a(c).wait_send()
        send_b(c).wait_send()
    rcopy(rc, rc, cs.at[0], cr.at[0], {'m1': ip[1]}).wait_send()
    for sem in (dsm.at[0], es.at[0], es.at[1], es.at[2]):
        rcopy(rd, rd, sem, drm.at[0], {'m1': ip[2]}).wait_send()
    for k in range(2):
        with jax.named_scope('w_f'):
            rcopy(rd, rd, es.at[1], fr.at[k], {'m2': jp[1]}).wait_recv()


def solution(mesh):
    assert mesh.shape['m1'] == 4 and mesh.shape['m2'] == 4 and mesh.shape['dp'] == 2

    def local_layer(x_blk, ln_scale, qn_scale, kn_scale, w_qkv, w_up, b_up, w_o, w_down, b_out):
        batch, patches, dim = x_blk.shape
        tokens = batch * patches
        qw, uw = w_qkv.shape[2] // 4, w_up.shape[1] // 4
        rows, block, nc, nb = tokens // 4, tokens // 8, dim // LANES, 3 + uw // qw
        assert qn_scale.shape[0] == LANES and uw % qw == 0 and nb == 7
        wide = 4 * LANES
        bf16 = jnp.bfloat16
        dma = pltpu.SemaphoreType.DMA
        hbm = pl.BlockSpec(memory_space=pltpu.HBM)
        vmem = pl.BlockSpec(memory_space=pltpu.VMEM)
        ln_rows = min(64, rows)
        out = pl.pallas_call(
            functools.partial(kernel, (batch, patches, dim, qw, uw)),
            out_shape=[
                pltpu.VMEM((tokens, dim), bf16),
                jax.ShapeDtypeStruct((tokens, 4 * dim), bf16),
                jax.ShapeDtypeStruct((nb, 4 * dim, qw), bf16),
                jax.ShapeDtypeStruct((nc, 2, (qw + uw) // 2, wide), bf16),
                jax.ShapeDtypeStruct((nc, 2, rows, wide), bf16)],
            in_specs=[hbm, vmem, vmem, vmem, hbm, hbm, vmem, hbm, hbm, vmem],
            out_specs=[vmem] + [hbm] * 4,
            scratch_shapes=[
                pltpu.VMEM((4, rows, dim), bf16),
                pltpu.VMEM((2, ln_rows, 4 * dim), bf16),
                pltpu.VMEM((3, tokens, qw), bf16),
                pltpu.VMEM((tokens, qw + uw), bf16),
                pltpu.VMEM((4 * dim, qw), bf16),
                pltpu.VMEM((2, block, 4 * dim), bf16),
                pltpu.VMEM((2, qw + uw, wide), bf16),
                pltpu.VMEM((2, 2, rows, wide), bf16),
                pltpu.VMEM((3, 2, rows, wide), bf16),
                pltpu.VMEM((2, rows, wide), bf16),
                pltpu.VMEM((2, rows, wide), bf16),
                pltpu.VMEM((nc, rows, wide), bf16),
                pltpu.VMEM((nc, 2, rows, LANES), bf16),
                pltpu.VMEM((nc, rows, LANES), bf16),
                pltpu.VMEM((nc, rows, LANES), bf16),
                dma((3,)), dma((3,)),
                dma((1,)), dma((nb, 3)), dma((1,)), dma((nb,)),
                dma((3,)), dma((3,)),
                dma((1,)), dma((nc, 3)), dma((1,)), dma((nc,)),
                dma((2,)), dma((nc,)), dma((2,)), dma((nc,)), dma((1,)), dma((nc,)), dma((1,)), dma((nc,)),
                dma((3,)), dma((nc,)), dma((2,)),
                dma((1,)), dma((4,)), dma((2,)), dma((2,)), dma((14,)), dma((1,))],
            compiler_params=pltpu.CompilerParams(collective_id=0, has_side_effects=True, vmem_limit_bytes=60_000_000),
            name='layer',
        )(x_blk.reshape(tokens, dim), ln_scale[None], qn_scale[None], kn_scale[None], w_qkv.transpose(1, 0, 2), w_up,
          b_up[None], w_o, w_down, b_out)[0]
        return out.reshape(batch, patches, dim)

    return jax.shard_map(local_layer, mesh=mesh, in_specs=(P('dp', None, 'm1'), P(), P(), P(), P('m1', None, 'm2'), P('m1', 'm2'), P('m2'), P('m2', 'm1'), P('m2', 'm1'), P('m1')), out_specs=P('dp', None, 'm1'), check_vma=False)
```

```python
import functools

import jax
import jax.numpy as jnp
from jax import lax
from jax.experimental import pallas as pl
from jax.experimental.pallas import tpu as pltpu
from jax.sharding import PartitionSpec as P

LN_EPS = 1e-6
MESH = pl.DeviceIdType.MESH
LANES = 128
AHEAD = 2


def xors(value):
    return (value, value + 1 - 2 * lax.rem(value, 2), value + 2 - 4 * lax.div(value, 2), 3 - value)


def ds(start, size):
    return pl.ds(pl.multiple_of(start, size if size < LANES else LANES), size)


def rows_at(start, size):
    return pl.ds(pl.multiple_of(start, 8), size)


def rcopy(src, dst, send_sem, recv_sem, device):
    return pltpu.make_async_remote_copy(src_ref=src, dst_ref=dst, send_sem=send_sem, recv_sem=recv_sem, device_id=device, device_id_type=MESH)


def dot(lhs, rhs):
    return jnp.dot(lhs, rhs, preferred_element_type=jnp.float32)


def head_norm(values, scale):
    mean = jnp.mean(values, axis=-1, keepdims=True)
    centered = values - mean
    variance = jnp.mean(centered * centered, axis=-1, keepdims=True)
    return (centered * lax.rsqrt(variance + LN_EPS) * scale).astype(jnp.bfloat16)


def kernel(sizes, x, lns, qns, kns, wq, wu, bu, wo, wd, bo,
           out, u, w1, w2, ra,
           xg, ubl, zq, h, rhs, lhs, w2b, pa, po, rav, ss, rb, rc, ud, rd,
           xs, xr, w1s, w1r, f1s, f1r, us, ur, w2s, w2r, f2s, f2r,
           as_, ar, bs, br, cs, cr, dsm, drm, es, er, fr, own_sem, rhs_sem, lhs_sem, ub_sem, w2b_sem, rav_sem):
    batch, patches, dim, qw, uw = sizes
    tokens = batch * patches
    rows = tokens // 4
    block = rows // 2
    half = dim // 2
    total = 4 * dim
    nub = uw // qw
    nc = dim // LANES
    wide = 4 * LANES
    heads = qw // LANES
    ln_rows = min(64, rows)

    g, i, j = lax.axis_index('dp'), lax.axis_index('m1'), lax.axis_index('m2')
    ip, jp = xors(i), xors(j)
    jy, jc = lax.div(j, 2), lax.rem(j, 2)
    mid = lax.div(lax.rem(i + 1, 4), 2)
    peers1 = ((0, ip[1]), (2 - mid, ip[3] + mid * (ip[2] - ip[3])), (1 + mid, ip[2] + mid * (ip[3] - ip[2])))

    barrier = pltpu.get_barrier_semaphore()
    peers = [{'m1': ip[e]} for e in (1, 2, 3)] + [{'m2': jp[e]} for e in (1, 2, 3)] + [{'dp': 1 - g}]
    for peer in peers:
        pl.semaphore_signal(barrier, inc=1, device_id=peer, device_id_type=MESH)
    with jax.named_scope('barrier'):
        pl.semaphore_wait(barrier, len(peers))

    mine = rows_at(j * rows, rows)
    x_far = rcopy(x.at[mine, :], xg.at[i], xs.at[0], xr.at[0], {'m1': ip[2]})
    x_near = rcopy(x.at[mine, :], xg.at[i], xs.at[1], xr.at[1], {'m1': ip[1]})
    x_own = pltpu.make_async_copy(x.at[mine, :], xg.at[i], own_sem.at[0])
    x_far.start()
    x_near.start()
    x_own.start()
    x_far_in = rcopy(xg.at[ip[2]], xg.at[ip[2]], xs.at[0], xr.at[0], {'m1': ip[2]})
    with jax.named_scope('w_xfar'):
        x_far_in.wait_recv()
    x_fwd = rcopy(xg.at[ip[2]], xg.at[ip[2]], xs.at[2], xr.at[2], {'m1': ip[1]})
    x_fwd.start()

    def z1(b, e):
        t = ip[e]
        if b < 3:
            src = wq.at[b, rows_at(g * half, half), ds(t * qw, qw)]
        else:
            src = wu.at[rows_at(g * half, half), ds(t * uw + (b - 3) * qw, qw)]
        return rcopy(src, w1.at[b, rows_at(i * dim + g * half, half), :], w1s.at[0], w1r.at[b, e - 1], {'m1': t})

    def piece1(b, k, s):
        part = w1.at[b, rows_at(s * dim + g * half, half), :]
        return (rcopy(part, part, w1s.at[0], w1r.at[b, k], {'m1': s}), rcopy(part, part, f1s.at[0], f1r.at[b], {'dp': 1 - g}))

    def forward1(b):
        for k, s in peers1:
            arrival, swap = piece1(b, k, s)
            with jax.named_scope('w_z1'):
                arrival.wait_recv()
            swap.start()

    def swapped1(b):
        part = w1.at[b, 0:3 * half, :]
        return rcopy(part, part, f1s.at[0], f1r.at[b], {'dp': 1 - g})

    def issue1(b):
        for e in (2, 3, 1):
            z1(b, e).start()

    issue1(0)
    issue1(1)

    qh, uh = qw // 2, uw // 2

    def z2(c, e):
        t = ip[e]
        cols, to = ds(c * LANES, LANES), ds(i * LANES, LANES)
        return [rcopy(wd.at[rows_at(t * uw + g * uh, uh), cols], w2.at[c, g, qh:qh + uh, to], w2s.at[0], w2r.at[c, e - 1], {'m1': t}),
                rcopy(wo.at[rows_at(t * qw + g * qh, qh), cols], w2.at[c, g, 0:qh, to], w2s.at[0], w2r.at[c, e - 1], {'m1': t})]

    def send2(c, *distances):
        for e in distances:
            for copy in z2(c, e):
                copy.start()

    def issue2(c):
        send2(c, 2, 3)

        @pl.when(c < nc - 6)
        def _():
            send2(c, 1)

    def forward2(c):
        for k, s in peers1:
            part = w2.at[c, g, :, ds(s * LANES, LANES)]
            with jax.named_scope('w_z2'):
                rcopy(part, part, w2s.at[0], w2r.at[c, k], {'m1': s}).wait_recv()
            rcopy(part, part, f2s.at[0], f2r.at[c], {'dp': 1 - g}).start()

    def next2(c):
        forward2(c)

        @pl.when(c + AHEAD < nc)
        def _():
            issue2(c + AHEAD)

    with jax.named_scope('w_xown'):
        x_own.wait()
    with jax.named_scope('w_xnear'):
        rcopy(xg.at[ip[1]], xg.at[ip[1]], xs.at[1], xr.at[1], {'m1': ip[1]}).wait_recv()
    with jax.named_scope('w_xfwd'):
        rcopy(xg.at[ip[3]], xg.at[ip[3]], xs.at[2], xr.at[2], {'m1': ip[1]}).wait_recv()

    def u_out(r, slot):
        return pltpu.make_async_copy(ubl.at[slot], u.at[rows_at(j * rows + r * ln_rows, ln_rows), :], ub_sem.at[slot])

    @pl.loop(0, rows // ln_rows)
    def _(r):
        slot = lax.rem(r, 2)

        @pl.when(r >= 2)
        def _():
            u_out(r - 2, slot).wait()
        at = rows_at(r * ln_rows, ln_rows)
        parts = [xg[s, at, :].astype(jnp.float32) for s in range(4)]
        mean = sum(jnp.sum(part, axis=-1, keepdims=True) for part in parts) / total
        parts = [part - mean for part in parts]
        variance = sum(jnp.sum(part * part, axis=-1, keepdims=True) for part in parts) / total
        inverse = lax.rsqrt(variance + LN_EPS)
        for s in range(4):
            cols = slice(s * dim, (s + 1) * dim)
            ubl[slot, :, cols] = (parts[s] * inverse * lns[:, cols]).astype(jnp.bfloat16)
        u_out(r, slot).start()

    for r in range(max(0, rows // ln_rows - 2), rows // ln_rows):
        u_out(r, r % 2).wait()

    def u_rows(q):
        return u.at[rows_at(q * rows, rows), :]

    u_far = rcopy(u_rows(j), u_rows(j), us.at[0], ur.at[0], {'m2': jp[2]})
    u_near = rcopy(u_rows(j), u_rows(j), us.at[1], ur.at[1], {'m2': jp[1]})
    u_far.start()
    u_near.start()
    for b in range(4):
        forward1(b)
        issue1(b + 2)
        if b:
            send2(nc - 7 + b, 1)
    with jax.named_scope('w_ufar'):
        rcopy(u_rows(jp[2]), u_rows(jp[2]), us.at[0], ur.at[0], {'m2': jp[2]}).wait_recv()
    u_fwd = rcopy(u_rows(jp[2]), u_rows(jp[2]), us.at[2], ur.at[2], {'m2': jp[1]})
    u_fwd.start()
    rcopy(u_rows(jp[1]), u_rows(jp[1]), us.at[1], ur.at[1], {'m2': jp[1]}).wait_recv()
    with jax.named_scope('w_ufwd'):
        rcopy(u_rows(jp[3]), u_rows(jp[3]), us.at[2], ur.at[2], {'m2': jp[1]}).wait_recv()

    def lhs_in(m, slot):
        return pltpu.make_async_copy(u.at[rows_at(m * block, block), :], lhs.at[slot], lhs_sem.at[slot])

    def product1(b, own, store):
        with jax.named_scope('w_f1'):
            swapped1(b).wait_recv()
        loads = [pltpu.make_async_copy(own, rhs.at[rows_at(i * dim, dim), :], rhs_sem.at[0])]
        for e in (1, 2, 3):
            at = rows_at(ip[e] * dim, dim)
            loads.append(pltpu.make_async_copy(w1.at[b, at, :], rhs.at[at, :], rhs_sem.at[e]))
        for load in loads:
            load.start()
        lhs_in(0, 0).start()
        for load in loads:
            load.wait()

        @pl.loop(0, tokens // block)
        def _(m):
            slot = lax.rem(m, 2)
            lhs_in(m, slot).wait()

            @pl.when(m + 1 < tokens // block)
            def _():
                lhs_in(m + 1, 1 - slot).start()
            with jax.named_scope('mm1'):
                store(rows_at(m * block, block), dot(lhs[slot], rhs[...]))

    @pl.loop(0, 3)
    def _(b):
        def store(at, value):
            zq[b, at, :] = value.astype(jnp.bfloat16)
        product1(b, wq.at[b, :, ds(i * qw, qw)], store)

        @pl.when(b == 1)
        def _():
            forward1(4)
            issue1(6)
            send2(nc - 3, 1)

    @pl.loop(0, batch)
    def _(n):
        at = rows_at(n * patches, patches)
        for head in range(heads):
            cols = slice(head * LANES, (head + 1) * LANES)
            query = head_norm(zq[0, at, cols].astype(jnp.float32), qns[...])
            key = head_norm(zq[1, at, cols].astype(jnp.float32), kns[...])
            scores = lax.dot_general(query, key, (((1,), (1,)), ((), ())), preferred_element_type=jnp.float32) * LANES ** -0.5
            scores = jnp.exp(scores - jnp.max(scores, axis=-1, keepdims=True))
            probs = (scores / jnp.sum(scores, axis=-1, keepdims=True)).astype(jnp.bfloat16)
            with jax.named_scope('attn'):
                h[at, cols] = dot(probs, zq[2, at, cols]).astype(jnp.bfloat16)

    forward1(5)
    for c in range(AHEAD // 2):
        issue2(c)
    send2(nc - 2, 1)

    @pl.loop(0, nub)
    def _(b):
        def store(at, value):
            value = value.astype(jnp.bfloat16).astype(jnp.float32) + bu[:, ds(i * uw + b * qw, qw)]
            value = 0.5 * value * (1.0 + lax.erf(value * 2.0 ** -0.5))
            h[at, ds(qw + b * qw, qw)] = value.astype(jnp.bfloat16)
        product1(b + 3, wu.at[:, ds(i * uw + b * qw, qw)], store)

        @pl.when(b == 1)
        def _():
            forward1(6)
            for c in range(AHEAD // 2, AHEAD):
                issue2(c)
            send2(nc - 1, 1)

        @pl.when(b == 2)
        def _():
            next2(0)

        @pl.when(b == 3)
        def _():
            next2(1)

    def quarter(yy, core):
        return (2 * yy + core) * rows

    def send_a(c, yy):
        return rcopy(pa.at[lax.rem(c, 2), yy], ra.at[c, yy], as_.at[lax.rem(c, 2)], ar.at[c], {'m2': jp[1]})

    def all_a(c):
        return rcopy(pa.at[lax.rem(c, 2)], ra.at[c], as_.at[lax.rem(c, 2)], ar.at[c], {'m2': jp[1]})

    def send_b(c):
        return rcopy(ss.at[lax.rem(c, 2)], rb.at[c], bs.at[lax.rem(c, 2)], br.at[c], {'m2': jp[2]})

    def send_c(c, k):
        src = rb.at[c, :, ds(ip[1 + 2 * k] * LANES, LANES)]
        return rcopy(src, rc.at[c, k], cs.at[0], cr.at[c], {'m1': ip[1]})

    def send_d(c):
        return rcopy(ud.at[c], rd.at[c], dsm.at[0], drm.at[c], {'m1': ip[2]})

    def out_part(c, q):
        return out.at[rows_at(q * rows, rows), ds(c * LANES, LANES)]

    def result(c, q, sem, recv, device):
        part = out_part(c, q)
        return rcopy(part, part, es.at[sem], recv, device)

    def product2(c):
        slot = lax.rem(c, 2)
        cols, to = ds(c * LANES, LANES), ds(i * LANES, LANES)
        loads = [pltpu.make_async_copy(wo.at[rows_at(i * qw, qw), cols], w2b.at[slot, 0:qw, to], w2b_sem.at[0]),
                 pltpu.make_async_copy(wd.at[rows_at(i * uw, uw), cols], w2b.at[slot, qw:qw + uw, to], w2b_sem.at[1])]
        for load in loads:
            load.start()
        with jax.named_scope('w_f2'):
            part = w2.at[c, 0, :, 0:3 * LANES]
            rcopy(part, part, f2s.at[0], f2r.at[c], {'dp': 1 - g}).wait_recv()
        for e in (1, 2, 3):
            to = ds(ip[e] * LANES, LANES)
            for k in range(2):
                sems = 2 + 4 * (e - 1) + 2 * k
                loads.append(pltpu.make_async_copy(w2.at[c, k, 0:qh, to], w2b.at[slot, k * qh:(k + 1) * qh, to], w2b_sem.at[sems]))
                loads.append(pltpu.make_async_copy(w2.at[c, k, qh:qh + uh, to], w2b.at[slot, qw + k * uh:qw + (k + 1) * uh, to], w2b_sem.at[sems + 1]))
        for load in loads[2:]:
            load.start()

        @pl.when(c >= 2)
        def _():
            all_a(c - 2).wait_send()
        with jax.named_scope('w_w2b'):
            for load in loads:
                load.wait()
        for yy in range(2):
            for sub in range(2):
                at = rows_at(quarter(yy, 1 - jc) + sub * block, block)
                pa[slot, yy, sub * block:(sub + 1) * block, :] = dot(h[at, :], w2b[slot]).astype(jnp.bfloat16)
            send_a(c, yy).start()
        keep = lax.rem(c, 3)
        for yy in range(2):
            for sub in range(2):
                at = rows_at(quarter(yy, jc) + sub * block, block)
                po[keep, yy, sub * block:(sub + 1) * block, :] = dot(h[at, :], w2b[slot]).astype(jnp.bfloat16)

    def add(a, b):
        return (a.astype(jnp.float32) + b.astype(jnp.float32)).astype(jnp.bfloat16)

    def sum_core(d):
        keep = lax.rem(d, 3)
        with jax.named_scope('w_a'):
            rcopy(ra.at[d], ra.at[d], as_.at[0], ar.at[d], {'m2': jp[1]}).wait_recv()
        load = pltpu.make_async_copy(ra.at[d], rav, rav_sem.at[0])
        load.start()

        @pl.when(d >= 2)
        def _():
            send_b(d - 2).wait_send()
        load.wait()
        ss[lax.rem(d, 2)] = add(po[keep, 1 - jy], rav[1 - jy])
        send_b(d).start()
        po[keep, jy] = add(po[keep, jy], rav[jy])

    def sum_y(d):
        with jax.named_scope('w_b'):
            rcopy(rb.at[d], rb.at[d], bs.at[0], br.at[d], {'m2': jp[2]}).wait_recv()
        rb[d] = add(po[lax.rem(d, 3), jy], rb[d])
        for k in range(2):
            send_c(d, k).start()

    def sum_near(d):
        with jax.named_scope('w_c'):
            rcopy(rc.at[d], rc.at[d], cs.at[0], cr.at[d], {'m1': ip[1]}).wait_recv()
        ud[d] = add(rb[d, :, ds(ip[2] * LANES, LANES)], rc[d, 1])
        send_d(d).start()

    def finish(d):
        with jax.named_scope('w_d'):
            rcopy(rd.at[d], rd.at[d], dsm.at[0], drm.at[d], {'m1': ip[2]}).wait_recv()
        cols = ds(d * LANES, LANES)
        value = rb[d, :, ds(i * LANES, LANES)].astype(jnp.float32) + rc[d, 0].astype(jnp.float32) + rd[d].astype(jnp.float32)
        value = xg[i, :, cols].astype(jnp.float32) + value + bo[cols][None, :]
        out[rows_at(j * rows, rows), cols] = value.astype(jnp.bfloat16)
        result(d, j, 0, er.at[d], {'m2': jp[2]}).start()
        result(d, j, 1, fr.at[0], {'m2': jp[1]}).start()

    def pass_on(d):
        with jax.named_scope('w_e'):
            result(d, jp[2], 0, er.at[d], {'m2': jp[2]}).wait_recv()
        result(d, jp[2], 2, fr.at[1], {'m2': jp[1]}).start()

    def run(step, first, last):
        @pl.loop(first, last)
        def _(d):
            step(d)

    early = 2 + 2 * mid

    def late(c, lag, step, last=nc):
        @pl.when((c >= lag) & (c < last))
        def _():
            step(c - lag)

    @pl.loop(0, nc)
    def _(c):
        late(c, 2, sum_y)
        late(c, 1, sum_core)

        @pl.when((c == nc - 2) & (mid == 1))
        def _():
            run(sum_near, 0, early)

        @pl.when((c >= 1) & (c + 1 < nc))
        def _():
            next2(c + 1)

        @pl.when((c == nc - 2) & (mid == 0))
        def _():
            run(sum_near, 0, early)

        @pl.when(c == nc - 1)
        def _():
            run(sum_near, early, early + 2)
            finish(0)
        product2(c)

    sum_core(nc - 1)
    run(sum_near, early + 2, early + 5)
    sum_y(nc - 2)
    run(sum_near, early + 5, nc - 2)
    run(finish, 1, 4)
    sum_y(nc - 1)
    sum_near(nc - 2)
    ready = nc // 2 + 3 * mid
    run(finish, 4, ready)
    sum_near(nc - 1)
    run(finish, ready, nc)
    run(pass_on, 0, nc)

    with jax.named_scope('drain0'):
      for copy in (x_far, x_near, x_fwd, u_far, u_near, u_fwd):
        copy.wait_send()
    for sem in (w1s, f1s):
        part = w1.at[:, 0:3 * half, :]
        rcopy(part, part, sem.at[0], w1r.at[0, 0], {'dp': 1 - g}).wait_send()
    for sem in (w2s, f2s):
        part = w2.at[:, 0, :, 0:3 * LANES]
        rcopy(part, part, sem.at[0], f2r.at[0], {'dp': 1 - g}).wait_send()
    for c in (nc - 2, nc - 1):
        all_a(c).wait_send()
        send_b(c).wait_send()
    rcopy(rc, rc, cs.at[0], cr.at[0], {'m1': ip[1]}).wait_send()
    for sem in (dsm.at[0], es.at[0], es.at[1], es.at[2]):
        rcopy(rd, rd, sem, drm.at[0], {'m1': ip[2]}).wait_send()
    for k in range(2):
        with jax.named_scope('w_f'):
            rcopy(rd, rd, es.at[1], fr.at[k], {'m2': jp[1]}).wait_recv()


def solution(mesh):
    assert mesh.shape['m1'] == 4 and mesh.shape['m2'] == 4 and mesh.shape['dp'] == 2

    def local_layer(x_blk, ln_scale, qn_scale, kn_scale, w_qkv, w_up, b_up, w_o, w_down, b_out):
        batch, patches, dim = x_blk.shape
        tokens = batch * patches
        qw, uw = w_qkv.shape[2] // 4, w_up.shape[1] // 4
        rows, block, nc, nb = tokens // 4, tokens // 8, dim // LANES, 3 + uw // qw
        assert qn_scale.shape[0] == LANES and uw % qw == 0 and nb == 7
        wide = 4 * LANES
        bf16 = jnp.bfloat16
        dma = pltpu.SemaphoreType.DMA
        hbm = pl.BlockSpec(memory_space=pltpu.HBM)
        vmem = pl.BlockSpec(memory_space=pltpu.VMEM)
        ln_rows = min(64, rows)
        out = pl.pallas_call(
            functools.partial(kernel, (batch, patches, dim, qw, uw)),
            out_shape=[
                pltpu.VMEM((tokens, dim), bf16),
                jax.ShapeDtypeStruct((tokens, 4 * dim), bf16),
                jax.ShapeDtypeStruct((nb, 4 * dim, qw), bf16),
                jax.ShapeDtypeStruct((nc, 2, (qw + uw) // 2, wide), bf16),
                jax.ShapeDtypeStruct((nc, 2, rows, wide), bf16)],
            in_specs=[hbm, vmem, vmem, vmem, hbm, hbm, vmem, hbm, hbm, vmem],
            out_specs=[vmem] + [hbm] * 4,
            scratch_shapes=[
                pltpu.VMEM((4, rows, dim), bf16),
                pltpu.VMEM((2, ln_rows, 4 * dim), bf16),
                pltpu.VMEM((3, tokens, qw), bf16),
                pltpu.VMEM((tokens, qw + uw), bf16),
                pltpu.VMEM((4 * dim, qw), bf16),
                pltpu.VMEM((2, block, 4 * dim), bf16),
                pltpu.VMEM((2, qw + uw, wide), bf16),
                pltpu.VMEM((2, 2, rows, wide), bf16),
                pltpu.VMEM((3, 2, rows, wide), bf16),
                pltpu.VMEM((2, rows, wide), bf16),
                pltpu.VMEM((2, rows, wide), bf16),
                pltpu.VMEM((nc, rows, wide), bf16),
                pltpu.VMEM((nc, 2, rows, LANES), bf16),
                pltpu.VMEM((nc, rows, LANES), bf16),
                pltpu.VMEM((nc, rows, LANES), bf16),
                dma((3,)), dma((3,)),
                dma((1,)), dma((nb, 3)), dma((1,)), dma((nb,)),
                dma((3,)), dma((3,)),
                dma((1,)), dma((nc, 3)), dma((1,)), dma((nc,)),
                dma((2,)), dma((nc,)), dma((2,)), dma((nc,)), dma((1,)), dma((nc,)), dma((1,)), dma((nc,)),
                dma((3,)), dma((nc,)), dma((2,)),
                dma((1,)), dma((4,)), dma((2,)), dma((2,)), dma((14,)), dma((1,))],
            compiler_params=pltpu.CompilerParams(collective_id=0, has_side_effects=True, vmem_limit_bytes=60_000_000),
            name='layer',
        )(x_blk.reshape(tokens, dim), ln_scale[None], qn_scale[None], kn_scale[None], w_qkv.transpose(1, 0, 2), w_up,
          b_up[None], w_o, w_down, b_out)[0]
        return out.reshape(batch, patches, dim)

    return jax.shard_map(local_layer, mesh=mesh, in_specs=(P('dp', None, 'm1'), P(), P(), P(), P('m1', None, 'm2'), P('m1', 'm2'), P('m2'), P('m2', 'm1'), P('m2', 'm1'), P('m1')), out_specs=P('dp', None, 'm1'), check_vma=False)
```

```python
import functools

import jax
import jax.numpy as jnp
from jax import lax
from jax.experimental import pallas as pl
from jax.experimental.pallas import tpu as pltpu
from jax.sharding import PartitionSpec as P

LN_EPS = 1e-6
MESH = pl.DeviceIdType.MESH
LANES = 128
AHEAD = 2


def xors(value):
    return (value, value + 1 - 2 * lax.rem(value, 2), value + 2 - 4 * lax.div(value, 2), 3 - value)


def ds(start, size):
    return pl.ds(pl.multiple_of(start, size if size < LANES else LANES), size)


def rows_at(start, size):
    return pl.ds(pl.multiple_of(start, 8), size)


def rcopy(src, dst, send_sem, recv_sem, device):
    return pltpu.make_async_remote_copy(src_ref=src, dst_ref=dst, send_sem=send_sem, recv_sem=recv_sem, device_id=device, device_id_type=MESH)


def dot(lhs, rhs):
    return jnp.dot(lhs, rhs, preferred_element_type=jnp.float32)


def head_norm(values, scale):
    mean = jnp.mean(values, axis=-1, keepdims=True)
    centered = values - mean
    variance = jnp.mean(centered * centered, axis=-1, keepdims=True)
    return (centered * lax.rsqrt(variance + LN_EPS) * scale).astype(jnp.bfloat16)


def kernel(sizes, x, lns, qns, kns, wq, wu, bu, wo, wd, bo,
           out, u, w1, w2, ra,
           xg, ubl, zq, h, rhs, lhs, w2b, pa, po, rav, ss, rb, rc, ud, rd,
           xs, xr, w1s, w1r, f1s, f1r, us, ur, w2s, w2r, f2s, f2r,
           as_, ar, bs, br, cs, cr, dsm, drm, es, er, fr, own_sem, rhs_sem, lhs_sem, ub_sem, w2b_sem, rav_sem):
    batch, patches, dim, qw, uw = sizes
    tokens = batch * patches
    rows = tokens // 4
    block = rows // 2
    half = dim // 2
    total = 4 * dim
    nub = uw // qw
    nc = dim // LANES
    wide = 4 * LANES
    heads = qw // LANES
    ln_rows = min(64, rows)

    g, i, j = lax.axis_index('dp'), lax.axis_index('m1'), lax.axis_index('m2')
    ip, jp = xors(i), xors(j)
    jy, jc = lax.div(j, 2), lax.rem(j, 2)
    mid = lax.div(lax.rem(i + 1, 4), 2)
    peers1 = ((0, ip[1]), (2 - mid, ip[3] + mid * (ip[2] - ip[3])), (1 + mid, ip[2] + mid * (ip[3] - ip[2])))

    barrier = pltpu.get_barrier_semaphore()
    peers = [{'m1': ip[e]} for e in (1, 2, 3)] + [{'m2': jp[e]} for e in (1, 2, 3)] + [{'dp': 1 - g}]
    for peer in peers:
        pl.semaphore_signal(barrier, inc=1, device_id=peer, device_id_type=MESH)
    pl.semaphore_wait(barrier, len(peers))

    mine = rows_at(j * rows, rows)
    x_far = rcopy(x.at[mine, :], xg.at[i], xs.at[0], xr.at[0], {'m1': ip[2]})
    x_near = rcopy(x.at[mine, :], xg.at[i], xs.at[1], xr.at[1], {'m1': ip[1]})
    x_own = pltpu.make_async_copy(x.at[mine, :], xg.at[i], own_sem.at[0])
    x_far.start()
    x_near.start()
    x_own.start()
    x_far_in = rcopy(xg.at[ip[2]], xg.at[ip[2]], xs.at[0], xr.at[0], {'m1': ip[2]})
    x_far_in.wait_recv()
    x_fwd = rcopy(xg.at[ip[2]], xg.at[ip[2]], xs.at[2], xr.at[2], {'m1': ip[1]})
    x_fwd.start()

    def z1(b, e):
        t = ip[e]
        if b < 3:
            src = wq.at[b, rows_at(g * half, half), ds(t * qw, qw)]
        else:
            src = wu.at[rows_at(g * half, half), ds(t * uw + (b - 3) * qw, qw)]
        return rcopy(src, w1.at[b, rows_at(i * dim + g * half, half), :], w1s.at[0], w1r.at[b, e - 1], {'m1': t})

    def piece1(b, k, s):
        part = w1.at[b, rows_at(s * dim + g * half, half), :]
        return (rcopy(part, part, w1s.at[0], w1r.at[b, k], {'m1': s}), rcopy(part, part, f1s.at[0], f1r.at[b], {'dp': 1 - g}))

    def forward1(b):
        for k, s in peers1:
            arrival, swap = piece1(b, k, s)
            arrival.wait_recv()
            swap.start()

    def swapped1(b):
        part = w1.at[b, 0:3 * half, :]
        return rcopy(part, part, f1s.at[0], f1r.at[b], {'dp': 1 - g})

    def issue1(b):
        for e in (2, 3, 1):
            z1(b, e).start()

    issue1(0)
    issue1(1)

    qh, uh = qw // 2, uw // 2

    def z2(c, e):
        t = ip[e]
        cols, to = ds(c * LANES, LANES), ds(i * LANES, LANES)
        return [rcopy(wd.at[rows_at(t * uw + g * uh, uh), cols], w2.at[c, g, qh:qh + uh, to], w2s.at[0], w2r.at[c, e - 1], {'m1': t}),
                rcopy(wo.at[rows_at(t * qw + g * qh, qh), cols], w2.at[c, g, 0:qh, to], w2s.at[0], w2r.at[c, e - 1], {'m1': t})]

    def issue2(c):
        for e in (2, 3, 1):
            for copy in z2(c, e):
                copy.start()

    def forward2(c):
        for k, s in peers1:
            part = w2.at[c, g, :, ds(s * LANES, LANES)]
            rcopy(part, part, w2s.at[0], w2r.at[c, k], {'m1': s}).wait_recv()
            rcopy(part, part, f2s.at[0], f2r.at[c], {'dp': 1 - g}).start()

    def next2(c):
        forward2(c)

        @pl.when(c + AHEAD < nc)
        def _():
            issue2(c + AHEAD)

    x_own.wait()
    rcopy(xg.at[ip[1]], xg.at[ip[1]], xs.at[1], xr.at[1], {'m1': ip[1]}).wait_recv()
    rcopy(xg.at[ip[3]], xg.at[ip[3]], xs.at[2], xr.at[2], {'m1': ip[1]}).wait_recv()

    def u_out(r, slot):
        return pltpu.make_async_copy(ubl.at[slot], u.at[rows_at(j * rows + r * ln_rows, ln_rows), :], ub_sem.at[slot])

    @pl.loop(0, rows // ln_rows)
    def _(r):
        slot = lax.rem(r, 2)

        @pl.when(r >= 2)
        def _():
            u_out(r - 2, slot).wait()
        at = rows_at(r * ln_rows, ln_rows)
        parts = [xg[s, at, :].astype(jnp.float32) for s in range(4)]
        mean = sum(jnp.sum(part, axis=-1, keepdims=True) for part in parts) / total
        parts = [part - mean for part in parts]
        variance = sum(jnp.sum(part * part, axis=-1, keepdims=True) for part in parts) / total
        inverse = lax.rsqrt(variance + LN_EPS)
        for s in range(4):
            cols = slice(s * dim, (s + 1) * dim)
            ubl[slot, :, cols] = (parts[s] * inverse * lns[:, cols]).astype(jnp.bfloat16)
        u_out(r, slot).start()

    for r in range(max(0, rows // ln_rows - 2), rows // ln_rows):
        u_out(r, r % 2).wait()

    def u_rows(q):
        return u.at[rows_at(q * rows, rows), :]

    u_far = rcopy(u_rows(j), u_rows(j), us.at[0], ur.at[0], {'m2': jp[2]})
    u_near = rcopy(u_rows(j), u_rows(j), us.at[1], ur.at[1], {'m2': jp[1]})
    u_far.start()
    u_near.start()
    for b in range(4):
        forward1(b)
        issue1(b + 2)
    rcopy(u_rows(jp[2]), u_rows(jp[2]), us.at[0], ur.at[0], {'m2': jp[2]}).wait_recv()
    u_fwd = rcopy(u_rows(jp[2]), u_rows(jp[2]), us.at[2], ur.at[2], {'m2': jp[1]})
    u_fwd.start()
    rcopy(u_rows(jp[1]), u_rows(jp[1]), us.at[1], ur.at[1], {'m2': jp[1]}).wait_recv()
    rcopy(u_rows(jp[3]), u_rows(jp[3]), us.at[2], ur.at[2], {'m2': jp[1]}).wait_recv()

    def lhs_in(m, slot):
        return pltpu.make_async_copy(u.at[rows_at(m * block, block), :], lhs.at[slot], lhs_sem.at[slot])

    def product1(b, own, store):
        swapped1(b).wait_recv()
        loads = [pltpu.make_async_copy(own, rhs.at[rows_at(i * dim, dim), :], rhs_sem.at[0])]
        for e in (1, 2, 3):
            at = rows_at(ip[e] * dim, dim)
            loads.append(pltpu.make_async_copy(w1.at[b, at, :], rhs.at[at, :], rhs_sem.at[e]))
        for load in loads:
            load.start()
        lhs_in(0, 0).start()
        for load in loads:
            load.wait()

        @pl.loop(0, tokens // block)
        def _(m):
            slot = lax.rem(m, 2)
            lhs_in(m, slot).wait()

            @pl.when(m + 1 < tokens // block)
            def _():
                lhs_in(m + 1, 1 - slot).start()
            store(rows_at(m * block, block), dot(lhs[slot], rhs[...]))

    @pl.loop(0, 3)
    def _(b):
        def store(at, value):
            zq[b, at, :] = value.astype(jnp.bfloat16)
        product1(b, wq.at[b, :, ds(i * qw, qw)], store)

        @pl.when(b == 1)
        def _():
            forward1(4)
            issue1(6)

    @pl.loop(0, batch)
    def _(n):
        at = rows_at(n * patches, patches)
        for head in range(heads):
            cols = slice(head * LANES, (head + 1) * LANES)
            query = head_norm(zq[0, at, cols].astype(jnp.float32), qns[...])
            key = head_norm(zq[1, at, cols].astype(jnp.float32), kns[...])
            scores = lax.dot_general(query, key, (((1,), (1,)), ((), ())), preferred_element_type=jnp.float32) * LANES ** -0.5
            scores = jnp.exp(scores - jnp.max(scores, axis=-1, keepdims=True))
            probs = (scores / jnp.sum(scores, axis=-1, keepdims=True)).astype(jnp.bfloat16)
            h[at, cols] = dot(probs, zq[2, at, cols]).astype(jnp.bfloat16)

    forward1(5)
    for c in range(AHEAD // 2):
        issue2(c)

    @pl.loop(0, nub)
    def _(b):
        def store(at, value):
            value = value.astype(jnp.bfloat16).astype(jnp.float32) + bu[:, ds(i * uw + b * qw, qw)]
            value = 0.5 * value * (1.0 + lax.erf(value * 2.0 ** -0.5))
            h[at, ds(qw + b * qw, qw)] = value.astype(jnp.bfloat16)
        product1(b + 3, wu.at[:, ds(i * uw + b * qw, qw)], store)

        @pl.when(b == 1)
        def _():
            forward1(6)
            for c in range(AHEAD // 2, AHEAD):
                issue2(c)

        @pl.when(b == 2)
        def _():
            next2(0)

        @pl.when(b == 3)
        def _():
            next2(1)

    def quarter(yy, core):
        return (2 * yy + core) * rows

    def send_a(c, yy):
        return rcopy(pa.at[lax.rem(c, 2), yy], ra.at[c, yy], as_.at[lax.rem(c, 2)], ar.at[c], {'m2': jp[1]})

    def all_a(c):
        return rcopy(pa.at[lax.rem(c, 2)], ra.at[c], as_.at[lax.rem(c, 2)], ar.at[c], {'m2': jp[1]})

    def send_b(c):
        return rcopy(ss.at[lax.rem(c, 2)], rb.at[c], bs.at[lax.rem(c, 2)], br.at[c], {'m2': jp[2]})

    def send_c(c, k):
        src = rb.at[c, :, ds(ip[1 + 2 * k] * LANES, LANES)]
        return rcopy(src, rc.at[c, k], cs.at[0], cr.at[c], {'m1': ip[1]})

    def send_d(c):
        return rcopy(ud.at[c], rd.at[c], dsm.at[0], drm.at[c], {'m1': ip[2]})

    def out_part(c, q):
        return out.at[rows_at(q * rows, rows), ds(c * LANES, LANES)]

    def result(c, q, sem, recv, device):
        part = out_part(c, q)
        return rcopy(part, part, es.at[sem], recv, device)

    def product2(c):
        slot = lax.rem(c, 2)
        cols, to = ds(c * LANES, LANES), ds(i * LANES, LANES)
        loads = [pltpu.make_async_copy(wo.at[rows_at(i * qw, qw), cols], w2b.at[slot, 0:qw, to], w2b_sem.at[0]),
                 pltpu.make_async_copy(wd.at[rows_at(i * uw, uw), cols], w2b.at[slot, qw:qw + uw, to], w2b_sem.at[1])]
        for load in loads:
            load.start()
        part = w2.at[c, 0, :, 0:3 * LANES]
        rcopy(part, part, f2s.at[0], f2r.at[c], {'dp': 1 - g}).wait_recv()
        for e in (1, 2, 3):
            to = ds(ip[e] * LANES, LANES)
            for k in range(2):
                sems = 2 + 4 * (e - 1) + 2 * k
                loads.append(pltpu.make_async_copy(w2.at[c, k, 0:qh, to], w2b.at[slot, k * qh:(k + 1) * qh, to], w2b_sem.at[sems]))
                loads.append(pltpu.make_async_copy(w2.at[c, k, qh:qh + uh, to], w2b.at[slot, qw + k * uh:qw + (k + 1) * uh, to], w2b_sem.at[sems + 1]))
        for load in loads[2:]:
            load.start()

        @pl.when(c >= 2)
        def _():
            all_a(c - 2).wait_send()
        for load in loads:
            load.wait()
        for yy in range(2):
            for sub in range(2):
                at = rows_at(quarter(yy, 1 - jc) + sub * block, block)
                pa[slot, yy, sub * block:(sub + 1) * block, :] = dot(h[at, :], w2b[slot]).astype(jnp.bfloat16)
            send_a(c, yy).start()
        keep = lax.rem(c, 3)
        for yy in range(2):
            for sub in range(2):
                at = rows_at(quarter(yy, jc) + sub * block, block)
                po[keep, yy, sub * block:(sub + 1) * block, :] = dot(h[at, :], w2b[slot]).astype(jnp.bfloat16)

    def add(a, b):
        return (a.astype(jnp.float32) + b.astype(jnp.float32)).astype(jnp.bfloat16)

    def sum_core(d):
        keep = lax.rem(d, 3)
        rcopy(ra.at[d], ra.at[d], as_.at[0], ar.at[d], {'m2': jp[1]}).wait_recv()
        load = pltpu.make_async_copy(ra.at[d], rav, rav_sem.at[0])
        load.start()

        @pl.when(d >= 2)
        def _():
            send_b(d - 2).wait_send()
        load.wait()
        ss[lax.rem(d, 2)] = add(po[keep, 1 - jy], rav[1 - jy])
        send_b(d).start()
        po[keep, jy] = add(po[keep, jy], rav[jy])

    def sum_y(d):
        rcopy(rb.at[d], rb.at[d], bs.at[0], br.at[d], {'m2': jp[2]}).wait_recv()
        rb[d] = add(po[lax.rem(d, 3), jy], rb[d])
        for k in range(2):
            send_c(d, k).start()

    def sum_near(d):
        rcopy(rc.at[d], rc.at[d], cs.at[0], cr.at[d], {'m1': ip[1]}).wait_recv()
        ud[d] = add(rb[d, :, ds(ip[2] * LANES, LANES)], rc[d, 1])
        send_d(d).start()

    def finish(d):
        rcopy(rd.at[d], rd.at[d], dsm.at[0], drm.at[d], {'m1': ip[2]}).wait_recv()
        cols = ds(d * LANES, LANES)
        value = rb[d, :, ds(i * LANES, LANES)].astype(jnp.float32) + rc[d, 0].astype(jnp.float32) + rd[d].astype(jnp.float32)
        value = xg[i, :, cols].astype(jnp.float32) + value + bo[cols][None, :]
        out[rows_at(j * rows, rows), cols] = value.astype(jnp.bfloat16)
        result(d, j, 0, er.at[d], {'m2': jp[2]}).start()
        result(d, j, 1, fr.at[0], {'m2': jp[1]}).start()

    def pass_on(d):
        result(d, jp[2], 0, er.at[d], {'m2': jp[2]}).wait_recv()
        result(d, jp[2], 2, fr.at[1], {'m2': jp[1]}).start()

    def run(step, first, last):
        @pl.loop(first, last)
        def _(d):
            step(d)

    early = 2 + 2 * mid

    def late(c, lag, step, last=nc):
        @pl.when((c >= lag) & (c < last))
        def _():
            step(c - lag)

    @pl.loop(0, nc)
    def _(c):
        late(c, 2, sum_y)
        late(c, 1, sum_core)

        @pl.when((c >= 1) & (c + 1 < nc))
        def _():
            next2(c + 1)

        @pl.when(c == nc - 2)
        def _():
            run(sum_near, 0, early)

        @pl.when(c == nc - 1)
        def _():
            run(sum_near, early, early + 2)
            finish(0)
        product2(c)

    sum_core(nc - 1)
    run(sum_near, early + 2, early + 5)
    sum_y(nc - 2)
    run(sum_near, early + 5, nc - 2)
    run(finish, 1, 4)
    sum_y(nc - 1)
    sum_near(nc - 2)
    run(finish, 4, nc - 3)
    sum_near(nc - 1)
    run(finish, nc - 3, nc)
    run(pass_on, 0, nc)

    for copy in (x_far, x_near, x_fwd, u_far, u_near, u_fwd):
      copy.wait_send()
    for sem in (w1s, f1s):
        part = w1.at[:, 0:3 * half, :]
        rcopy(part, part, sem.at[0], w1r.at[0, 0], {'dp': 1 - g}).wait_send()
    for sem in (w2s, f2s):
        part = w2.at[:, 0, :, 0:3 * LANES]
        rcopy(part, part, sem.at[0], f2r.at[0], {'dp': 1 - g}).wait_send()
    for c in (nc - 2, nc - 1):
        all_a(c).wait_send()
        send_b(c).wait_send()
    rcopy(rc, rc, cs.at[0], cr.at[0], {'m1': ip[1]}).wait_send()
    for sem in (dsm.at[0], es.at[0], es.at[1], es.at[2]):
        rcopy(rd, rd, sem, drm.at[0], {'m1': ip[2]}).wait_send()
    for k in range(2):
        rcopy(rd, rd, es.at[1], fr.at[k], {'m2': jp[1]}).wait_recv()


def solution(mesh):
    assert mesh.shape['m1'] == 4 and mesh.shape['m2'] == 4 and mesh.shape['dp'] == 2

    def local_layer(x_blk, ln_scale, qn_scale, kn_scale, w_qkv, w_up, b_up, w_o, w_down, b_out):
        batch, patches, dim = x_blk.shape
        tokens = batch * patches
        qw, uw = w_qkv.shape[2] // 4, w_up.shape[1] // 4
        rows, block, nc, nb = tokens // 4, tokens // 8, dim // LANES, 3 + uw // qw
        assert qn_scale.shape[0] == LANES and uw % qw == 0 and nb == 7
        wide = 4 * LANES
        bf16 = jnp.bfloat16
        dma = pltpu.SemaphoreType.DMA
        hbm = pl.BlockSpec(memory_space=pltpu.HBM)
        vmem = pl.BlockSpec(memory_space=pltpu.VMEM)
        ln_rows = min(64, rows)
        out = pl.pallas_call(
            functools.partial(kernel, (batch, patches, dim, qw, uw)),
            out_shape=[
                pltpu.VMEM((tokens, dim), bf16),
                jax.ShapeDtypeStruct((tokens, 4 * dim), bf16),
                jax.ShapeDtypeStruct((nb, 4 * dim, qw), bf16),
                jax.ShapeDtypeStruct((nc, 2, (qw + uw) // 2, wide), bf16),
                jax.ShapeDtypeStruct((nc, 2, rows, wide), bf16)],
            in_specs=[hbm, vmem, vmem, vmem, hbm, hbm, vmem, hbm, hbm, vmem],
            out_specs=[vmem] + [hbm] * 4,
            scratch_shapes=[
                pltpu.VMEM((4, rows, dim), bf16),
                pltpu.VMEM((2, ln_rows, 4 * dim), bf16),
                pltpu.VMEM((3, tokens, qw), bf16),
                pltpu.VMEM((tokens, qw + uw), bf16),
                pltpu.VMEM((4 * dim, qw), bf16),
                pltpu.VMEM((2, block, 4 * dim), bf16),
                pltpu.VMEM((2, qw + uw, wide), bf16),
                pltpu.VMEM((2, 2, rows, wide), bf16),
                pltpu.VMEM((3, 2, rows, wide), bf16),
                pltpu.VMEM((2, rows, wide), bf16),
                pltpu.VMEM((2, rows, wide), bf16),
                pltpu.VMEM((nc, rows, wide), bf16),
                pltpu.VMEM((nc, 2, rows, LANES), bf16),
                pltpu.VMEM((nc, rows, LANES), bf16),
                pltpu.VMEM((nc, rows, LANES), bf16),
                dma((3,)), dma((3,)),
                dma((1,)), dma((nb, 3)), dma((1,)), dma((nb,)),
                dma((3,)), dma((3,)),
                dma((1,)), dma((nc, 3)), dma((1,)), dma((nc,)),
                dma((2,)), dma((nc,)), dma((2,)), dma((nc,)), dma((1,)), dma((nc,)), dma((1,)), dma((nc,)),
                dma((3,)), dma((nc,)), dma((2,)),
                dma((1,)), dma((4,)), dma((2,)), dma((2,)), dma((14,)), dma((1,))],
            compiler_params=pltpu.CompilerParams(collective_id=0, has_side_effects=True, vmem_limit_bytes=60_000_000),
            name='layer',
        )(x_blk.reshape(tokens, dim), ln_scale[None], qn_scale[None], kn_scale[None], w_qkv.transpose(1, 0, 2), w_up,
          b_up[None], w_o, w_down, b_out)[0]
        return out.reshape(batch, patches, dim)

    return jax.shard_map(local_layer, mesh=mesh, in_specs=(P('dp', None, 'm1'), P(), P(), P(), P('m1', None, 'm2'), P('m1', 'm2'), P('m2'), P('m2', 'm1'), P('m2', 'm1'), P('m1')), out_specs=P('dp', None, 'm1'), check_vma=False)
```

```python
import functools

import jax
import jax.numpy as jnp
from jax import lax
from jax.experimental import pallas as pl
from jax.experimental.pallas import tpu as pltpu
from jax.sharding import PartitionSpec as P

LN_EPS = 1e-6
MESH = pl.DeviceIdType.MESH
LANES = 128
AHEAD = 2


def xors(value):
    return (value, value + 1 - 2 * lax.rem(value, 2), value + 2 - 4 * lax.div(value, 2), 3 - value)


def ds(start, size):
    return pl.ds(pl.multiple_of(start, size if size < LANES else LANES), size)


def rows_at(start, size):
    return pl.ds(pl.multiple_of(start, 8), size)


def rcopy(src, dst, send_sem, recv_sem, device):
    return pltpu.make_async_remote_copy(src_ref=src, dst_ref=dst, send_sem=send_sem, recv_sem=recv_sem, device_id=device, device_id_type=MESH)


def dot(lhs, rhs):
    return jnp.dot(lhs, rhs, preferred_element_type=jnp.float32)


def head_norm(values, scale):
    mean = jnp.mean(values, axis=-1, keepdims=True)
    centered = values - mean
    variance = jnp.mean(centered * centered, axis=-1, keepdims=True)
    return (centered * lax.rsqrt(variance + LN_EPS) * scale).astype(jnp.bfloat16)


def kernel(sizes, x, lns, qns, kns, wq, wu, bu, wo, wd, bo,
           out, u, w1, w2, ra,
           xg, ubl, zq, h, rhs, lhs, w2b, pa, po, rav, ss, rb, rc, ud, rd,
           xs, xr, w1s, w1r, f1s, f1r, us, ur, w2s, w2r, f2s, f2r,
           as_, ar, bs, br, cs, cr, dsm, drm, es, er, fr, own_sem, rhs_sem, lhs_sem, ub_sem, w2b_sem, rav_sem):
    batch, patches, dim, qw, uw = sizes
    tokens = batch * patches
    rows = tokens // 4
    block = rows // 2
    half = dim // 2
    total = 4 * dim
    nub = uw // qw
    nc = dim // LANES
    wide = 4 * LANES
    heads = qw // LANES
    ln_rows = min(64, rows)

    g, i, j = lax.axis_index('dp'), lax.axis_index('m1'), lax.axis_index('m2')
    ip, jp = xors(i), xors(j)
    jy, jc = lax.div(j, 2), lax.rem(j, 2)
    mid = lax.div(lax.rem(i + 1, 4), 2)
    peers1 = ((0, ip[1]), (2 - mid, ip[3] + mid * (ip[2] - ip[3])), (1 + mid, ip[2] + mid * (ip[3] - ip[2])))

    barrier = pltpu.get_barrier_semaphore()
    peers = [{'m1': ip[e]} for e in (1, 2, 3)] + [{'m2': jp[e]} for e in (1, 2, 3)] + [{'dp': 1 - g}]
    for peer in peers:
        pl.semaphore_signal(barrier, inc=1, device_id=peer, device_id_type=MESH)
    pl.semaphore_wait(barrier, len(peers))

    mine = rows_at(j * rows, rows)
    x_far = rcopy(x.at[mine, :], xg.at[i], xs.at[0], xr.at[0], {'m1': ip[2]})
    x_near = rcopy(x.at[mine, :], xg.at[i], xs.at[1], xr.at[1], {'m1': ip[1]})
    x_own = pltpu.make_async_copy(x.at[mine, :], xg.at[i], own_sem.at[0])
    x_far.start()
    x_near.start()
    x_own.start()
    x_far_in = rcopy(xg.at[ip[2]], xg.at[ip[2]], xs.at[0], xr.at[0], {'m1': ip[2]})
    x_far_in.wait_recv()
    x_fwd = rcopy(xg.at[ip[2]], xg.at[ip[2]], xs.at[2], xr.at[2], {'m1': ip[1]})
    x_fwd.start()

    def z1(b, e):
        t = ip[e]
        if b < 3:
            src = wq.at[b, rows_at(g * half, half), ds(t * qw, qw)]
        else:
            src = wu.at[rows_at(g * half, half), ds(t * uw + (b - 3) * qw, qw)]
        return rcopy(src, w1.at[b, rows_at(i * dim + g * half, half), :], w1s.at[0], w1r.at[b, e - 1], {'m1': t})

    def piece1(b, k, s):
        part = w1.at[b, rows_at(s * dim + g * half, half), :]
        return (rcopy(part, part, w1s.at[0], w1r.at[b, k], {'m1': s}), rcopy(part, part, f1s.at[0], f1r.at[b], {'dp': 1 - g}))

    def forward1(b):
        for k, s in peers1:
            arrival, swap = piece1(b, k, s)
            arrival.wait_recv()
            swap.start()

    def swapped1(b):
        part = w1.at[b, 0:3 * half, :]
        return rcopy(part, part, f1s.at[0], f1r.at[b], {'dp': 1 - g})

    def issue1(b):
        for e in (2, 3, 1):
            z1(b, e).start()

    issue1(0)
    issue1(1)

    qh, uh = qw // 2, uw // 2

    def z2(c, e):
        t = ip[e]
        cols, to = ds(c * LANES, LANES), ds(i * LANES, LANES)
        return [rcopy(wd.at[rows_at(t * uw + g * uh, uh), cols], w2.at[c, g, qh:qh + uh, to], w2s.at[0], w2r.at[c, e - 1], {'m1': t}),
                rcopy(wo.at[rows_at(t * qw + g * qh, qh), cols], w2.at[c, g, 0:qh, to], w2s.at[0], w2r.at[c, e - 1], {'m1': t})]

    def issue2(c):
        for e in (2, 3, 1):
            for copy in z2(c, e):
                copy.start()

    def forward2(c):
        for k, s in peers1:
            part = w2.at[c, g, :, ds(s * LANES, LANES)]
            rcopy(part, part, w2s.at[0], w2r.at[c, k], {'m1': s}).wait_recv()
            rcopy(part, part, f2s.at[0], f2r.at[c], {'dp': 1 - g}).start()

    def next2(c):
        forward2(c)

        @pl.when(c + AHEAD < nc)
        def _():
            issue2(c + AHEAD)

    x_own.wait()
    rcopy(xg.at[ip[1]], xg.at[ip[1]], xs.at[1], xr.at[1], {'m1': ip[1]}).wait_recv()
    rcopy(xg.at[ip[3]], xg.at[ip[3]], xs.at[2], xr.at[2], {'m1': ip[1]}).wait_recv()

    def u_out(r, slot):
        return pltpu.make_async_copy(ubl.at[slot], u.at[rows_at(j * rows + r * ln_rows, ln_rows), :], ub_sem.at[slot])

    @pl.loop(0, rows // ln_rows)
    def _(r):
        slot = lax.rem(r, 2)

        @pl.when(r >= 2)
        def _():
            u_out(r - 2, slot).wait()
        at = rows_at(r * ln_rows, ln_rows)
        parts = [xg[s, at, :].astype(jnp.float32) for s in range(4)]
        mean = sum(jnp.sum(part, axis=-1, keepdims=True) for part in parts) / total
        parts = [part - mean for part in parts]
        variance = sum(jnp.sum(part * part, axis=-1, keepdims=True) for part in parts) / total
        inverse = lax.rsqrt(variance + LN_EPS)
        for s in range(4):
            cols = slice(s * dim, (s + 1) * dim)
            ubl[slot, :, cols] = (parts[s] * inverse * lns[:, cols]).astype(jnp.bfloat16)
        u_out(r, slot).start()

    for r in range(max(0, rows // ln_rows - 2), rows // ln_rows):
        u_out(r, r % 2).wait()

    def u_rows(q):
        return u.at[rows_at(q * rows, rows), :]

    u_far = rcopy(u_rows(j), u_rows(j), us.at[0], ur.at[0], {'m2': jp[2]})
    u_near = rcopy(u_rows(j), u_rows(j), us.at[1], ur.at[1], {'m2': jp[1]})
    u_far.start()
    u_near.start()
    for b in range(4):
        forward1(b)
        issue1(b + 2)
    rcopy(u_rows(jp[2]), u_rows(jp[2]), us.at[0], ur.at[0], {'m2': jp[2]}).wait_recv()
    u_fwd = rcopy(u_rows(jp[2]), u_rows(jp[2]), us.at[2], ur.at[2], {'m2': jp[1]})
    u_fwd.start()
    rcopy(u_rows(jp[1]), u_rows(jp[1]), us.at[1], ur.at[1], {'m2': jp[1]}).wait_recv()
    rcopy(u_rows(jp[3]), u_rows(jp[3]), us.at[2], ur.at[2], {'m2': jp[1]}).wait_recv()

    def lhs_in(m, slot):
        return pltpu.make_async_copy(u.at[rows_at(m * block, block), :], lhs.at[slot], lhs_sem.at[slot])

    def product1(b, own, store):
        swapped1(b).wait_recv()
        loads = [pltpu.make_async_copy(own, rhs.at[rows_at(i * dim, dim), :], rhs_sem.at[0])]
        for e in (1, 2, 3):
            at = rows_at(ip[e] * dim, dim)
            loads.append(pltpu.make_async_copy(w1.at[b, at, :], rhs.at[at, :], rhs_sem.at[e]))
        for load in loads:
            load.start()
        lhs_in(0, 0).start()
        for load in loads:
            load.wait()

        @pl.loop(0, tokens // block)
        def _(m):
            slot = lax.rem(m, 2)
            lhs_in(m, slot).wait()

            @pl.when(m + 1 < tokens // block)
            def _():
                lhs_in(m + 1, 1 - slot).start()
            store(rows_at(m * block, block), dot(lhs[slot], rhs[...]))

    @pl.loop(0, 3)
    def _(b):
        def store(at, value):
            zq[b, at, :] = value.astype(jnp.bfloat16)
        product1(b, wq.at[b, :, ds(i * qw, qw)], store)

        @pl.when(b == 1)
        def _():
            forward1(4)
            issue1(6)

    @pl.loop(0, batch)
    def _(n):
        at = rows_at(n * patches, patches)
        for head in range(heads):
            cols = slice(head * LANES, (head + 1) * LANES)
            query = head_norm(zq[0, at, cols].astype(jnp.float32), qns[...])
            key = head_norm(zq[1, at, cols].astype(jnp.float32), kns[...])
            scores = lax.dot_general(query, key, (((1,), (1,)), ((), ())), preferred_element_type=jnp.float32) * LANES ** -0.5
            scores = jnp.exp(scores - jnp.max(scores, axis=-1, keepdims=True))
            probs = (scores / jnp.sum(scores, axis=-1, keepdims=True)).astype(jnp.bfloat16)
            h[at, cols] = dot(probs, zq[2, at, cols]).astype(jnp.bfloat16)

    forward1(5)
    for c in range(AHEAD // 2):
        issue2(c)

    @pl.loop(0, nub)
    def _(b):
        def store(at, value):
            value = value.astype(jnp.bfloat16).astype(jnp.float32) + bu[:, ds(i * uw + b * qw, qw)]
            value = 0.5 * value * (1.0 + lax.erf(value * 2.0 ** -0.5))
            h[at, ds(qw + b * qw, qw)] = value.astype(jnp.bfloat16)
        product1(b + 3, wu.at[:, ds(i * uw + b * qw, qw)], store)

        @pl.when(b == 1)
        def _():
            forward1(6)
            for c in range(AHEAD // 2, AHEAD):
                issue2(c)

        @pl.when(b == 2)
        def _():
            next2(0)

        @pl.when(b == 3)
        def _():
            next2(1)

    def quarter(yy, core):
        return (2 * yy + core) * rows

    def send_a(c, yy):
        return rcopy(pa.at[lax.rem(c, 2), yy], ra.at[c, yy], as_.at[lax.rem(c, 2)], ar.at[c], {'m2': jp[1]})

    def all_a(c):
        return rcopy(pa.at[lax.rem(c, 2)], ra.at[c], as_.at[lax.rem(c, 2)], ar.at[c], {'m2': jp[1]})

    def send_b(c):
        return rcopy(ss.at[lax.rem(c, 2)], rb.at[c], bs.at[lax.rem(c, 2)], br.at[c], {'m2': jp[2]})

    def send_c(c, k):
        src = rb.at[c, :, ds(ip[1 + 2 * k] * LANES, LANES)]
        return rcopy(src, rc.at[c, k], cs.at[0], cr.at[c], {'m1': ip[1]})

    def send_d(c):
        return rcopy(ud.at[c], rd.at[c], dsm.at[0], drm.at[c], {'m1': ip[2]})

    def out_part(c, q):
        return out.at[rows_at(q * rows, rows), ds(c * LANES, LANES)]

    def result(c, q, sem, recv, device):
        part = out_part(c, q)
        return rcopy(part, part, es.at[sem], recv, device)

    def product2(c):
        slot = lax.rem(c, 2)
        cols, to = ds(c * LANES, LANES), ds(i * LANES, LANES)
        loads = [pltpu.make_async_copy(wo.at[rows_at(i * qw, qw), cols], w2b.at[slot, 0:qw, to], w2b_sem.at[0]),
                 pltpu.make_async_copy(wd.at[rows_at(i * uw, uw), cols], w2b.at[slot, qw:qw + uw, to], w2b_sem.at[0])]
        for load in loads:
            load.start()
        part = w2.at[c, 0, :, 0:3 * LANES]
        rcopy(part, part, f2s.at[0], f2r.at[c], {'dp': 1 - g}).wait_recv()
        for e in (1, 2, 3):
            to = ds(ip[e] * LANES, LANES)
            for k in range(2):
                loads.append(pltpu.make_async_copy(w2.at[c, k, 0:qh, to], w2b.at[slot, k * qh:(k + 1) * qh, to], w2b_sem.at[0]))
                loads.append(pltpu.make_async_copy(w2.at[c, k, qh:qh + uh, to], w2b.at[slot, qw + k * uh:qw + (k + 1) * uh, to], w2b_sem.at[0]))
        for load in loads[2:]:
            load.start()

        @pl.when(c >= 2)
        def _():
            all_a(c - 2).wait_send()
        pltpu.make_async_copy(w2b.at[1 - slot], w2b.at[slot], w2b_sem.at[0]).wait()
        for yy in range(2):
            for sub in range(2):
                at = rows_at(quarter(yy, 1 - jc) + sub * block, block)
                pa[slot, yy, sub * block:(sub + 1) * block, :] = dot(h[at, :], w2b[slot]).astype(jnp.bfloat16)
            send_a(c, yy).start()
        keep = lax.rem(c, 3)
        for yy in range(2):
            for sub in range(2):
                at = rows_at(quarter(yy, jc) + sub * block, block)
                po[keep, yy, sub * block:(sub + 1) * block, :] = dot(h[at, :], w2b[slot]).astype(jnp.bfloat16)

    def add(a, b):
        return (a.astype(jnp.float32) + b.astype(jnp.float32)).astype(jnp.bfloat16)

    def sum_core(d):
        keep = lax.rem(d, 3)
        rcopy(ra.at[d], ra.at[d], as_.at[0], ar.at[d], {'m2': jp[1]}).wait_recv()
        load = pltpu.make_async_copy(ra.at[d], rav, rav_sem.at[0])
        load.start()

        @pl.when(d >= 2)
        def _():
            send_b(d - 2).wait_send()
        load.wait()
        ss[lax.rem(d, 2)] = add(po[keep, 1 - jy], rav[1 - jy])
        send_b(d).start()
        po[keep, jy] = add(po[keep, jy], rav[jy])

    def sum_y(d):
        rcopy(rb.at[d], rb.at[d], bs.at[0], br.at[d], {'m2': jp[2]}).wait_recv()
        rb[d] = add(po[lax.rem(d, 3), jy], rb[d])
        for k in range(2):
            send_c(d, k).start()

    def sum_near(d):
        rcopy(rc.at[d], rc.at[d], cs.at[0], cr.at[d], {'m1': ip[1]}).wait_recv()
        ud[d] = add(rb[d, :, ds(ip[2] * LANES, LANES)], rc[d, 1])
        send_d(d).start()

    def finish(d):
        rcopy(rd.at[d], rd.at[d], dsm.at[0], drm.at[d], {'m1': ip[2]}).wait_recv()
        cols = ds(d * LANES, LANES)
        value = rb[d, :, ds(i * LANES, LANES)].astype(jnp.float32) + rc[d, 0].astype(jnp.float32) + rd[d].astype(jnp.float32)
        value = xg[i, :, cols].astype(jnp.float32) + value + bo[cols][None, :]
        out[rows_at(j * rows, rows), cols] = value.astype(jnp.bfloat16)
        result(d, j, 0, er.at[d], {'m2': jp[2]}).start()
        result(d, j, 1, fr.at[0], {'m2': jp[1]}).start()

    def pass_on(d):
        result(d, jp[2], 0, er.at[d], {'m2': jp[2]}).wait_recv()
        result(d, jp[2], 2, fr.at[1], {'m2': jp[1]}).start()

    def run(step, first, last):
        @pl.loop(first, last)
        def _(d):
            step(d)

    early = 2 + 2 * mid

    def late(c, lag, step, last=nc):
        @pl.when((c >= lag) & (c < last))
        def _():
            step(c - lag)

    @pl.loop(0, nc)
    def _(c):
        late(c, 2, sum_y)
        late(c, 1, sum_core)

        @pl.when((c == nc - 2) & (mid == 1))
        def _():
            run(sum_near, 0, early)

        @pl.when((c >= 1) & (c + 1 < nc))
        def _():
            next2(c + 1)

        @pl.when((c == nc - 2) & (mid == 0))
        def _():
            run(sum_near, 0, early)

        @pl.when(c == nc - 1)
        def _():
            run(sum_near, early, early + 2)
            finish(0)
        product2(c)

    sum_core(nc - 1)
    run(sum_near, early + 2, early + 5)
    sum_y(nc - 2)
    run(sum_near, early + 5, nc - 2)
    run(finish, 1, 4)
    sum_y(nc - 1)
    sum_near(nc - 2)
    ready = nc // 2 + 3 * mid
    run(finish, 4, ready)
    sum_near(nc - 1)
    run(finish, ready, nc)
    run(pass_on, 0, nc)

    for copy in (x_far, x_near, x_fwd, u_far, u_near, u_fwd):
      copy.wait_send()
    for sem in (w1s, f1s):
        part = w1.at[:, 0:3 * half, :]
        rcopy(part, part, sem.at[0], w1r.at[0, 0], {'dp': 1 - g}).wait_send()
    for sem in (w2s, f2s):
        part = w2.at[:, 0, :, 0:3 * LANES]
        rcopy(part, part, sem.at[0], f2r.at[0], {'dp': 1 - g}).wait_send()
    for c in (nc - 2, nc - 1):
        all_a(c).wait_send()
        send_b(c).wait_send()
    rcopy(rc, rc, cs.at[0], cr.at[0], {'m1': ip[1]}).wait_send()
    for sem in (dsm.at[0], es.at[0], es.at[1], es.at[2]):
        rcopy(rd, rd, sem, drm.at[0], {'m1': ip[2]}).wait_send()
    for k in range(2):
        rcopy(rd, rd, es.at[1], fr.at[k], {'m2': jp[1]}).wait_recv()


def solution(mesh):
    assert mesh.shape['m1'] == 4 and mesh.shape['m2'] == 4 and mesh.shape['dp'] == 2

    def local_layer(x_blk, ln_scale, qn_scale, kn_scale, w_qkv, w_up, b_up, w_o, w_down, b_out):
        batch, patches, dim = x_blk.shape
        tokens = batch * patches
        qw, uw = w_qkv.shape[2] // 4, w_up.shape[1] // 4
        rows, block, nc, nb = tokens // 4, tokens // 8, dim // LANES, 3 + uw // qw
        assert qn_scale.shape[0] == LANES and uw % qw == 0 and nb == 7
        wide = 4 * LANES
        bf16 = jnp.bfloat16
        dma = pltpu.SemaphoreType.DMA
        hbm = pl.BlockSpec(memory_space=pltpu.HBM)
        vmem = pl.BlockSpec(memory_space=pltpu.VMEM)
        ln_rows = min(64, rows)
        out = pl.pallas_call(
            functools.partial(kernel, (batch, patches, dim, qw, uw)),
            out_shape=[
                pltpu.VMEM((tokens, dim), bf16),
                jax.ShapeDtypeStruct((tokens, 4 * dim), bf16),
                jax.ShapeDtypeStruct((nb, 4 * dim, qw), bf16),
                jax.ShapeDtypeStruct((nc, 2, (qw + uw) // 2, wide), bf16),
                jax.ShapeDtypeStruct((nc, 2, rows, wide), bf16)],
            in_specs=[hbm, vmem, vmem, vmem, hbm, hbm, vmem, hbm, hbm, vmem],
            out_specs=[vmem] + [hbm] * 4,
            scratch_shapes=[
                pltpu.VMEM((4, rows, dim), bf16),
                pltpu.VMEM((2, ln_rows, 4 * dim), bf16),
                pltpu.VMEM((3, tokens, qw), bf16),
                pltpu.VMEM((tokens, qw + uw), bf16),
                pltpu.VMEM((4 * dim, qw), bf16),
                pltpu.VMEM((2, block, 4 * dim), bf16),
                pltpu.VMEM((2, qw + uw, wide), bf16),
                pltpu.VMEM((2, 2, rows, wide), bf16),
                pltpu.VMEM((3, 2, rows, wide), bf16),
                pltpu.VMEM((2, rows, wide), bf16),
                pltpu.VMEM((2, rows, wide), bf16),
                pltpu.VMEM((nc, rows, wide), bf16),
                pltpu.VMEM((nc, 2, rows, LANES), bf16),
                pltpu.VMEM((nc, rows, LANES), bf16),
                pltpu.VMEM((nc, rows, LANES), bf16),
                dma((3,)), dma((3,)),
                dma((1,)), dma((nb, 3)), dma((1,)), dma((nb,)),
                dma((3,)), dma((3,)),
                dma((1,)), dma((nc, 3)), dma((1,)), dma((nc,)),
                dma((2,)), dma((nc,)), dma((2,)), dma((nc,)), dma((1,)), dma((nc,)), dma((1,)), dma((nc,)),
                dma((3,)), dma((nc,)), dma((2,)),
                dma((1,)), dma((4,)), dma((2,)), dma((2,)), dma((1,)), dma((1,))],
            compiler_params=pltpu.CompilerParams(collective_id=0, has_side_effects=True, vmem_limit_bytes=60_000_000),
            name='layer',
        )(x_blk.reshape(tokens, dim), ln_scale[None], qn_scale[None], kn_scale[None], w_qkv.transpose(1, 0, 2), w_up,
          b_up[None], w_o, w_down, b_out)[0]
        return out.reshape(batch, patches, dim)

    return jax.shard_map(local_layer, mesh=mesh, in_specs=(P('dp', None, 'm1'), P(), P(), P(), P('m1', None, 'm2'), P('m1', 'm2'), P('m2'), P('m2', 'm1'), P('m2', 'm1'), P('m1')), out_specs=P('dp', None, 'm1'), check_vma=False)
```

```python
import functools

import jax
import jax.numpy as jnp
from jax import lax
from jax.experimental import pallas as pl
from jax.experimental.pallas import tpu as pltpu
from jax.sharding import PartitionSpec as P

LN_EPS = 1e-6
MESH = pl.DeviceIdType.MESH
LANES = 128
AHEAD = 2


def xors(value):
    return (value, value + 1 - 2 * lax.rem(value, 2), value + 2 - 4 * lax.div(value, 2), 3 - value)


def ds(start, size):
    return pl.ds(pl.multiple_of(start, size if size < LANES else LANES), size)


def rows_at(start, size):
    return pl.ds(pl.multiple_of(start, 8), size)


def rcopy(src, dst, send_sem, recv_sem, device):
    return pltpu.make_async_remote_copy(src_ref=src, dst_ref=dst, send_sem=send_sem, recv_sem=recv_sem, device_id=device, device_id_type=MESH)


def dot(lhs, rhs):
    return jnp.dot(lhs, rhs, preferred_element_type=jnp.float32)


def head_norm(values, scale):
    mean = jnp.mean(values, axis=-1, keepdims=True)
    centered = values - mean
    variance = jnp.mean(centered * centered, axis=-1, keepdims=True)
    return (centered * lax.rsqrt(variance + LN_EPS) * scale).astype(jnp.bfloat16)


def kernel(sizes, x, lns, qns, kns, wq, wu, bu, wo, wd, bo,
           out, u, w1, w2, ra,
           xg, ubl, zq, h, rhs, lhs, w2b, pa, po, rav, ss, rb, rc, ud, rd,
           xs, xr, w1s, w1r, f1s, f1r, us, ur, w2s, w2r, f2s, f2r,
           as_, ar, bs, br, cs, cr, dsm, drm, es, er, fr, own_sem, rhs_sem, lhs_sem, ub_sem, w2b_sem, rav_sem):
    batch, patches, dim, qw, uw = sizes
    tokens = batch * patches
    rows = tokens // 4
    block = rows // 2
    half = dim // 2
    total = 4 * dim
    nub = uw // qw
    nc = dim // LANES
    wide = 4 * LANES
    heads = qw // LANES
    ln_rows = min(64, rows)

    g, i, j = lax.axis_index('dp'), lax.axis_index('m1'), lax.axis_index('m2')
    ip, jp = xors(i), xors(j)
    jy, jc = lax.div(j, 2), lax.rem(j, 2)
    mid = lax.div(lax.rem(i + 1, 4), 2)
    peers1 = ((0, ip[1]), (2 - mid, ip[3] + mid * (ip[2] - ip[3])), (1 + mid, ip[2] + mid * (ip[3] - ip[2])))

    barrier = pltpu.get_barrier_semaphore()
    peers = [{'m1': ip[e]} for e in (1, 2, 3)] + [{'m2': jp[e]} for e in (1, 2, 3)] + [{'dp': 1 - g}]
    for peer in peers:
        pl.semaphore_signal(barrier, inc=1, device_id=peer, device_id_type=MESH)
    pl.semaphore_wait(barrier, len(peers))

    mine = rows_at(j * rows, rows)
    x_far = rcopy(x.at[mine, :], xg.at[i], xs.at[0], xr.at[0], {'m1': ip[2]})
    x_near = rcopy(x.at[mine, :], xg.at[i], xs.at[1], xr.at[1], {'m1': ip[1]})
    x_own = pltpu.make_async_copy(x.at[mine, :], xg.at[i], own_sem.at[0])
    x_far.start()
    x_near.start()
    x_own.start()
    x_far_in = rcopy(xg.at[ip[2]], xg.at[ip[2]], xs.at[0], xr.at[0], {'m1': ip[2]})
    x_far_in.wait_recv()
    x_fwd = rcopy(xg.at[ip[2]], xg.at[ip[2]], xs.at[2], xr.at[2], {'m1': ip[1]})
    x_fwd.start()

    def z1(b, e):
        t = ip[e]
        if b < 3:
            src = wq.at[b, rows_at(g * half, half), ds(t * qw, qw)]
        else:
            src = wu.at[rows_at(g * half, half), ds(t * uw + (b - 3) * qw, qw)]
        return rcopy(src, w1.at[b, rows_at(i * dim + g * half, half), :], w1s.at[0], w1r.at[b, e - 1], {'m1': t})

    def piece1(b, k, s):
        part = w1.at[b, rows_at(s * dim + g * half, half), :]
        return (rcopy(part, part, w1s.at[0], w1r.at[b, k], {'m1': s}), rcopy(part, part, f1s.at[0], f1r.at[b], {'dp': 1 - g}))

    def forward1(b):
        for k, s in peers1:
            arrival, swap = piece1(b, k, s)
            arrival.wait_recv()
            swap.start()

    def swapped1(b):
        part = w1.at[b, 0:3 * half, :]
        return rcopy(part, part, f1s.at[0], f1r.at[b], {'dp': 1 - g})

    def issue1(b):
        for e in (2, 3, 1):
            z1(b, e).start()

    issue1(0)
    issue1(1)

    qh, uh = qw // 2, uw // 2

    def z2(c, e):
        t = ip[e]
        cols, to = ds(c * LANES, LANES), ds(i * LANES, LANES)
        return [rcopy(wd.at[rows_at(t * uw + g * uh, uh), cols], w2.at[c, g, qh:qh + uh, to], w2s.at[0], w2r.at[c, e - 1], {'m1': t}),
                rcopy(wo.at[rows_at(t * qw + g * qh, qh), cols], w2.at[c, g, 0:qh, to], w2s.at[0], w2r.at[c, e - 1], {'m1': t})]

    def issue2(c):
        for e in (2, 3, 1):
            for copy in z2(c, e):
                copy.start()

    def forward2(c):
        for k, s in peers1:
            part = w2.at[c, g, :, ds(s * LANES, LANES)]
            rcopy(part, part, w2s.at[0], w2r.at[c, k], {'m1': s}).wait_recv()
            rcopy(part, part, f2s.at[0], f2r.at[c], {'dp': 1 - g}).start()

    def next2(c):
        forward2(c)

        @pl.when(c + AHEAD < nc)
        def _():
            issue2(c + AHEAD)

    x_own.wait()
    rcopy(xg.at[ip[1]], xg.at[ip[1]], xs.at[1], xr.at[1], {'m1': ip[1]}).wait_recv()
    rcopy(xg.at[ip[3]], xg.at[ip[3]], xs.at[2], xr.at[2], {'m1': ip[1]}).wait_recv()

    def u_out(r, slot):
        return pltpu.make_async_copy(ubl.at[slot], u.at[rows_at(j * rows + r * ln_rows, ln_rows), :], ub_sem.at[slot])

    @pl.loop(0, rows // ln_rows)
    def _(r):
        slot = lax.rem(r, 2)

        @pl.when(r >= 2)
        def _():
            u_out(r - 2, slot).wait()
        at = rows_at(r * ln_rows, ln_rows)
        parts = [xg[s, at, :].astype(jnp.float32) for s in range(4)]
        mean = sum(jnp.sum(part, axis=-1, keepdims=True) for part in parts) / total
        parts = [part - mean for part in parts]
        variance = sum(jnp.sum(part * part, axis=-1, keepdims=True) for part in parts) / total
        inverse = lax.rsqrt(variance + LN_EPS)
        for s in range(4):
            cols = slice(s * dim, (s + 1) * dim)
            ubl[slot, :, cols] = (parts[s] * inverse * lns[:, cols]).astype(jnp.bfloat16)
        u_out(r, slot).start()

    for r in range(max(0, rows // ln_rows - 2), rows // ln_rows):
        u_out(r, r % 2).wait()

    def u_rows(q):
        return u.at[rows_at(q * rows, rows), :]

    u_far = rcopy(u_rows(j), u_rows(j), us.at[0], ur.at[0], {'m2': jp[2]})
    u_near = rcopy(u_rows(j), u_rows(j), us.at[1], ur.at[1], {'m2': jp[1]})
    u_far.start()
    u_near.start()
    for b in range(4):
        forward1(b)
        issue1(b + 2)
    rcopy(u_rows(jp[2]), u_rows(jp[2]), us.at[0], ur.at[0], {'m2': jp[2]}).wait_recv()
    u_fwd = rcopy(u_rows(jp[2]), u_rows(jp[2]), us.at[2], ur.at[2], {'m2': jp[1]})
    u_fwd.start()
    rcopy(u_rows(jp[1]), u_rows(jp[1]), us.at[1], ur.at[1], {'m2': jp[1]}).wait_recv()
    rcopy(u_rows(jp[3]), u_rows(jp[3]), us.at[2], ur.at[2], {'m2': jp[1]}).wait_recv()

    def lhs_in(m, slot):
        return pltpu.make_async_copy(u.at[rows_at(m * block, block), :], lhs.at[slot], lhs_sem.at[slot])

    def product1(b, own, store):
        swapped1(b).wait_recv()
        loads = [pltpu.make_async_copy(own, rhs.at[rows_at(i * dim, dim), :], rhs_sem.at[0])]
        for e in (1, 2, 3):
            at = rows_at(ip[e] * dim, dim)
            loads.append(pltpu.make_async_copy(w1.at[b, at, :], rhs.at[at, :], rhs_sem.at[e]))
        for load in loads:
            load.start()
        lhs_in(0, 0).start()
        for load in loads:
            load.wait()

        @pl.loop(0, tokens // block)
        def _(m):
            slot = lax.rem(m, 2)
            lhs_in(m, slot).wait()

            @pl.when(m + 1 < tokens // block)
            def _():
                lhs_in(m + 1, 1 - slot).start()
            store(rows_at(m * block, block), dot(lhs[slot], rhs[...]))

    @pl.loop(0, 3)
    def _(b):
        def store(at, value):
            zq[b, at, :] = value.astype(jnp.bfloat16)
        product1(b, wq.at[b, :, ds(i * qw, qw)], store)

        @pl.when(b == 1)
        def _():
            forward1(4)
            issue1(6)

    @pl.loop(0, batch)
    def _(n):
        at = rows_at(n * patches, patches)
        for head in range(heads):
            cols = slice(head * LANES, (head + 1) * LANES)
            query = head_norm(zq[0, at, cols].astype(jnp.float32), qns[...])
            key = head_norm(zq[1, at, cols].astype(jnp.float32), kns[...])
            scores = lax.dot_general(query, key, (((1,), (1,)), ((), ())), preferred_element_type=jnp.float32) * LANES ** -0.5
            scores = jnp.exp(scores - jnp.max(scores, axis=-1, keepdims=True))
            probs = (scores / jnp.sum(scores, axis=-1, keepdims=True)).astype(jnp.bfloat16)
            h[at, cols] = dot(probs, zq[2, at, cols]).astype(jnp.bfloat16)

    forward1(5)
    for c in range(AHEAD // 2):
        issue2(c)

    @pl.loop(0, nub)
    def _(b):
        def store(at, value):
            value = value.astype(jnp.bfloat16).astype(jnp.float32) + bu[:, ds(i * uw + b * qw, qw)]
            value = 0.5 * value * (1.0 + lax.erf(value * 2.0 ** -0.5))
            h[at, ds(qw + b * qw, qw)] = value.astype(jnp.bfloat16)
        product1(b + 3, wu.at[:, ds(i * uw + b * qw, qw)], store)

        @pl.when(b == 1)
        def _():
            forward1(6)
            for c in range(AHEAD // 2, AHEAD):
                issue2(c)

        @pl.when(b == 2)
        def _():
            next2(0)

        @pl.when(b == 3)
        def _():
            next2(1)

    def quarter(yy, core):
        return (2 * yy + core) * rows

    def send_a(c, yy):
        return rcopy(pa.at[lax.rem(c, 2), yy], ra.at[c, yy], as_.at[lax.rem(c, 2)], ar.at[c], {'m2': jp[1]})

    def all_a(c):
        return rcopy(pa.at[lax.rem(c, 2)], ra.at[c], as_.at[lax.rem(c, 2)], ar.at[c], {'m2': jp[1]})

    def send_b(c):
        return rcopy(ss.at[lax.rem(c, 2)], rb.at[c], bs.at[lax.rem(c, 2)], br.at[c], {'m2': jp[2]})

    def send_c(c, k):
        src = rb.at[c, :, ds(ip[1 + 2 * k] * LANES, LANES)]
        return rcopy(src, rc.at[c, k], cs.at[0], cr.at[c], {'m1': ip[1]})

    def send_d(c):
        return rcopy(ud.at[c], rd.at[c], dsm.at[0], drm.at[c], {'m1': ip[2]})

    def out_part(c, q):
        return out.at[rows_at(q * rows, rows), ds(c * LANES, LANES)]

    def result(c, q, sem, recv, device):
        part = out_part(c, q)
        return rcopy(part, part, es.at[sem], recv, device)

    def product2(c):
        slot = lax.rem(c, 2)
        cols, to = ds(c * LANES, LANES), ds(i * LANES, LANES)
        loads = [pltpu.make_async_copy(wo.at[rows_at(i * qw, qw), cols], w2b.at[slot, 0:qw, to], w2b_sem.at[0]),
                 pltpu.make_async_copy(wd.at[rows_at(i * uw, uw), cols], w2b.at[slot, qw:qw + uw, to], w2b_sem.at[1])]
        for load in loads:
            load.start()
        part = w2.at[c, 0, :, 0:3 * LANES]
        rcopy(part, part, f2s.at[0], f2r.at[c], {'dp': 1 - g}).wait_recv()
        for e in (1, 2, 3):
            to = ds(ip[e] * LANES, LANES)
            for k in range(2):
                sems = 2 + 4 * (e - 1) + 2 * k
                loads.append(pltpu.make_async_copy(w2.at[c, k, 0:qh, to], w2b.at[slot, k * qh:(k + 1) * qh, to], w2b_sem.at[sems]))
                loads.append(pltpu.make_async_copy(w2.at[c, k, qh:qh + uh, to], w2b.at[slot, qw + k * uh:qw + (k + 1) * uh, to], w2b_sem.at[sems + 1]))
        for load in loads[2:]:
            load.start()

        @pl.when(c >= 2)
        def _():
            all_a(c - 2).wait_send()
        for load in loads:
            load.wait()
        for yy in range(2):
            for sub in range(2):
                at = rows_at(quarter(yy, 1 - jc) + sub * block, block)
                pa[slot, yy, sub * block:(sub + 1) * block, :] = dot(h[at, :], w2b[slot]).astype(jnp.bfloat16)
            send_a(c, yy).start()
        keep = lax.rem(c, 3)
        for yy in range(2):
            for sub in range(2):
                at = rows_at(quarter(yy, jc) + sub * block, block)
                po[keep, yy, sub * block:(sub + 1) * block, :] = dot(h[at, :], w2b[slot]).astype(jnp.bfloat16)

    def add(a, b):
        return (a.astype(jnp.float32) + b.astype(jnp.float32)).astype(jnp.bfloat16)

    def sum_core(d):
        keep = lax.rem(d, 3)
        rcopy(ra.at[d], ra.at[d], as_.at[0], ar.at[d], {'m2': jp[1]}).wait_recv()
        load = pltpu.make_async_copy(ra.at[d], rav, rav_sem.at[0])
        load.start()

        @pl.when(d >= 2)
        def _():
            send_b(d - 2).wait_send()
        load.wait()
        ss[lax.rem(d, 2)] = add(po[keep, 1 - jy], rav[1 - jy])
        send_b(d).start()
        po[keep, jy] = add(po[keep, jy], rav[jy])

    def sum_y(d):
        rcopy(rb.at[d], rb.at[d], bs.at[0], br.at[d], {'m2': jp[2]}).wait_recv()
        rb[d] = add(po[lax.rem(d, 3), jy], rb[d])
        for k in range(2):
            send_c(d, k).start()

    def sum_near(d):
        rcopy(rc.at[d], rc.at[d], cs.at[0], cr.at[d], {'m1': ip[1]}).wait_recv()
        ud[d] = add(rb[d, :, ds(ip[2] * LANES, LANES)], rc[d, 1])
        send_d(d).start()

    def finish(d):
        rcopy(rd.at[d], rd.at[d], dsm.at[0], drm.at[d], {'m1': ip[2]}).wait_recv()
        cols = ds(d * LANES, LANES)
        value = rb[d, :, ds(i * LANES, LANES)].astype(jnp.float32) + rc[d, 0].astype(jnp.float32) + rd[d].astype(jnp.float32)
        value = xg[i, :, cols].astype(jnp.float32) + value + bo[cols][None, :]
        out[rows_at(j * rows, rows), cols] = value.astype(jnp.bfloat16)
        result(d, j, 0, er.at[d], {'m2': jp[2]}).start()
        result(d, j, 1, fr.at[0], {'m2': jp[1]}).start()

    def pass_on(d):
        result(d, jp[2], 0, er.at[d], {'m2': jp[2]}).wait_recv()
        result(d, jp[2], 2, fr.at[1], {'m2': jp[1]}).start()

    def run(step, first, last):
        @pl.loop(first, last)
        def _(d):
            step(d)

    early = 1 + 3 * mid

    def late(c, lag, step, last=nc):
        @pl.when((c >= lag) & (c < last))
        def _():
            step(c - lag)

    @pl.loop(0, nc)
    def _(c):
        late(c, 2, sum_y)
        late(c, 1, sum_core)

        @pl.when((c >= 1) & (c + 1 < nc))
        def _():
            next2(c + 1)

        @pl.when(c == nc - 2)
        def _():
            run(sum_near, 0, early)

        @pl.when(c == nc - 1)
        def _():
            run(sum_near, early, early + 2)
            finish(0)
        product2(c)

    sum_core(nc - 1)
    run(sum_near, early + 2, early + 5)
    sum_y(nc - 2)
    run(sum_near, early + 5, nc - 2)
    run(finish, 1, 4)
    sum_y(nc - 1)
    sum_near(nc - 2)
    run(finish, 4, nc - 3)
    sum_near(nc - 1)
    run(finish, nc - 3, nc)
    run(pass_on, 0, nc)

    for copy in (x_far, x_near, x_fwd, u_far, u_near, u_fwd):
      copy.wait_send()
    for sem in (w1s, f1s):
        part = w1.at[:, 0:3 * half, :]
        rcopy(part, part, sem.at[0], w1r.at[0, 0], {'dp': 1 - g}).wait_send()
    for sem in (w2s, f2s):
        part = w2.at[:, 0, :, 0:3 * LANES]
        rcopy(part, part, sem.at[0], f2r.at[0], {'dp': 1 - g}).wait_send()
    for c in (nc - 2, nc - 1):
        all_a(c).wait_send()
        send_b(c).wait_send()
    rcopy(rc, rc, cs.at[0], cr.at[0], {'m1': ip[1]}).wait_send()
    for sem in (dsm.at[0], es.at[0], es.at[1], es.at[2]):
        rcopy(rd, rd, sem, drm.at[0], {'m1': ip[2]}).wait_send()
    for k in range(2):
        rcopy(rd, rd, es.at[1], fr.at[k], {'m2': jp[1]}).wait_recv()


def solution(mesh):
    assert mesh.shape['m1'] == 4 and mesh.shape['m2'] == 4 and mesh.shape['dp'] == 2

    def local_layer(x_blk, ln_scale, qn_scale, kn_scale, w_qkv, w_up, b_up, w_o, w_down, b_out):
        batch, patches, dim = x_blk.shape
        tokens = batch * patches
        qw, uw = w_qkv.shape[2] // 4, w_up.shape[1] // 4
        rows, block, nc, nb = tokens // 4, tokens // 8, dim // LANES, 3 + uw // qw
        assert qn_scale.shape[0] == LANES and uw % qw == 0 and nb == 7
        wide = 4 * LANES
        bf16 = jnp.bfloat16
        dma = pltpu.SemaphoreType.DMA
        hbm = pl.BlockSpec(memory_space=pltpu.HBM)
        vmem = pl.BlockSpec(memory_space=pltpu.VMEM)
        ln_rows = min(64, rows)
        out = pl.pallas_call(
            functools.partial(kernel, (batch, patches, dim, qw, uw)),
            out_shape=[
                pltpu.VMEM((tokens, dim), bf16),
                jax.ShapeDtypeStruct((tokens, 4 * dim), bf16),
                jax.ShapeDtypeStruct((nb, 4 * dim, qw), bf16),
                jax.ShapeDtypeStruct((nc, 2, (qw + uw) // 2, wide), bf16),
                jax.ShapeDtypeStruct((nc, 2, rows, wide), bf16)],
            in_specs=[hbm, vmem, vmem, vmem, hbm, hbm, vmem, hbm, hbm, vmem],
            out_specs=[vmem] + [hbm] * 4,
            scratch_shapes=[
                pltpu.VMEM((4, rows, dim), bf16),
                pltpu.VMEM((2, ln_rows, 4 * dim), bf16),
                pltpu.VMEM((3, tokens, qw), bf16),
                pltpu.VMEM((tokens, qw + uw), bf16),
                pltpu.VMEM((4 * dim, qw), bf16),
                pltpu.VMEM((2, block, 4 * dim), bf16),
                pltpu.VMEM((2, qw + uw, wide), bf16),
                pltpu.VMEM((2, 2, rows, wide), bf16),
                pltpu.VMEM((3, 2, rows, wide), bf16),
                pltpu.VMEM((2, rows, wide), bf16),
                pltpu.VMEM((2, rows, wide), bf16),
                pltpu.VMEM((nc, rows, wide), bf16),
                pltpu.VMEM((nc, 2, rows, LANES), bf16),
                pltpu.VMEM((nc, rows, LANES), bf16),
                pltpu.VMEM((nc, rows, LANES), bf16),
                dma((3,)), dma((3,)),
                dma((1,)), dma((nb, 3)), dma((1,)), dma((nb,)),
                dma((3,)), dma((3,)),
                dma((1,)), dma((nc, 3)), dma((1,)), dma((nc,)),
                dma((2,)), dma((nc,)), dma((2,)), dma((nc,)), dma((1,)), dma((nc,)), dma((1,)), dma((nc,)),
                dma((3,)), dma((nc,)), dma((2,)),
                dma((1,)), dma((4,)), dma((2,)), dma((2,)), dma((14,)), dma((1,))],
            compiler_params=pltpu.CompilerParams(collective_id=0, has_side_effects=True, vmem_limit_bytes=60_000_000),
            name='layer',
        )(x_blk.reshape(tokens, dim), ln_scale[None], qn_scale[None], kn_scale[None], w_qkv.transpose(1, 0, 2), w_up,
          b_up[None], w_o, w_down, b_out)[0]
        return out.reshape(batch, patches, dim)

    return jax.shard_map(local_layer, mesh=mesh, in_specs=(P('dp', None, 'm1'), P(), P(), P(), P('m1', None, 'm2'), P('m1', 'm2'), P('m2'), P('m2', 'm1'), P('m2', 'm1'), P('m1')), out_specs=P('dp', None, 'm1'), check_vma=False)
```

```python
import functools

import jax
import jax.numpy as jnp
from jax import lax
from jax.experimental import pallas as pl
from jax.experimental.pallas import tpu as pltpu
from jax.sharding import PartitionSpec as P

LN_EPS = 1e-6
MESH = pl.DeviceIdType.MESH
LANES = 128
AHEAD = 2


def xors(value):
    return (value, value + 1 - 2 * lax.rem(value, 2), value + 2 - 4 * lax.div(value, 2), 3 - value)


def ds(start, size):
    return pl.ds(pl.multiple_of(start, size if size < LANES else LANES), size)


def rows_at(start, size):
    return pl.ds(pl.multiple_of(start, 8), size)


def rcopy(src, dst, send_sem, recv_sem, device):
    return pltpu.make_async_remote_copy(src_ref=src, dst_ref=dst, send_sem=send_sem, recv_sem=recv_sem, device_id=device, device_id_type=MESH)


def dot(lhs, rhs):
    return jnp.dot(lhs, rhs, preferred_element_type=jnp.float32)


def head_norm(values, scale):
    mean = jnp.mean(values, axis=-1, keepdims=True)
    centered = values - mean
    variance = jnp.mean(centered * centered, axis=-1, keepdims=True)
    return (centered * lax.rsqrt(variance + LN_EPS) * scale).astype(jnp.bfloat16)


def kernel(sizes, x, lns, qns, kns, wq, wu, bu, wo, wd, bo,
           out, u, w1, w2, ra,
           xg, ubl, zq, h, rhs, lhs, w2b, pa, po, rav, ss, rb, rc, ud, rd,
           xs, xr, w1s, w1r, f1s, f1r, us, ur, w2s, w2r, f2s, f2r,
           as_, ar, bs, br, cs, cr, dsm, drm, es, er, fr, own_sem, rhs_sem, lhs_sem, ub_sem, w2b_sem, rav_sem):
    batch, patches, dim, qw, uw = sizes
    tokens = batch * patches
    rows = tokens // 4
    block = rows // 2
    half = dim // 2
    total = 4 * dim
    nub = uw // qw
    nc = dim // LANES
    wide = 4 * LANES
    heads = qw // LANES
    ln_rows = min(64, rows)

    g, i, j = lax.axis_index('dp'), lax.axis_index('m1'), lax.axis_index('m2')
    ip, jp = xors(i), xors(j)
    jy, jc = lax.div(j, 2), lax.rem(j, 2)
    mid = lax.div(lax.rem(i + 1, 4), 2)
    peers1 = ((0, ip[1]), (2 - mid, ip[3] + mid * (ip[2] - ip[3])), (1 + mid, ip[2] + mid * (ip[3] - ip[2])))

    barrier = pltpu.get_barrier_semaphore()
    peers = [{'m1': ip[e]} for e in (1, 2, 3)] + [{'m2': jp[e]} for e in (1, 2, 3)] + [{'dp': 1 - g}]
    for peer in peers:
        pl.semaphore_signal(barrier, inc=1, device_id=peer, device_id_type=MESH)
    pl.semaphore_wait(barrier, len(peers))

    mine = rows_at(j * rows, rows)
    x_far = rcopy(x.at[mine, :], xg.at[i], xs.at[0], xr.at[0], {'m1': ip[2]})
    x_near = rcopy(x.at[mine, :], xg.at[i], xs.at[1], xr.at[1], {'m1': ip[1]})
    x_own = pltpu.make_async_copy(x.at[mine, :], xg.at[i], own_sem.at[0])
    x_far.start()
    x_near.start()
    x_own.start()
    x_far_in = rcopy(xg.at[ip[2]], xg.at[ip[2]], xs.at[0], xr.at[0], {'m1': ip[2]})
    x_far_in.wait_recv()
    x_fwd = rcopy(xg.at[ip[2]], xg.at[ip[2]], xs.at[2], xr.at[2], {'m1': ip[1]})
    x_fwd.start()

    def z1(b, e):
        t = ip[e]
        if b < 3:
            src = wq.at[b, rows_at(g * half, half), ds(t * qw, qw)]
        else:
            src = wu.at[rows_at(g * half, half), ds(t * uw + (b - 3) * qw, qw)]
        return rcopy(src, w1.at[b, rows_at(i * dim + g * half, half), :], w1s.at[0], w1r.at[b, e - 1], {'m1': t})

    def piece1(b, k, s):
        part = w1.at[b, rows_at(s * dim + g * half, half), :]
        return (rcopy(part, part, w1s.at[0], w1r.at[b, k], {'m1': s}), rcopy(part, part, f1s.at[0], f1r.at[b], {'dp': 1 - g}))

    def forward1(b):
        for k, s in peers1:
            arrival, swap = piece1(b, k, s)
            arrival.wait_recv()
            swap.start()

    def swapped1(b):
        part = w1.at[b, 0:3 * half, :]
        return rcopy(part, part, f1s.at[0], f1r.at[b], {'dp': 1 - g})

    def issue1(b):
        for e in (2, 3, 1):
            z1(b, e).start()

    issue1(0)
    issue1(1)

    qh, uh = qw // 2, uw // 2

    def z2(c, e):
        t = ip[e]
        cols, to = ds(c * LANES, LANES), ds(i * LANES, LANES)
        return [rcopy(wd.at[rows_at(t * uw + g * uh, uh), cols], w2.at[c, g, qh:qh + uh, to], w2s.at[0], w2r.at[c, e - 1], {'m1': t}),
                rcopy(wo.at[rows_at(t * qw + g * qh, qh), cols], w2.at[c, g, 0:qh, to], w2s.at[0], w2r.at[c, e - 1], {'m1': t})]

    def issue2(c):
        for e in (2, 3, 1):
            for copy in z2(c, e):
                copy.start()

    def forward2(c):
        for k, s in peers1:
            part = w2.at[c, g, :, ds(s * LANES, LANES)]
            rcopy(part, part, w2s.at[0], w2r.at[c, k], {'m1': s}).wait_recv()
            rcopy(part, part, f2s.at[0], f2r.at[c], {'dp': 1 - g}).start()

    def next2(c):
        forward2(c)

        @pl.when(c + AHEAD < nc)
        def _():
            issue2(c + AHEAD)

    x_own.wait()
    rcopy(xg.at[ip[1]], xg.at[ip[1]], xs.at[1], xr.at[1], {'m1': ip[1]}).wait_recv()
    rcopy(xg.at[ip[3]], xg.at[ip[3]], xs.at[2], xr.at[2], {'m1': ip[1]}).wait_recv()

    def u_out(r, slot):
        return pltpu.make_async_copy(ubl.at[slot], u.at[rows_at(j * rows + r * ln_rows, ln_rows), :], ub_sem.at[slot])

    @pl.loop(0, rows // ln_rows)
    def _(r):
        slot = lax.rem(r, 2)

        @pl.when(r >= 2)
        def _():
            u_out(r - 2, slot).wait()
        at = rows_at(r * ln_rows, ln_rows)
        parts = [xg[s, at, :].astype(jnp.float32) for s in range(4)]
        mean = sum(jnp.sum(part, axis=-1, keepdims=True) for part in parts) / total
        parts = [part - mean for part in parts]
        variance = sum(jnp.sum(part * part, axis=-1, keepdims=True) for part in parts) / total
        inverse = lax.rsqrt(variance + LN_EPS)
        for s in range(4):
            cols = slice(s * dim, (s + 1) * dim)
            ubl[slot, :, cols] = (parts[s] * inverse * lns[:, cols]).astype(jnp.bfloat16)
        u_out(r, slot).start()

    for r in range(max(0, rows // ln_rows - 2), rows // ln_rows):
        u_out(r, r % 2).wait()

    def u_rows(q):
        return u.at[rows_at(q * rows, rows), :]

    u_far = rcopy(u_rows(j), u_rows(j), us.at[0], ur.at[0], {'m2': jp[2]})
    u_near = rcopy(u_rows(j), u_rows(j), us.at[1], ur.at[1], {'m2': jp[1]})
    u_far.start()
    u_near.start()
    for b in range(4):
        forward1(b)
        issue1(b + 2)
    rcopy(u_rows(jp[2]), u_rows(jp[2]), us.at[0], ur.at[0], {'m2': jp[2]}).wait_recv()
    u_fwd = rcopy(u_rows(jp[2]), u_rows(jp[2]), us.at[2], ur.at[2], {'m2': jp[1]})
    u_fwd.start()
    rcopy(u_rows(jp[1]), u_rows(jp[1]), us.at[1], ur.at[1], {'m2': jp[1]}).wait_recv()
    rcopy(u_rows(jp[3]), u_rows(jp[3]), us.at[2], ur.at[2], {'m2': jp[1]}).wait_recv()

    def lhs_in(m, slot):
        return pltpu.make_async_copy(u.at[rows_at(m * block, block), :], lhs.at[slot], lhs_sem.at[slot])

    def product1(b, own, store):
        swapped1(b).wait_recv()
        loads = [pltpu.make_async_copy(own, rhs.at[rows_at(i * dim, dim), :], rhs_sem.at[0])]
        for e in (1, 2, 3):
            at = rows_at(ip[e] * dim, dim)
            loads.append(pltpu.make_async_copy(w1.at[b, at, :], rhs.at[at, :], rhs_sem.at[e]))
        for load in loads:
            load.start()
        lhs_in(0, 0).start()
        for load in loads:
            load.wait()

        @pl.loop(0, tokens // block)
        def _(m):
            slot = lax.rem(m, 2)
            lhs_in(m, slot).wait()

            @pl.when(m + 1 < tokens // block)
            def _():
                lhs_in(m + 1, 1 - slot).start()
            store(rows_at(m * block, block), dot(lhs[slot], rhs[...]))

    @pl.loop(0, 3)
    def _(b):
        def store(at, value):
            zq[b, at, :] = value.astype(jnp.bfloat16)
        product1(b, wq.at[b, :, ds(i * qw, qw)], store)

        @pl.when(b == 1)
        def _():
            forward1(4)
            issue1(6)

    @pl.loop(0, batch)
    def _(n):
        at = rows_at(n * patches, patches)
        for head in range(heads):
            cols = slice(head * LANES, (head + 1) * LANES)
            query = head_norm(zq[0, at, cols].astype(jnp.float32), qns[...])
            key = head_norm(zq[1, at, cols].astype(jnp.float32), kns[...])
            scores = lax.dot_general(query, key, (((1,), (1,)), ((), ())), preferred_element_type=jnp.float32) * LANES ** -0.5
            scores = jnp.exp(scores - jnp.max(scores, axis=-1, keepdims=True))
            probs = (scores / jnp.sum(scores, axis=-1, keepdims=True)).astype(jnp.bfloat16)
            h[at, cols] = dot(probs, zq[2, at, cols]).astype(jnp.bfloat16)

    forward1(5)
    for c in range(AHEAD // 2):
        issue2(c)

    @pl.loop(0, nub)
    def _(b):
        def store(at, value):
            value = value.astype(jnp.bfloat16).astype(jnp.float32) + bu[:, ds(i * uw + b * qw, qw)]
            value = 0.5 * value * (1.0 + lax.erf(value * 2.0 ** -0.5))
            h[at, ds(qw + b * qw, qw)] = value.astype(jnp.bfloat16)
        product1(b + 3, wu.at[:, ds(i * uw + b * qw, qw)], store)

        @pl.when(b == 1)
        def _():
            forward1(6)
            for c in range(AHEAD // 2, AHEAD):
                issue2(c)

        @pl.when(b == 2)
        def _():
            next2(0)

        @pl.when(b == 3)
        def _():
            next2(1)

    def quarter(yy, core):
        return (2 * yy + core) * rows

    def send_a(c, yy):
        return rcopy(pa.at[lax.rem(c, 2), yy], ra.at[c, yy], as_.at[lax.rem(c, 2)], ar.at[c], {'m2': jp[1]})

    def all_a(c):
        return rcopy(pa.at[lax.rem(c, 2)], ra.at[c], as_.at[lax.rem(c, 2)], ar.at[c], {'m2': jp[1]})

    def send_b(c):
        return rcopy(ss.at[lax.rem(c, 2)], rb.at[c], bs.at[lax.rem(c, 2)], br.at[c], {'m2': jp[2]})

    def send_c(c, k):
        src = rb.at[c, :, ds(ip[1 + 2 * k] * LANES, LANES)]
        return rcopy(src, rc.at[c, k], cs.at[0], cr.at[c], {'m1': ip[1]})

    def send_d(c):
        return rcopy(ud.at[c], rd.at[c], dsm.at[0], drm.at[c], {'m1': ip[2]})

    def out_part(c, q):
        return out.at[rows_at(q * rows, rows), ds(c * LANES, LANES)]

    def result(c, q, sem, recv, device):
        part = out_part(c, q)
        return rcopy(part, part, es.at[sem], recv, device)

    def product2(c):
        slot = lax.rem(c, 2)
        cols, to = ds(c * LANES, LANES), ds(i * LANES, LANES)
        loads = [pltpu.make_async_copy(wo.at[rows_at(i * qw, qw), cols], w2b.at[slot, 0:qw, to], w2b_sem.at[0]),
                 pltpu.make_async_copy(wd.at[rows_at(i * uw, uw), cols], w2b.at[slot, qw:qw + uw, to], w2b_sem.at[1])]
        for load in loads:
            load.start()
        part = w2.at[c, 0, :, 0:3 * LANES]
        rcopy(part, part, f2s.at[0], f2r.at[c], {'dp': 1 - g}).wait_recv()
        for e in (1, 2, 3):
            to = ds(ip[e] * LANES, LANES)
            for k in range(2):
                sems = 2 + 4 * (e - 1) + 2 * k
                loads.append(pltpu.make_async_copy(w2.at[c, k, 0:qh, to], w2b.at[slot, k * qh:(k + 1) * qh, to], w2b_sem.at[sems]))
                loads.append(pltpu.make_async_copy(w2.at[c, k, qh:qh + uh, to], w2b.at[slot, qw + k * uh:qw + (k + 1) * uh, to], w2b_sem.at[sems + 1]))
        for load in loads[2:]:
            load.start()

        @pl.when(c >= 2)
        def _():
            all_a(c - 2).wait_send()
        for load in loads:
            load.wait()
        for yy in range(2):
            for sub in range(2):
                at = rows_at(quarter(yy, 1 - jc) + sub * block, block)
                pa[slot, yy, sub * block:(sub + 1) * block, :] = dot(h[at, :], w2b[slot]).astype(jnp.bfloat16)
            send_a(c, yy).start()
        keep = lax.rem(c, 3)
        for yy in range(2):
            for sub in range(2):
                at = rows_at(quarter(yy, jc) + sub * block, block)
                po[keep, yy, sub * block:(sub + 1) * block, :] = dot(h[at, :], w2b[slot]).astype(jnp.bfloat16)

    def add(a, b):
        return (a.astype(jnp.float32) + b.astype(jnp.float32)).astype(jnp.bfloat16)

    def sum_core(d):
        keep = lax.rem(d, 3)
        rcopy(ra.at[d], ra.at[d], as_.at[0], ar.at[d], {'m2': jp[1]}).wait_recv()
        load = pltpu.make_async_copy(ra.at[d], rav, rav_sem.at[0])
        load.start()

        @pl.when(d >= 2)
        def _():
            send_b(d - 2).wait_send()
        load.wait()
        ss[lax.rem(d, 2)] = add(po[keep, 1 - jy], rav[1 - jy])
        send_b(d).start()
        po[keep, jy] = add(po[keep, jy], rav[jy])

    def sum_y(d):
        rcopy(rb.at[d], rb.at[d], bs.at[0], br.at[d], {'m2': jp[2]}).wait_recv()
        rb[d] = add(po[lax.rem(d, 3), jy], rb[d])
        for k in range(2):
            send_c(d, k).start()

    def sum_near(d):
        rcopy(rc.at[d], rc.at[d], cs.at[0], cr.at[d], {'m1': ip[1]}).wait_recv()
        ud[d] = add(rb[d, :, ds(ip[2] * LANES, LANES)], rc[d, 1])
        send_d(d).start()

    def finish(d):
        rcopy(rd.at[d], rd.at[d], dsm.at[0], drm.at[d], {'m1': ip[2]}).wait_recv()
        cols = ds(d * LANES, LANES)
        value = rb[d, :, ds(i * LANES, LANES)].astype(jnp.float32) + rc[d, 0].astype(jnp.float32) + rd[d].astype(jnp.float32)
        value = xg[i, :, cols].astype(jnp.float32) + value + bo[cols][None, :]
        out[rows_at(j * rows, rows), cols] = value.astype(jnp.bfloat16)
        result(d, j, 0, er.at[d], {'m2': jp[2]}).start()
        result(d, j, 1, fr.at[0], {'m2': jp[1]}).start()

    def pass_on(d):
        result(d, jp[2], 0, er.at[d], {'m2': jp[2]}).wait_recv()
        result(d, jp[2], 2, fr.at[1], {'m2': jp[1]}).start()

    def run(step, first, last):
        @pl.loop(first, last)
        def _(d):
            step(d)

    early = 2 + mid

    def late(c, lag, step, last=nc):
        @pl.when((c >= lag) & (c < last))
        def _():
            step(c - lag)

    @pl.loop(0, nc)
    def _(c):
        late(c, 2, sum_y)
        late(c, 1, sum_core)

        @pl.when((c >= 1) & (c + 1 < nc))
        def _():
            next2(c + 1)

        @pl.when(c == nc - 2)
        def _():
            run(sum_near, 0, early)

        @pl.when(c == nc - 1)
        def _():
            run(sum_near, early, early + 2)
            finish(0)
        product2(c)

    sum_core(nc - 1)
    run(sum_near, early + 2, early + 5)
    sum_y(nc - 2)
    run(sum_near, early + 5, nc - 2)
    run(finish, 1, 4)
    sum_y(nc - 1)
    sum_near(nc - 2)
    run(finish, 4, nc - 3)
    sum_near(nc - 1)
    run(finish, nc - 3, nc)
    run(pass_on, 0, nc)

    for copy in (x_far, x_near, x_fwd, u_far, u_near, u_fwd):
      copy.wait_send()
    for sem in (w1s, f1s):
        part = w1.at[:, 0:3 * half, :]
        rcopy(part, part, sem.at[0], w1r.at[0, 0], {'dp': 1 - g}).wait_send()
    for sem in (w2s, f2s):
        part = w2.at[:, 0, :, 0:3 * LANES]
        rcopy(part, part, sem.at[0], f2r.at[0], {'dp': 1 - g}).wait_send()
    for c in (nc - 2, nc - 1):
        all_a(c).wait_send()
        send_b(c).wait_send()
    rcopy(rc, rc, cs.at[0], cr.at[0], {'m1': ip[1]}).wait_send()
    for sem in (dsm.at[0], es.at[0], es.at[1], es.at[2]):
        rcopy(rd, rd, sem, drm.at[0], {'m1': ip[2]}).wait_send()
    for k in range(2):
        rcopy(rd, rd, es.at[1], fr.at[k], {'m2': jp[1]}).wait_recv()


def solution(mesh):
    assert mesh.shape['m1'] == 4 and mesh.shape['m2'] == 4 and mesh.shape['dp'] == 2

    def local_layer(x_blk, ln_scale, qn_scale, kn_scale, w_qkv, w_up, b_up, w_o, w_down, b_out):
        batch, patches, dim = x_blk.shape
        tokens = batch * patches
        qw, uw = w_qkv.shape[2] // 4, w_up.shape[1] // 4
        rows, block, nc, nb = tokens // 4, tokens // 8, dim // LANES, 3 + uw // qw
        assert qn_scale.shape[0] == LANES and uw % qw == 0 and nb == 7
        wide = 4 * LANES
        bf16 = jnp.bfloat16
        dma = pltpu.SemaphoreType.DMA
        hbm = pl.BlockSpec(memory_space=pltpu.HBM)
        vmem = pl.BlockSpec(memory_space=pltpu.VMEM)
        ln_rows = min(64, rows)
        out = pl.pallas_call(
            functools.partial(kernel, (batch, patches, dim, qw, uw)),
            out_shape=[
                pltpu.VMEM((tokens, dim), bf16),
                jax.ShapeDtypeStruct((tokens, 4 * dim), bf16),
                jax.ShapeDtypeStruct((nb, 4 * dim, qw), bf16),
                jax.ShapeDtypeStruct((nc, 2, (qw + uw) // 2, wide), bf16),
                jax.ShapeDtypeStruct((nc, 2, rows, wide), bf16)],
            in_specs=[hbm, vmem, vmem, vmem, hbm, hbm, vmem, hbm, hbm, vmem],
            out_specs=[vmem] + [hbm] * 4,
            scratch_shapes=[
                pltpu.VMEM((4, rows, dim), bf16),
                pltpu.VMEM((2, ln_rows, 4 * dim), bf16),
                pltpu.VMEM((3, tokens, qw), bf16),
                pltpu.VMEM((tokens, qw + uw), bf16),
                pltpu.VMEM((4 * dim, qw), bf16),
                pltpu.VMEM((2, block, 4 * dim), bf16),
                pltpu.VMEM((2, qw + uw, wide), bf16),
                pltpu.VMEM((2, 2, rows, wide), bf16),
                pltpu.VMEM((3, 2, rows, wide), bf16),
                pltpu.VMEM((2, rows, wide), bf16),
                pltpu.VMEM((2, rows, wide), bf16),
                pltpu.VMEM((nc, rows, wide), bf16),
                pltpu.VMEM((nc, 2, rows, LANES), bf16),
                pltpu.VMEM((nc, rows, LANES), bf16),
                pltpu.VMEM((nc, rows, LANES), bf16),
                dma((3,)), dma((3,)),
                dma((1,)), dma((nb, 3)), dma((1,)), dma((nb,)),
                dma((3,)), dma((3,)),
                dma((1,)), dma((nc, 3)), dma((1,)), dma((nc,)),
                dma((2,)), dma((nc,)), dma((2,)), dma((nc,)), dma((1,)), dma((nc,)), dma((1,)), dma((nc,)),
                dma((3,)), dma((nc,)), dma((2,)),
                dma((1,)), dma((4,)), dma((2,)), dma((2,)), dma((14,)), dma((1,))],
            compiler_params=pltpu.CompilerParams(collective_id=0, has_side_effects=True, vmem_limit_bytes=60_000_000),
            name='layer',
        )(x_blk.reshape(tokens, dim), ln_scale[None], qn_scale[None], kn_scale[None], w_qkv.transpose(1, 0, 2), w_up,
          b_up[None], w_o, w_down, b_out)[0]
        return out.reshape(batch, patches, dim)

    return jax.shard_map(local_layer, mesh=mesh, in_specs=(P('dp', None, 'm1'), P(), P(), P(), P('m1', None, 'm2'), P('m1', 'm2'), P('m2'), P('m2', 'm1'), P('m2', 'm1'), P('m1')), out_specs=P('dp', None, 'm1'), check_vma=False)
```

```python
import functools

import jax
import jax.numpy as jnp
from jax import lax
from jax.experimental import pallas as pl
from jax.experimental.pallas import tpu as pltpu
from jax.sharding import PartitionSpec as P

LN_EPS = 1e-6
MESH = pl.DeviceIdType.MESH
LANES = 128
AHEAD = 3


def xors(value):
    return (value, value + 1 - 2 * lax.rem(value, 2), value + 2 - 4 * lax.div(value, 2), 3 - value)


def ds(start, size):
    return pl.ds(pl.multiple_of(start, size if size < LANES else LANES), size)


def rows_at(start, size):
    return pl.ds(pl.multiple_of(start, 8), size)


def rcopy(src, dst, send_sem, recv_sem, device):
    return pltpu.make_async_remote_copy(src_ref=src, dst_ref=dst, send_sem=send_sem, recv_sem=recv_sem, device_id=device, device_id_type=MESH)


def dot(lhs, rhs):
    return jnp.dot(lhs, rhs, preferred_element_type=jnp.float32)


def head_norm(values, scale):
    mean = jnp.mean(values, axis=-1, keepdims=True)
    centered = values - mean
    variance = jnp.mean(centered * centered, axis=-1, keepdims=True)
    return (centered * lax.rsqrt(variance + LN_EPS) * scale).astype(jnp.bfloat16)


def kernel(sizes, x, lns, qns, kns, wq, wu, bu, wo, wd, bo,
           out, u, w1, w2, ra,
           xg, ubl, zq, h, rhs, lhs, w2b, pa, po, rav, ss, rb, rc, ud, rd,
           xs, xr, w1s, w1r, f1s, f1r, us, ur, w2s, w2r, f2s, f2r,
           as_, ar, bs, br, cs, cr, dsm, drm, es, er, fr, own_sem, rhs_sem, lhs_sem, ub_sem, w2b_sem, rav_sem):
    batch, patches, dim, qw, uw = sizes
    tokens = batch * patches
    rows = tokens // 4
    block = rows // 2
    half = dim // 2
    total = 4 * dim
    nub = uw // qw
    nc = dim // LANES
    wide = 4 * LANES
    heads = qw // LANES
    ln_rows = min(64, rows)

    g, i, j = lax.axis_index('dp'), lax.axis_index('m1'), lax.axis_index('m2')
    ip, jp = xors(i), xors(j)
    jy, jc = lax.div(j, 2), lax.rem(j, 2)
    mid = lax.div(lax.rem(i + 1, 4), 2)
    peers1 = ((0, ip[1]), (2 - mid, ip[3] + mid * (ip[2] - ip[3])), (1 + mid, ip[2] + mid * (ip[3] - ip[2])))

    barrier = pltpu.get_barrier_semaphore()
    peers = [{'m1': ip[e]} for e in (1, 2, 3)] + [{'m2': jp[e]} for e in (1, 2, 3)] + [{'dp': 1 - g}]
    for peer in peers:
        pl.semaphore_signal(barrier, inc=1, device_id=peer, device_id_type=MESH)
    pl.semaphore_wait(barrier, len(peers))

    mine = rows_at(j * rows, rows)
    x_far = rcopy(x.at[mine, :], xg.at[i], xs.at[0], xr.at[0], {'m1': ip[2]})
    x_near = rcopy(x.at[mine, :], xg.at[i], xs.at[1], xr.at[1], {'m1': ip[1]})
    x_own = pltpu.make_async_copy(x.at[mine, :], xg.at[i], own_sem.at[0])
    x_far.start()
    x_near.start()
    x_own.start()
    x_far_in = rcopy(xg.at[ip[2]], xg.at[ip[2]], xs.at[0], xr.at[0], {'m1': ip[2]})
    x_far_in.wait_recv()
    x_fwd = rcopy(xg.at[ip[2]], xg.at[ip[2]], xs.at[2], xr.at[2], {'m1': ip[1]})
    x_fwd.start()

    def z1(b, e):
        t = ip[e]
        if b < 3:
            src = wq.at[b, rows_at(g * half, half), ds(t * qw, qw)]
        else:
            src = wu.at[rows_at(g * half, half), ds(t * uw + (b - 3) * qw, qw)]
        return rcopy(src, w1.at[b, rows_at(i * dim + g * half, half), :], w1s.at[0], w1r.at[b, e - 1], {'m1': t})

    def piece1(b, k, s):
        part = w1.at[b, rows_at(s * dim + g * half, half), :]
        return (rcopy(part, part, w1s.at[0], w1r.at[b, k], {'m1': s}), rcopy(part, part, f1s.at[0], f1r.at[b], {'dp': 1 - g}))

    def forward1(b):
        for k, s in peers1:
            arrival, swap = piece1(b, k, s)
            arrival.wait_recv()
            swap.start()

    def swapped1(b):
        part = w1.at[b, 0:3 * half, :]
        return rcopy(part, part, f1s.at[0], f1r.at[b], {'dp': 1 - g})

    def issue1(b):
        for e in (2, 3, 1):
            z1(b, e).start()

    issue1(0)
    issue1(1)

    qh, uh = qw // 2, uw // 2

    def z2(c, e):
        t = ip[e]
        cols, to = ds(c * LANES, LANES), ds(i * LANES, LANES)
        return [rcopy(wd.at[rows_at(t * uw + g * uh, uh), cols], w2.at[c, g, qh:qh + uh, to], w2s.at[0], w2r.at[c, e - 1], {'m1': t}),
                rcopy(wo.at[rows_at(t * qw + g * qh, qh), cols], w2.at[c, g, 0:qh, to], w2s.at[0], w2r.at[c, e - 1], {'m1': t})]

    def issue2(c):
        for e in (2, 3, 1):
            for copy in z2(c, e):
                copy.start()

    def forward2(c):
        for k, s in peers1:
            part = w2.at[c, g, :, ds(s * LANES, LANES)]
            rcopy(part, part, w2s.at[0], w2r.at[c, k], {'m1': s}).wait_recv()
            rcopy(part, part, f2s.at[0], f2r.at[c], {'dp': 1 - g}).start()

    def next2(c):
        forward2(c)

        @pl.when(c + AHEAD < nc)
        def _():
            issue2(c + AHEAD)

    x_own.wait()
    rcopy(xg.at[ip[1]], xg.at[ip[1]], xs.at[1], xr.at[1], {'m1': ip[1]}).wait_recv()
    rcopy(xg.at[ip[3]], xg.at[ip[3]], xs.at[2], xr.at[2], {'m1': ip[1]}).wait_recv()

    def u_out(r, slot):
        return pltpu.make_async_copy(ubl.at[slot], u.at[rows_at(j * rows + r * ln_rows, ln_rows), :], ub_sem.at[slot])

    @pl.loop(0, rows // ln_rows)
    def _(r):
        slot = lax.rem(r, 2)

        @pl.when(r >= 2)
        def _():
            u_out(r - 2, slot).wait()
        at = rows_at(r * ln_rows, ln_rows)
        parts = [xg[s, at, :].astype(jnp.float32) for s in range(4)]
        mean = sum(jnp.sum(part, axis=-1, keepdims=True) for part in parts) / total
        parts = [part - mean for part in parts]
        variance = sum(jnp.sum(part * part, axis=-1, keepdims=True) for part in parts) / total
        inverse = lax.rsqrt(variance + LN_EPS)
        for s in range(4):
            cols = slice(s * dim, (s + 1) * dim)
            ubl[slot, :, cols] = (parts[s] * inverse * lns[:, cols]).astype(jnp.bfloat16)
        u_out(r, slot).start()

    for r in range(max(0, rows // ln_rows - 2), rows // ln_rows):
        u_out(r, r % 2).wait()

    def u_rows(q):
        return u.at[rows_at(q * rows, rows), :]

    u_far = rcopy(u_rows(j), u_rows(j), us.at[0], ur.at[0], {'m2': jp[2]})
    u_near = rcopy(u_rows(j), u_rows(j), us.at[1], ur.at[1], {'m2': jp[1]})
    u_far.start()
    u_near.start()
    for b in range(4):
        forward1(b)
        issue1(b + 2)
    rcopy(u_rows(jp[2]), u_rows(jp[2]), us.at[0], ur.at[0], {'m2': jp[2]}).wait_recv()
    u_fwd = rcopy(u_rows(jp[2]), u_rows(jp[2]), us.at[2], ur.at[2], {'m2': jp[1]})
    u_fwd.start()
    rcopy(u_rows(jp[1]), u_rows(jp[1]), us.at[1], ur.at[1], {'m2': jp[1]}).wait_recv()
    rcopy(u_rows(jp[3]), u_rows(jp[3]), us.at[2], ur.at[2], {'m2': jp[1]}).wait_recv()

    def lhs_in(m, slot):
        return pltpu.make_async_copy(u.at[rows_at(m * block, block), :], lhs.at[slot], lhs_sem.at[slot])

    def product1(b, own, store):
        swapped1(b).wait_recv()
        loads = [pltpu.make_async_copy(own, rhs.at[rows_at(i * dim, dim), :], rhs_sem.at[0])]
        for e in (1, 2, 3):
            at = rows_at(ip[e] * dim, dim)
            loads.append(pltpu.make_async_copy(w1.at[b, at, :], rhs.at[at, :], rhs_sem.at[e]))
        for load in loads:
            load.start()
        lhs_in(0, 0).start()
        for load in loads:
            load.wait()

        @pl.loop(0, tokens // block)
        def _(m):
            slot = lax.rem(m, 2)
            lhs_in(m, slot).wait()

            @pl.when(m + 1 < tokens // block)
            def _():
                lhs_in(m + 1, 1 - slot).start()
            store(rows_at(m * block, block), dot(lhs[slot], rhs[...]))

    @pl.loop(0, 3)
    def _(b):
        def store(at, value):
            zq[b, at, :] = value.astype(jnp.bfloat16)
        product1(b, wq.at[b, :, ds(i * qw, qw)], store)

        @pl.when(b == 1)
        def _():
            forward1(4)
            issue1(6)

    @pl.loop(0, batch)
    def _(n):
        at = rows_at(n * patches, patches)
        for head in range(heads):
            cols = slice(head * LANES, (head + 1) * LANES)
            query = head_norm(zq[0, at, cols].astype(jnp.float32), qns[...])
            key = head_norm(zq[1, at, cols].astype(jnp.float32), kns[...])
            scores = lax.dot_general(query, key, (((1,), (1,)), ((), ())), preferred_element_type=jnp.float32) * LANES ** -0.5
            scores = jnp.exp(scores - jnp.max(scores, axis=-1, keepdims=True))
            probs = (scores / jnp.sum(scores, axis=-1, keepdims=True)).astype(jnp.bfloat16)
            h[at, cols] = dot(probs, zq[2, at, cols]).astype(jnp.bfloat16)

    forward1(5)
    for c in range(AHEAD // 2):
        issue2(c)

    @pl.loop(0, nub)
    def _(b):
        def store(at, value):
            value = value.astype(jnp.bfloat16).astype(jnp.float32) + bu[:, ds(i * uw + b * qw, qw)]
            value = 0.5 * value * (1.0 + lax.erf(value * 2.0 ** -0.5))
            h[at, ds(qw + b * qw, qw)] = value.astype(jnp.bfloat16)
        product1(b + 3, wu.at[:, ds(i * uw + b * qw, qw)], store)

        @pl.when(b == 1)
        def _():
            forward1(6)
            for c in range(AHEAD // 2, AHEAD):
                issue2(c)

        @pl.when(b == 2)
        def _():
            next2(0)

        @pl.when(b == 3)
        def _():
            next2(1)

    def quarter(yy, core):
        return (2 * yy + core) * rows

    def send_a(c, yy):
        return rcopy(pa.at[lax.rem(c, 2), yy], ra.at[c, yy], as_.at[lax.rem(c, 2)], ar.at[c], {'m2': jp[1]})

    def all_a(c):
        return rcopy(pa.at[lax.rem(c, 2)], ra.at[c], as_.at[lax.rem(c, 2)], ar.at[c], {'m2': jp[1]})

    def send_b(c):
        return rcopy(ss.at[lax.rem(c, 2)], rb.at[c], bs.at[lax.rem(c, 2)], br.at[c], {'m2': jp[2]})

    def send_c(c, k):
        src = rb.at[c, :, ds(ip[1 + 2 * k] * LANES, LANES)]
        return rcopy(src, rc.at[c, k], cs.at[0], cr.at[c], {'m1': ip[1]})

    def send_d(c):
        return rcopy(ud.at[c], rd.at[c], dsm.at[0], drm.at[c], {'m1': ip[2]})

    def out_part(c, q):
        return out.at[rows_at(q * rows, rows), ds(c * LANES, LANES)]

    def result(c, q, sem, recv, device):
        part = out_part(c, q)
        return rcopy(part, part, es.at[sem], recv, device)

    def product2(c):
        slot = lax.rem(c, 2)
        cols, to = ds(c * LANES, LANES), ds(i * LANES, LANES)
        loads = [pltpu.make_async_copy(wo.at[rows_at(i * qw, qw), cols], w2b.at[slot, 0:qw, to], w2b_sem.at[0]),
                 pltpu.make_async_copy(wd.at[rows_at(i * uw, uw), cols], w2b.at[slot, qw:qw + uw, to], w2b_sem.at[1])]
        for load in loads:
            load.start()
        part = w2.at[c, 0, :, 0:3 * LANES]
        rcopy(part, part, f2s.at[0], f2r.at[c], {'dp': 1 - g}).wait_recv()
        for e in (1, 2, 3):
            to = ds(ip[e] * LANES, LANES)
            for k in range(2):
                sems = 2 + 4 * (e - 1) + 2 * k
                loads.append(pltpu.make_async_copy(w2.at[c, k, 0:qh, to], w2b.at[slot, k * qh:(k + 1) * qh, to], w2b_sem.at[sems]))
                loads.append(pltpu.make_async_copy(w2.at[c, k, qh:qh + uh, to], w2b.at[slot, qw + k * uh:qw + (k + 1) * uh, to], w2b_sem.at[sems + 1]))
        for load in loads[2:]:
            load.start()

        @pl.when(c >= 2)
        def _():
            all_a(c - 2).wait_send()
        for load in loads:
            load.wait()
        for yy in range(2):
            for sub in range(2):
                at = rows_at(quarter(yy, 1 - jc) + sub * block, block)
                pa[slot, yy, sub * block:(sub + 1) * block, :] = dot(h[at, :], w2b[slot]).astype(jnp.bfloat16)
            send_a(c, yy).start()
        keep = lax.rem(c, 3)
        for yy in range(2):
            for sub in range(2):
                at = rows_at(quarter(yy, jc) + sub * block, block)
                po[keep, yy, sub * block:(sub + 1) * block, :] = dot(h[at, :], w2b[slot]).astype(jnp.bfloat16)

    def add(a, b):
        return (a.astype(jnp.float32) + b.astype(jnp.float32)).astype(jnp.bfloat16)

    def sum_core(d):
        keep = lax.rem(d, 3)
        rcopy(ra.at[d], ra.at[d], as_.at[0], ar.at[d], {'m2': jp[1]}).wait_recv()
        load = pltpu.make_async_copy(ra.at[d], rav, rav_sem.at[0])
        load.start()

        @pl.when(d >= 2)
        def _():
            send_b(d - 2).wait_send()
        load.wait()
        ss[lax.rem(d, 2)] = add(po[keep, 1 - jy], rav[1 - jy])
        send_b(d).start()
        po[keep, jy] = add(po[keep, jy], rav[jy])

    def sum_y(d):
        rcopy(rb.at[d], rb.at[d], bs.at[0], br.at[d], {'m2': jp[2]}).wait_recv()
        rb[d] = add(po[lax.rem(d, 3), jy], rb[d])
        for k in range(2):
            send_c(d, k).start()

    def sum_near(d):
        rcopy(rc.at[d], rc.at[d], cs.at[0], cr.at[d], {'m1': ip[1]}).wait_recv()
        ud[d] = add(rb[d, :, ds(ip[2] * LANES, LANES)], rc[d, 1])
        send_d(d).start()

    def finish(d):
        rcopy(rd.at[d], rd.at[d], dsm.at[0], drm.at[d], {'m1': ip[2]}).wait_recv()
        cols = ds(d * LANES, LANES)
        value = rb[d, :, ds(i * LANES, LANES)].astype(jnp.float32) + rc[d, 0].astype(jnp.float32) + rd[d].astype(jnp.float32)
        value = xg[i, :, cols].astype(jnp.float32) + value + bo[cols][None, :]
        out[rows_at(j * rows, rows), cols] = value.astype(jnp.bfloat16)
        result(d, j, 0, er.at[d], {'m2': jp[2]}).start()
        result(d, j, 1, fr.at[0], {'m2': jp[1]}).start()

    def pass_on(d):
        result(d, jp[2], 0, er.at[d], {'m2': jp[2]}).wait_recv()
        result(d, jp[2], 2, fr.at[1], {'m2': jp[1]}).start()

    def run(step, first, last):
        @pl.loop(first, last)
        def _(d):
            step(d)

    early = 2 + 2 * mid

    def late(c, lag, step, last=nc):
        @pl.when((c >= lag) & (c < last))
        def _():
            step(c - lag)

    @pl.loop(0, nc)
    def _(c):
        late(c, 2, sum_y)
        late(c, 1, sum_core)

        @pl.when((c >= 1) & (c + 1 < nc))
        def _():
            next2(c + 1)

        @pl.when(c == nc - 2)
        def _():
            run(sum_near, 0, early)

        @pl.when(c == nc - 1)
        def _():
            run(sum_near, early, early + 2)
            finish(0)
        product2(c)

    sum_core(nc - 1)
    run(sum_near, early + 2, early + 5)
    sum_y(nc - 2)
    run(sum_near, early + 5, nc - 2)
    run(finish, 1, 4)
    sum_y(nc - 1)
    sum_near(nc - 2)
    run(finish, 4, nc - 3)
    sum_near(nc - 1)
    run(finish, nc - 3, nc)
    run(pass_on, 0, nc)

    for copy in (x_far, x_near, x_fwd, u_far, u_near, u_fwd):
      copy.wait_send()
    for sem in (w1s, f1s):
        part = w1.at[:, 0:3 * half, :]
        rcopy(part, part, sem.at[0], w1r.at[0, 0], {'dp': 1 - g}).wait_send()
    for sem in (w2s, f2s):
        part = w2.at[:, 0, :, 0:3 * LANES]
        rcopy(part, part, sem.at[0], f2r.at[0], {'dp': 1 - g}).wait_send()
    for c in (nc - 2, nc - 1):
        all_a(c).wait_send()
        send_b(c).wait_send()
    rcopy(rc, rc, cs.at[0], cr.at[0], {'m1': ip[1]}).wait_send()
    for sem in (dsm.at[0], es.at[0], es.at[1], es.at[2]):
        rcopy(rd, rd, sem, drm.at[0], {'m1': ip[2]}).wait_send()
    for k in range(2):
        rcopy(rd, rd, es.at[1], fr.at[k], {'m2': jp[1]}).wait_recv()


def solution(mesh):
    assert mesh.shape['m1'] == 4 and mesh.shape['m2'] == 4 and mesh.shape['dp'] == 2

    def local_layer(x_blk, ln_scale, qn_scale, kn_scale, w_qkv, w_up, b_up, w_o, w_down, b_out):
        batch, patches, dim = x_blk.shape
        tokens = batch * patches
        qw, uw = w_qkv.shape[2] // 4, w_up.shape[1] // 4
        rows, block, nc, nb = tokens // 4, tokens // 8, dim // LANES, 3 + uw // qw
        assert qn_scale.shape[0] == LANES and uw % qw == 0 and nb == 7
        wide = 4 * LANES
        bf16 = jnp.bfloat16
        dma = pltpu.SemaphoreType.DMA
        hbm = pl.BlockSpec(memory_space=pltpu.HBM)
        vmem = pl.BlockSpec(memory_space=pltpu.VMEM)
        ln_rows = min(64, rows)
        out = pl.pallas_call(
            functools.partial(kernel, (batch, patches, dim, qw, uw)),
            out_shape=[
                pltpu.VMEM((tokens, dim), bf16),
                jax.ShapeDtypeStruct((tokens, 4 * dim), bf16),
                jax.ShapeDtypeStruct((nb, 4 * dim, qw), bf16),
                jax.ShapeDtypeStruct((nc, 2, (qw + uw) // 2, wide), bf16),
                jax.ShapeDtypeStruct((nc, 2, rows, wide), bf16)],
            in_specs=[hbm, vmem, vmem, vmem, hbm, hbm, vmem, hbm, hbm, vmem],
            out_specs=[vmem] + [hbm] * 4,
            scratch_shapes=[
                pltpu.VMEM((4, rows, dim), bf16),
                pltpu.VMEM((2, ln_rows, 4 * dim), bf16),
                pltpu.VMEM((3, tokens, qw), bf16),
                pltpu.VMEM((tokens, qw + uw), bf16),
                pltpu.VMEM((4 * dim, qw), bf16),
                pltpu.VMEM((2, block, 4 * dim), bf16),
                pltpu.VMEM((2, qw + uw, wide), bf16),
                pltpu.VMEM((2, 2, rows, wide), bf16),
                pltpu.VMEM((3, 2, rows, wide), bf16),
                pltpu.VMEM((2, rows, wide), bf16),
                pltpu.VMEM((2, rows, wide), bf16),
                pltpu.VMEM((nc, rows, wide), bf16),
                pltpu.VMEM((nc, 2, rows, LANES), bf16),
                pltpu.VMEM((nc, rows, LANES), bf16),
                pltpu.VMEM((nc, rows, LANES), bf16),
                dma((3,)), dma((3,)),
                dma((1,)), dma((nb, 3)), dma((1,)), dma((nb,)),
                dma((3,)), dma((3,)),
                dma((1,)), dma((nc, 3)), dma((1,)), dma((nc,)),
                dma((2,)), dma((nc,)), dma((2,)), dma((nc,)), dma((1,)), dma((nc,)), dma((1,)), dma((nc,)),
                dma((3,)), dma((nc,)), dma((2,)),
                dma((1,)), dma((4,)), dma((2,)), dma((2,)), dma((14,)), dma((1,))],
            compiler_params=pltpu.CompilerParams(collective_id=0, has_side_effects=True, vmem_limit_bytes=60_000_000),
            name='layer',
        )(x_blk.reshape(tokens, dim), ln_scale[None], qn_scale[None], kn_scale[None], w_qkv.transpose(1, 0, 2), w_up,
          b_up[None], w_o, w_down, b_out)[0]
        return out.reshape(batch, patches, dim)

    return jax.shard_map(local_layer, mesh=mesh, in_specs=(P('dp', None, 'm1'), P(), P(), P(), P('m1', None, 'm2'), P('m1', 'm2'), P('m2'), P('m2', 'm1'), P('m2', 'm1'), P('m1')), out_specs=P('dp', None, 'm1'), check_vma=False)
```
